32 devices in a mesh: hp: 4 (over x, y), cp: 8 (over z, core).
Axes of the slice: x: 2, y: 2, z: 4, core: 2. Of those that a mesh axis runs over, the one named last changes fastest.
Arguments:
- q: bfloat16 [6144, 12, 128], P('cp', 'hp'), parts along dimension 1
- k: bfloat16 [6144, 12, 128], P('cp', 'hp'), parts along dimension 1
- v: bfloat16 [6144, 12, 128], P('cp', 'hp'), parts along dimension 1
- u_bias: float32 [12, 128], P('hp'), parts along dimension 0
- v_bias: float32 [12, 128], P('hp'), parts along dimension 0
- rel_table: bfloat16 [6144, 1536], P('cp')
- w_rel: bfloat16 [1536, 12, 128], P(None, 'hp'), parts along dimension 1
- d_out: bfloat16 [6144, 12, 128], P('cp', 'hp'), parts along dimension 1
Outputs:
- output 1: bfloat16 [6144, 12, 128], P('cp', 'hp'), parts along dimension 1
- output 2: bfloat16 [6144, 12, 128], P('cp', 'hp'), parts along dimension 1
- output 3: bfloat16 [6144, 12, 128], P('cp', 'hp'), parts along dimension 1
- output 4: bfloat16 [6144, 12, 128], P('cp', 'hp'), parts along dimension 1
- output 5: float32 [12, 128], P('hp'), parts along dimension 0
- output 6: float32 [12, 128], P('hp'), parts along dimension 0
- output 7: float32 [1536, 12, 128], P(None, 'hp'), parts along dimension 1
There are 4 independent parts. The reference program is written for one: setup_inputs(seed, part) draws one part's arguments, and reference() takes and returns one part's arrays. A program takes and returns all parts, laid end to end along the dimension named above; an argument that names none is the same for every part.
All inputs are finite; a program needn't handle non-finite values.
Results may differ from the reference program's by a relative error of at most 0.014711.
Values are sent between devices in bfloat16 or wider.
A program may use at most 1 GiB of HBM per device.

```python
import math
import jax
import jax.numpy as jnp
from jax import lax

SEQ_LEN = 6144
HEADS_PART = 3
HEAD_DIM = 128
MODEL_DIM = 1536
ROW_BLOCK = math.gcd(SEQ_LEN, 256)
INV_SQRT = HEAD_DIM ** -0.5


def setup_inputs(seed: int = 0, part: int = 0) -> dict:
    part_key = jax.random.fold_in(jax.random.key(seed), part)
    keys_part = jax.random.split(part_key, 7)
    table_keys = jax.random.split(jax.random.key(seed + 17), 2)
    seq_shape = (SEQ_LEN, HEADS_PART, HEAD_DIM)
    head_shape = (HEADS_PART, HEAD_DIM)
    q = jax.random.normal(keys_part[0], seq_shape, jnp.float32)
    k = 2.0 * jax.random.normal(keys_part[1], seq_shape, jnp.float32)
    v = jax.random.normal(keys_part[2], seq_shape, jnp.float32)
    u_bias = 0.5 * jax.random.normal(keys_part[3], head_shape, jnp.float32)
    v_bias = jax.random.normal(keys_part[4], head_shape, jnp.float32)
    w_rel = jax.random.normal(keys_part[5], (MODEL_DIM, HEADS_PART, HEAD_DIM), jnp.float32) * MODEL_DIM ** -0.5
    d_out = jax.random.normal(keys_part[6], seq_shape, jnp.float32)
    freq_cols = 10000.0 ** (-jax.random.uniform(table_keys[0], (MODEL_DIM,), jnp.float32))
    phases = 2.0 * math.pi * jax.random.uniform(table_keys[1], (MODEL_DIM,), jnp.float32)
    offsets = jnp.arange(SEQ_LEN, dtype=jnp.float32)
    rel_table = jnp.sin(offsets[:, None] * freq_cols[None, :] + phases[None, :])
    return {
        'q': q.astype(jnp.bfloat16),
        'k': k.astype(jnp.bfloat16),
        'v': v.astype(jnp.bfloat16),
        'u_bias': u_bias,
        'v_bias': v_bias,
        'rel_table': rel_table.astype(jnp.bfloat16),
        'w_rel': w_rel.astype(jnp.bfloat16),
        'd_out': d_out.astype(jnp.bfloat16),
    }


def attention(q_u, q_v, k, v, rel):
    key_pos = jnp.arange(SEQ_LEN)

    def one_head(head_args):
        qu_h, qv_h, k_h, v_h, rel_h = head_args

        def row_block(start):
            qu_rows = lax.dynamic_slice_in_dim(qu_h, start, ROW_BLOCK)
            qv_rows = lax.dynamic_slice_in_dim(qv_h, start, ROW_BLOCK)
            query_pos = start + jnp.arange(ROW_BLOCK)
            offset_ij = query_pos[:, None] - key_pos[None, :]
            content = jnp.dot(qu_rows, k_h.T)
            by_offset = jnp.dot(qv_rows, rel_h.T)
            position = jnp.take_along_axis(by_offset, jnp.clip(offset_ij, 0, SEQ_LEN - 1), axis=1)
            score_ij = jnp.where(offset_ij >= 0, (content + position) * INV_SQRT, -jnp.inf)
            return jnp.dot(jax.nn.softmax(score_ij, axis=-1), v_h)

        starts = jnp.arange(0, SEQ_LEN, ROW_BLOCK)
        return lax.map(jax.checkpoint(row_block), starts).reshape(SEQ_LEN, HEAD_DIM)

    per_head = lax.map(jax.checkpoint(one_head), tuple(stacked.transpose(1, 0, 2) for stacked in (q_u, q_v, k, v, rel)))
    return per_head.transpose(1, 0, 2)


def reference(q, k, v, u_bias, v_bias, rel_table, w_rel, d_out):
    rel = jnp.dot(rel_table, w_rel.reshape(MODEL_DIM, HEADS_PART * HEAD_DIM), preferred_element_type=jnp.float32)
    rel = rel.astype(jnp.bfloat16).reshape(SEQ_LEN, HEADS_PART, HEAD_DIM)
    q_wide = q.astype(jnp.float32)
    q_u = (q_wide + u_bias).astype(jnp.bfloat16).astype(jnp.float32)
    q_v = (q_wide + v_bias).astype(jnp.bfloat16).astype(jnp.float32)
    out_full, pullback = jax.vjp(attention, q_u, q_v, k.astype(jnp.float32), v.astype(jnp.float32), rel.astype(jnp.float32))
    g_qu, g_qv, g_k, g_v, g_rel = pullback(d_out.astype(jnp.float32))
    d_rel = g_rel.astype(jnp.bfloat16).reshape(SEQ_LEN, HEADS_PART * HEAD_DIM)
    d_w_rel = jnp.dot(rel_table.T, d_rel, preferred_element_type=jnp.float32).reshape(MODEL_DIM, HEADS_PART, HEAD_DIM)
    return (
        out_full.astype(jnp.bfloat16),
        (g_qu + g_qv).astype(jnp.bfloat16),
        g_k.astype(jnp.bfloat16),
        g_v.astype(jnp.bfloat16),
        g_qu.sum(axis=0),
        g_qv.sum(axis=0),
        d_w_rel,
    )
```

```python
import functools
import math

import jax
import jax.numpy as jnp
from jax import lax
from jax.experimental import pallas as pl
from jax.experimental.pallas import tpu as pltpu
from jax.sharding import PartitionSpec as P

F32, BF16 = jnp.float32, jnp.bfloat16
ROWS = 256
COLS = 512
NT = (((1,), (1,)), ((), ()))
NN = (((1,), (0,)), ((), ()))


def mm(a, b, dims=NN, precision=None):
    return lax.dot_general(a, b, dims, preferred_element_type=F32, precision=precision)


def fold_lanes(op, x):
    acc = x[:, :128]
    for g in range(1, x.shape[1] // 128):
        acc = op(acc, x[:, g * 128:(g + 1) * 128])
    return acc


def shear(window, shift):
    half = window.shape[0] // 2
    width = window.shape[1]
    top = pltpu.roll(window[:half, 128:], shift, 1, stride=1, stride_axis=0)[:, 128:]
    low = pltpu.roll(window[half:, :width - 128], shift, 1, stride=1, stride_axis=0)[:, 128:]
    return jnp.concatenate([top, low], axis=0)


def tile_grads(q0, out_row, q_ref, k_ref, v_ref, do_ref, rel_ref, bias_ref, o_ref, dq_ref, dkt, dvt, drt, bias_acc, buf, m_ref, l_ref, acc_ref, gu_ref, gv_ref):
    seq, dim = k_ref.shape
    scale = dim ** -0.5
    steps = (q0 + ROWS + COLS - 1) // COLS
    rel0 = seq - ROWS - q0

    def at(base, size):
        return pl.ds(pl.multiple_of(base, ROWS), size)

    q_wide = q_ref[at(q0, ROWS), :].astype(F32)
    q_u = (q_wide + bias_ref[0:1, :]).astype(BF16)
    q_v = (q_wide + bias_ref[1:2, :]).astype(BF16)

    @pl.loop(0, steps)
    def _(c):
        buf[:, at(c * COLS + ROWS, COLS)] = mm(q_v, rel_ref[at(rel0 + c * COLS, COLS), :], NT)

    m_ref[...] = jnp.full_like(m_ref, -jnp.inf)
    row_minus_col = lax.broadcasted_iota(jnp.int32, (ROWS, COLS), 0) - lax.broadcasted_iota(jnp.int32, (ROWS, COLS), 1)

    @pl.loop(0, steps)
    def _(c):
        j0 = c * COLS
        score = mm(q_u, k_ref[at(j0, COLS), :], NT) + shear(buf[:, at(j0 + ROWS, COLS + ROWS)], 1)
        score = jnp.where(row_minus_col >= j0 - q0, score, -jnp.inf)
        buf[:, at(j0 + ROWS, COLS)] = score
        m_ref[...] = jnp.maximum(m_ref[...], fold_lanes(jnp.maximum, score))

    row_max = jnp.max(m_ref[...], axis=1, keepdims=True)
    l_ref[...] = jnp.zeros_like(l_ref)
    acc_ref[...] = jnp.zeros_like(acc_ref)

    @pl.loop(0, steps)
    def _(c):
        j0 = c * COLS
        prob = jnp.exp2((buf[:, at(j0 + ROWS, COLS)] - row_max) * (scale * math.log2(math.e)))
        buf[:, at(j0 + ROWS, COLS)] = prob
        l_ref[...] += fold_lanes(jnp.add, prob)
        acc_ref[...] += mm(prob.astype(BF16), v_ref[at(j0, COLS), :])

    inv_sum = 1.0 / jnp.sum(l_ref[...], axis=1, keepdims=True)
    out = acc_ref[...] * inv_sum
    o_ref[at(out_row, ROWS), :] = out.astype(BF16)
    d_out = do_ref[at(q0, ROWS), :]
    do_wide = d_out.astype(F32)
    delta = jnp.sum(do_wide * out, axis=1, keepdims=True)
    anti = (lax.broadcasted_iota(jnp.int32, (ROWS, ROWS), 0) + lax.broadcasted_iota(jnp.int32, (ROWS, ROWS), 1) == ROWS - 1)
    anti_b = anti.astype(F32).astype(BF16)
    do_t = do_wide.T.astype(BF16)
    qu_t = q_u.astype(F32).T.astype(BF16)
    qv_rt = mm(anti_b, q_v).T.astype(BF16)
    gu_ref[...] = jnp.zeros_like(gu_ref)
    gv_ref[...] = jnp.zeros_like(gv_ref)

    @pl.loop(0, steps)
    def _(c):
        j0 = c * COLS
        cols = at(j0, COLS)
        prob = buf[:, at(j0 + ROWS, COLS)] * inv_sum
        ds = (prob * (mm(d_out, v_ref[cols, :], NT) - delta)).astype(BF16)
        buf[:, at(j0 + ROWS, COLS)] = mm(anti_b, ds)
        dvt[:, cols] += mm(do_t, prob.astype(BF16))
        dkt[:, cols] += mm(qu_t, ds)
        gu_ref[...] += mm(ds, k_ref[cols, :])

    @pl.loop(0, steps)
    def _(c):
        c0 = c * COLS
        by_offset = shear(buf[:, at(c0, COLS + ROWS)], 0).astype(BF16)
        cols = at(rel0 + c0, COLS)
        gv_ref[...] += mm(by_offset, rel_ref[cols, :])
        drt[:, cols] += mm(qv_rt, by_offset)

    g_u = gu_ref[...]
    g_vr = gv_ref[...]
    g_v = mm(anti.astype(F32), g_vr, precision=lax.Precision.HIGHEST)
    dq_ref[at(out_row, ROWS), :] = ((g_u + g_v) * scale).astype(BF16)
    bias_acc[0:1, :] += jnp.sum(g_u, axis=0, keepdims=True) * scale
    bias_acc[1:2, :] += jnp.sum(g_vr, axis=0, keepdims=True) * scale


def tile_index(i, core):
    return 4 * (i // 2) + jnp.where(i % 2 == 0, core, 3 - core)


def group_kernel(xs, rels, bias_ref, o_out, g_out, bias_acc, xh, relh, dkt, dvt, drt, part, red, o_tiles, *rest):
    scratch, sems = rest[:6], rest[6:]
    in_send, in_recv, fwd_send, fwd_recv, part_send, part_recv, tile_send, red_send, out_recv, g_recv = sems
    n_arr, n_heads, block, dim = xs.shape
    n_dev = lax.axis_size('cp')
    n_chips = n_dev // 2
    seq = block * n_dev
    scale = dim ** -0.5
    me = lax.axis_index('cp')
    chip, core = me // 2, me % 2
    head = jnp.minimum(chip, n_heads - 1)
    active = chip < n_heads
    partner = 2 * chip + 1 - core
    n_tiles = seq // ROWS // 2

    barrier = pltpu.get_barrier_semaphore()
    for d in range(1, n_dev):
        pl.semaphore_signal(barrier, inc=1, device_id={'cp': (me + d) % n_dev}, device_id_type=pl.DeviceIdType.MESH)
    pl.semaphore_wait(barrier, n_dev - 1)

    def push(src, dst, send, recv, dev):
        return pltpu.make_async_remote_copy(src_ref=src, dst_ref=dst, send_sem=send, recv_sem=recv, device_id={'cp': dev}, device_id_type=pl.DeviceIdType.MESH)

    def rows_of(dev):
        return pl.ds(pl.multiple_of(dev * block, block), block)

    def flip_rows_of(dev):
        return pl.ds(pl.multiple_of(seq - block - dev * block, block), block)

    def input_pair(dest_head, src_dev, x_src, rel_src, send, recv, dev):
        return (
            push(x_src, xh.at[:, rows_of(src_dev), :], send.at[0], recv.at[0], dev),
            push(rel_src, relh.at[flip_rows_of(src_dev), :], send.at[1], recv.at[1], dev),
        )

    def send_to(dest_head):
        return input_pair(dest_head, me, xs.at[:, dest_head], rels.at[dest_head], in_send.at[dest_head], in_recv.at[chip], 2 * dest_head + core)

    def relay(src_chip):
        src_dev = 2 * src_chip + core
        return input_pair(head, src_dev, xh.at[:, rows_of(src_dev), :], relh.at[flip_rows_of(src_dev), :], fwd_send.at[src_chip], fwd_recv.at[src_chip], partner)

    def relay_own():
        return input_pair(head, me, xs.at[:, head], rels.at[head], fwd_send.at[chip], fwd_recv.at[chip], partner)

    def local_own():
        return (
            pltpu.make_async_copy(xs.at[:, head], xh.at[:, rows_of(me), :], in_recv.at[chip, 0]),
            pltpu.make_async_copy(rels.at[head], relh.at[flip_rows_of(me), :], in_recv.at[chip, 1]),
        )

    for dest in range(n_heads):
        @pl.when(chip != dest)
        def _():
            for copy in send_to(dest):
                copy.start()

    dkt[...] = jnp.zeros_like(dkt)
    dvt[...] = jnp.zeros_like(dvt)
    drt[...] = jnp.zeros_like(drt)
    bias_acc[...] = jnp.zeros_like(bias_acc)
    scratch[0][:, :ROWS] = jnp.zeros((ROWS, ROWS), F32)
    relh[pl.ds(seq, COLS), :] = jnp.zeros((COLS, dim), BF16)

    @pl.when(active)
    def _():
        for copy in local_own():
            copy.start()
        for copy in relay_own():
            copy.start()
        for src in range(n_chips):
            @pl.when(chip != src)
            def _():
                x_in, rel_in = input_pair(head, 2 * src + core, xs.at[:, head], rels.at[head], in_send.at[0], in_recv.at[src], partner)
                x_in.wait_recv()
                rel_in.wait_recv()
                for copy in relay(src):
                    copy.start()
        for copy in local_own():
            copy.wait()
        for src in range(n_chips):
            x_in, rel_in = input_pair(head, 2 * src + 1 - core, xs.at[:, head], rels.at[head], fwd_send.at[src], fwd_recv.at[src], partner)
            x_in.wait_recv()
            rel_in.wait_recv()

    q_ref, k_ref, v_ref, do_ref = (xh.at[a] for a in range(4))

    @pl.when(active)
    def _():
        @pl.loop(0, n_tiles)
        def _(i):
            tile_grads(tile_index(i, core) * ROWS, i * ROWS, q_ref, k_ref, v_ref, do_ref, relh, bias_ref.at[head], o_tiles.at[0], o_tiles.at[1], dkt, dvt, drt, bias_acc, *scratch)

        def part_copy(a, src_chip, parity):
            dev = 2 * src_chip + parity
            acc = (dkt, dvt, drt)[a]
            cols = flip_rows_of(dev) if a == 2 else rows_of(dev)
            return push(acc.at[:, cols], part.at[a, src_chip], part_send.at[a, src_chip], part_recv.at[a, src_chip], partner)

        def tile_copy(i):
            tile = tile_index(i, core)
            per = block // ROWS
            owner = tile // per
            src = o_tiles.at[:, pl.ds(i * ROWS, ROWS), :]
            dst = o_out.at[:, head, pl.ds(pl.multiple_of((tile % per) * ROWS, ROWS), ROWS), :]
            return owner, pltpu.make_async_copy(src, dst, out_recv), push(src, dst, tile_send.at[i], out_recv, owner)

        def red_copy(a, zi):
            owner = 2 * zi + core
            src, dst = red.at[a, zi], g_out.at[a, head]
            return owner, pltpu.make_async_copy(src, dst, g_recv), push(src, dst, red_send.at[a, zi], g_recv, owner)

        def start(owner, local, remote):
            @pl.when(owner == me)
            def _():
                local.start()

            @pl.when(owner != me)
            def _():
                remote.start()

        def finish(owner, local, remote):
            @pl.when(owner != me)
            def _():
                remote.wait_send()

        for a in range(3):
            for zi in range(n_chips):
                part_copy(a, zi, 1 - core).start()
        for i in range(n_tiles):
            start(*tile_copy(i))
        for a in range(3):
            for zi in range(n_chips):
                part_copy(a, zi, core).wait_recv()
                acc = (dkt, dvt, drt)[a]
                dev = 2 * zi + core
                cols = flip_rows_of(dev) if a == 2 else rows_of(dev)
                total = acc[:, cols] + part[a, zi]
                red[a, zi] = (total if a == 1 else total * scale).astype(BF16)
                start(*red_copy(a, zi))
        for a in range(3):
            for zi in range(n_chips):
                part_copy(a, zi, 1 - core).wait_send()
                finish(*red_copy(a, zi))
        for i in range(n_tiles):
            finish(*tile_copy(i))
        for src in range(n_chips):
            @pl.when(chip != src)
            def _():
                for copy in relay(src):
                    copy.wait_send()
        for copy in relay_own():
            copy.wait_send()

    for dest in range(n_heads):
        @pl.when(chip != dest)
        def _():
            for copy in send_to(dest):
                copy.wait_send()
    pltpu.make_async_copy(o_out, o_out, out_recv).wait()
    pltpu.make_async_copy(g_out, g_out, g_recv).wait()


def group_call(xs, rels, bias, n_dev):
    n_arr, n_heads, block, dim = xs.shape
    seq = block * n_dev
    n_chips = n_dev // 2
    n_tiles = seq // ROWS // 2
    anyw = pl.BlockSpec(memory_space=pl.ANY)
    vmem = pl.BlockSpec(memory_space=pltpu.VMEM)
    dma = pltpu.SemaphoreType.DMA
    return pl.pallas_call(
        group_kernel,
        name='rel_attention',
        in_specs=[anyw, anyw, vmem],
        out_specs=[anyw, anyw, vmem],
        out_shape=[
            jax.ShapeDtypeStruct((2, n_heads, block, dim), BF16),
            jax.ShapeDtypeStruct((3, n_heads, dim, block), BF16),
            jax.ShapeDtypeStruct((8, dim), F32),
        ],
        scratch_shapes=[
            pltpu.VMEM((n_arr, seq, dim), BF16),
            pltpu.VMEM((seq + COLS, dim), BF16),
            pltpu.VMEM((dim, seq), F32),
            pltpu.VMEM((dim, seq), F32),
            pltpu.VMEM((dim, seq + COLS), F32),
            pltpu.VMEM((3, n_chips, dim, block), F32),
            pltpu.VMEM((3, n_chips, dim, block), BF16),
            pltpu.VMEM((2, seq // 2, dim), BF16),
            pltpu.VMEM((ROWS, seq + 2 * ROWS), F32),
            pltpu.VMEM((ROWS, 128), F32),
            pltpu.VMEM((ROWS, 128), F32),
            pltpu.VMEM((ROWS, dim), F32),
            pltpu.VMEM((ROWS, dim), F32),
            pltpu.VMEM((ROWS, dim), F32),
            dma((n_heads, 2)), dma((n_chips, 2)), dma((n_chips, 2)), dma((n_chips, 2)),
            dma((3, n_chips)), dma((3, n_chips)), dma((n_tiles,)), dma((3, n_chips)), dma, dma,
        ],
        compiler_params=pltpu.CompilerParams(vmem_limit_bytes=62 * 2**20, collective_id=0, has_side_effects=True),
    )(xs, rels, bias)


def solution(mesh):
    n_dev = mesh.shape['cp']
    seq_spec = P('cp', 'hp', None)
    head_spec = P('hp', None)
    weight_spec = P(None, 'hp', None)

    def local_fn(q, k, v, u_bias, v_bias, rel_table, w_rel, d_out):
        block, n_heads, dim = q.shape
        rel = jnp.einsum('uo,ojf->juf', rel_table, w_rel, preferred_element_type=F32).astype(BF16)
        xs = jnp.stack([x.transpose(1, 0, 2) for x in (q, k, v, d_out)])
        bias = jnp.pad(jnp.stack([u_bias, v_bias], axis=1), ((0, 0), (0, 6), (0, 0)))
        o, g, bias_acc = group_call(xs, rel[:, ::-1], bias, n_dev)
        chip = lax.axis_index('cp') // 2
        mine = (jnp.arange(n_heads) == chip)[None, :, None]
        d_bias = lax.psum(jnp.where(mine, bias_acc[:2, None, :], 0.0), 'cp')
        d_rel = g[2][:, :, ::-1]
        d_w_rel = lax.psum(jnp.einsum('uo,jfu->ojf', rel_table, d_rel, preferred_element_type=F32), 'cp')
        return (
            o[0].transpose(1, 0, 2),
            o[1].transpose(1, 0, 2),
            g[0].transpose(2, 0, 1),
            g[1].transpose(2, 0, 1),
            d_bias[0],
            d_bias[1],
            d_w_rel,
        )

    return jax.shard_map(
        local_fn,
        mesh=mesh,
        in_specs=(seq_spec, seq_spec, seq_spec, head_spec, head_spec, P('cp', None), weight_spec, seq_spec),
        out_specs=(seq_spec, seq_spec, seq_spec, seq_spec, head_spec, head_spec, weight_spec),
        check_vma=False,
    )
```

```python
import functools
import math

import jax
import jax.numpy as jnp
from jax import lax
from jax.experimental import pallas as pl
from jax.experimental.pallas import tpu as pltpu
from jax.sharding import PartitionSpec as P

F32, BF16 = jnp.float32, jnp.bfloat16
ROWS = 512
COLS = 512
NT = (((1,), (1,)), ((), ()))
NN = (((1,), (0,)), ((), ()))


def mm(a, b, dims=NN, precision=None):
    return lax.dot_general(a, b, dims, preferred_element_type=F32, precision=precision)


def fold_lanes(op, x):
    acc = x[:, :128]
    for g in range(1, x.shape[1] // 128):
        acc = op(acc, x[:, g * 128:(g + 1) * 128])
    return acc


def shear(buf, start, shift):
    out = []
    for g in range(ROWS // 128):
        part = buf[g * 128:(g + 1) * 128, pl.ds(pl.multiple_of(start - (g + 1) * 128, 128), COLS + 128)]
        out.append(pltpu.roll(part, shift, 1, stride=1, stride_axis=0)[:, 128:])
    return jnp.concatenate(out, axis=0)


def flip_rows(anti, x):
    return jnp.concatenate([mm(anti, x[g * 256:(g + 1) * 256]) for g in reversed(range(x.shape[0] // 256))], axis=0)


def tile_grads(q0, out_row, q_ref, k_ref, v_ref, do_ref, rel_ref, bias_ref, o_ref, dq_ref, dkt, dvt, drt, bias_acc, buf, m_ref, l_ref, acc_ref, gu_ref, gv_ref):
    seq, dim = k_ref.shape
    scale = dim ** -0.5
    steps = (q0 + ROWS + COLS - 1) // COLS
    rel0 = seq - ROWS - q0

    def at(base, size):
        return pl.ds(pl.multiple_of(base, 256), size)

    q_wide = q_ref[at(q0, ROWS), :].astype(F32)
    q_u = (q_wide + bias_ref[0:1, :]).astype(BF16)
    q_v = (q_wide + bias_ref[1:2, :]).astype(BF16)

    def offset_scores(c):
        buf[:, at(c * COLS + ROWS, COLS)] = mm(q_v, rel_ref[at(rel0 + c * COLS, COLS), :], NT)

    def scores(c):
        j0 = c * COLS
        return mm(q_u, k_ref[at(j0, COLS), :], NT) + shear(buf, j0 + 2 * ROWS, 1)

    def keep(c, score):
        buf[:, at(c * COLS + ROWS, COLS)] = score
        m_ref[...] = jnp.maximum(m_ref[...], fold_lanes(jnp.maximum, score))

    m_ref[...] = jnp.full_like(m_ref, -jnp.inf)
    offset_scores(0)

    @pl.loop(0, steps - 1)
    def _(c):
        offset_scores(c + 1)
        keep(c, scores(c))

    row_minus_col = lax.broadcasted_iota(jnp.int32, (ROWS, COLS), 0) - lax.broadcasted_iota(jnp.int32, (ROWS, COLS), 1)
    last = steps - 1
    keep(last, jnp.where(row_minus_col >= last * COLS - q0, scores(last), -jnp.inf))

    row_max = jnp.max(m_ref[...], axis=1, keepdims=True)
    l_ref[...] = jnp.zeros_like(l_ref)
    acc_ref[...] = jnp.zeros_like(acc_ref)

    @pl.loop(0, steps)
    def _(c):
        j0 = c * COLS
        prob = jnp.exp2((buf[:, at(j0 + ROWS, COLS)] - row_max) * (scale * math.log2(math.e)))
        buf[:, at(j0 + ROWS, COLS)] = prob
        l_ref[...] += fold_lanes(jnp.add, prob)
        acc_ref[...] += mm(prob.astype(BF16), v_ref[at(j0, COLS), :])

    inv_sum = 1.0 / jnp.sum(l_ref[...], axis=1, keepdims=True)
    out = acc_ref[...] * inv_sum
    o_ref[at(out_row, ROWS), :] = out.astype(BF16)
    d_out = do_ref[at(q0, ROWS), :]
    do_wide = d_out.astype(F32)
    delta = jnp.sum(do_wide * out, axis=1, keepdims=True)
    anti = (lax.broadcasted_iota(jnp.int32, (256, 256), 0) + lax.broadcasted_iota(jnp.int32, (256, 256), 1) == 255)
    anti_b = anti.astype(F32).astype(BF16)
    do_t = do_wide.T.astype(BF16)
    qu_t = q_u.astype(F32).T.astype(BF16)
    qv_rt = flip_rows(anti_b, q_v).T.astype(BF16)
    gu_ref[...] = jnp.zeros_like(gu_ref)
    gv_ref[...] = jnp.zeros_like(gv_ref)

    def by_key(c):
        j0 = c * COLS
        cols = at(j0, COLS)
        prob = buf[:, at(j0 + ROWS, COLS)] * inv_sum
        ds = (prob * (mm(d_out, v_ref[cols, :], NT) - delta)).astype(BF16)
        dvt[:, cols] += mm(do_t, prob.astype(BF16))
        dkt[:, cols] += mm(qu_t, ds)
        gu_ref[...] += mm(ds, k_ref[cols, :])
        buf[:, at(j0 + ROWS, COLS)] = flip_rows(anti_b, ds)

    def by_offset(c):
        c0 = c * COLS
        ds = shear(buf, c0 + ROWS, 0).astype(BF16)
        cols = at(rel0 + c0, COLS)
        gv_ref[...] += mm(ds, rel_ref[cols, :])
        drt[:, cols] += mm(qv_rt, ds)

    by_key(0)

    @pl.loop(1, steps)
    def _(c):
        by_offset(c - 1)
        by_key(c)

    by_offset(steps - 1)

    g_u = gu_ref[...]
    g_vr = gv_ref[...]
    anti_f = anti.astype(F32)
    g_v = jnp.concatenate([mm(anti_f, g_vr[g * 256:(g + 1) * 256], precision=lax.Precision.HIGHEST) for g in reversed(range(ROWS // 256))], axis=0)
    dq_ref[at(out_row, ROWS), :] = ((g_u + g_v) * scale).astype(BF16)
    bias_acc[0:1, :] += jnp.sum(g_u, axis=0, keepdims=True) * scale
    bias_acc[1:2, :] += jnp.sum(g_vr, axis=0, keepdims=True) * scale


def tile_index(i, core):
    return 4 * (i // 2) + jnp.where(i % 2 == 0, core, 3 - core)


def group_kernel(xs, rels, bias_ref, o_out, g_out, bias_out, xh, relh, rel_flip, dkt, dvt, drt, part, red, o_tiles, bias_acc, bias_in, *rest):
    scratch, sems = rest[:6], rest[6:]
    in_send, in_recv, fwd_send, fwd_recv, part_send, part_recv, tile_send, red_send, bias_send, out_recv, g_recv, bias_recv = sems
    n_arr, n_heads, block, dim = xs.shape
    n_dev = lax.axis_size('cp')
    n_chips = n_dev // 2
    seq = block * n_dev
    scale = dim ** -0.5
    me = lax.axis_index('cp')
    chip, core = me // 2, me % 2
    head = jnp.minimum(chip, n_heads - 1)
    active = chip < n_heads
    partner = 2 * chip + 1 - core
    n_tiles = seq // ROWS // 2

    barrier = pltpu.get_barrier_semaphore()
    for d in range(1, n_dev):
        pl.semaphore_signal(barrier, inc=1, device_id={'cp': (me + d) % n_dev}, device_id_type=pl.DeviceIdType.MESH)
    pl.semaphore_wait(barrier, n_dev - 1)

    def push(src, dst, send, recv, dev):
        return pltpu.make_async_remote_copy(src_ref=src, dst_ref=dst, send_sem=send, recv_sem=recv, device_id={'cp': dev}, device_id_type=pl.DeviceIdType.MESH)

    def rows_of(dev):
        return pl.ds(pl.multiple_of(dev * block, block), block)

    def flip_rows_of(dev):
        return pl.ds(pl.multiple_of(seq - block - dev * block, block), block)

    def x_copy(dest, src_dev, src, send, recv, dev):
        return push(src, xh.at[:, rows_of(src_dev), :], send.at[0], recv.at[0], dev)

    def rel_copy(dest, src_dev, src, send, recv, dev):
        return push(src, relh.at[flip_rows_of(src_dev), :], send.at[1], recv.at[1], dev)

    def to_head(make, srcs, dest):
        return make(dest, me, srcs, in_send.at[dest], in_recv.at[chip], 2 * dest + core)

    def x_to_head(dest):
        return to_head(x_copy, xs.at[:, dest], dest)

    def rel_to_head(dest):
        return to_head(rel_copy, rel_flip.at[dest], dest)

    def x_to_partner(dev, src, recv_dev):
        return x_copy(head, dev, src, fwd_send.at[dev // 2], fwd_recv.at[dev // 2], recv_dev)

    def rel_to_partner(dev, src, recv_dev):
        return rel_copy(head, dev, src, fwd_send.at[dev // 2], fwd_recv.at[dev // 2], recv_dev)

    def x_local():
        return pltpu.make_async_copy(xs.at[:, head], xh.at[:, rows_of(me), :], in_recv.at[chip, 0])

    def rel_local():
        return pltpu.make_async_copy(rel_flip.at[head], relh.at[flip_rows_of(me), :], in_recv.at[chip, 1])

    anti = (lax.broadcasted_iota(jnp.int32, (256, 256), 0) + lax.broadcasted_iota(jnp.int32, (256, 256), 1) == 255).astype(F32).astype(BF16)
    orders = ((1, 2), (2, 0), (0, 1), (2, 0, 1))
    for z, order in enumerate(orders):
        @pl.when(chip == z)
        def _():
            for dest in order:
                if dest != z:
                    x_to_head(dest).start()

    @pl.when(active)
    def _():
        x_local().start()
        x_to_partner(me, xs.at[:, head], partner).start()

    for h in range(n_heads):
        rel_flip[h] = flip_rows(anti, rels[h]).astype(BF16)

    for z, order in enumerate(orders):
        @pl.when(chip == z)
        def _():
            for dest in order:
                if dest != z:
                    rel_to_head(dest).start()

    @pl.when(active)
    def _():
        rel_local().start()
        rel_to_partner(me, rel_flip.at[head], partner).start()

    dkt[...] = jnp.zeros_like(dkt)
    dvt[...] = jnp.zeros_like(dvt)
    drt[...] = jnp.zeros_like(drt)
    bias_acc[...] = jnp.zeros_like(bias_acc)
    scratch[0][:, :ROWS] = jnp.zeros((ROWS, ROWS), F32)
    relh[pl.ds(seq, COLS), :] = jnp.zeros((COLS, dim), BF16)

    q_ref, k_ref, v_ref, do_ref = (xh.at[a] for a in range(4))
    pieces = ROWS // 256

    def start(owner, local, remote):
        @pl.when(owner == me)
        def _():
            local().start()

        @pl.when(owner != me)
        def _():
            remote().start()

    def finish(owner, local, remote):
        @pl.when(owner != me)
        def _():
            remote().wait_send()

    def tile_copy(i, g):
        piece = tile_index(i, core) * pieces + g
        per = block // 256
        owner = piece // per
        src = o_tiles.at[:, pl.ds(pl.multiple_of(i * ROWS + g * 256, 256), 256), :]
        dst = o_out.at[:, head, pl.ds(pl.multiple_of((piece % per) * 256, 256), 256), :]
        return owner, lambda: pltpu.make_async_copy(src, dst, out_recv), lambda: push(src, dst, tile_send.at[i, g], out_recv, owner)

    def ready_blocks(i):
        return (2 * ROWS * i + block - 1) // block

    @pl.when(active)
    def _():
        @pl.loop(0, n_tiles)
        def _(i):
            @pl.loop(ready_blocks(i), ready_blocks(i + 1))
            def _(dev):
                @pl.when(dev == me)
                def _():
                    x_local().wait()
                    rel_local().wait()

                @pl.when((dev % 2 == core) & (dev != me))
                def _():
                    x_copy(head, dev, xs.at[:, head], in_send.at[0], in_recv.at[dev // 2], partner).wait_recv()
                    rel_copy(head, dev, rel_flip.at[head], in_send.at[0], in_recv.at[dev // 2], partner).wait_recv()
                    x_to_partner(dev, xh.at[:, rows_of(dev), :], partner).start()
                    rel_to_partner(dev, relh.at[flip_rows_of(dev), :], partner).start()

            @pl.loop(ready_blocks(i), ready_blocks(i + 1))
            def _(dev):
                @pl.when(dev % 2 != core)
                def _():
                    x_to_partner(dev, xs.at[:, head], partner).wait_recv()
                    rel_to_partner(dev, rel_flip.at[head], partner).wait_recv()

            tile_grads(tile_index(i, core) * ROWS, i * ROWS, q_ref, k_ref, v_ref, do_ref, relh, bias_ref.at[head], o_tiles.at[0], o_tiles.at[1], dkt, dvt, drt, bias_acc, *scratch)
            for g in range(pieces):
                start(*tile_copy(i, g))

        def acc_cols(a, dev):
            return (dkt, dvt, drt)[a], flip_rows_of(dev) if a == 2 else rows_of(dev)

        def part_copy(a, src_chip, parity):
            acc, cols = acc_cols(a, 2 * src_chip + parity)
            return push(acc.at[:, cols], part.at[a, src_chip], part_send.at[a, src_chip], part_recv.at[a, src_chip], partner)

        def red_copy(a, zi):
            owner = 2 * zi + core
            src, dst = red.at[a, zi], g_out.at[a, head]
            return owner, lambda: pltpu.make_async_copy(src, dst, g_recv), lambda: push(src, dst, red_send.at[a, zi], g_recv, owner)

        def bias_copy(d):
            owner = (me + d) % n_dev
            src, dst = bias_acc, bias_in.at[2 * head + core]
            return owner, lambda: pltpu.make_async_copy(src, dst, bias_recv), lambda: push(src, dst, bias_send.at[d], bias_recv, owner)

        arrays = (2, 0, 1)
        for a in arrays:
            for zi in range(n_chips):
                part_copy(a, zi, 1 - core).start()
        for d in range(n_dev):
            start(*bias_copy(d))
        for a in arrays:
            for zi in range(n_chips):
                part_copy(a, zi, core).wait_recv()
                acc, cols = acc_cols(a, 2 * zi + core)
                total = acc[:, cols] + part[a, zi]
                red[a, zi] = (total if a == 1 else total * scale).astype(BF16)
                start(*red_copy(a, zi))
        for a in arrays:
            for zi in range(n_chips):
                part_copy(a, zi, 1 - core).wait_send()
                finish(*red_copy(a, zi))
        for d in range(n_dev):
            finish(*bias_copy(d))

        @pl.loop(0, n_tiles)
        def _(i):
            for g in range(pieces):
                finish(*tile_copy(i, g))

        @pl.loop(0, n_chips)
        def _(z):
            x_to_partner(2 * z + core, xs.at[:, head], partner).wait_send()
            rel_to_partner(2 * z + core, rel_flip.at[head], partner).wait_send()

    for dest in range(n_heads):
        @pl.when(chip != dest)
        def _():
            x_to_head(dest).wait_send()
            rel_to_head(dest).wait_send()
    pltpu.make_async_copy(bias_in, bias_in, bias_recv).wait()
    for h in range(n_heads):
        bias_out[h] = bias_in[2 * h] + bias_in[2 * h + 1]
    pltpu.make_async_copy(o_out, o_out, out_recv).wait()
    pltpu.make_async_copy(g_out, g_out, g_recv).wait()


def group_call(xs, rels, bias, n_dev):
    n_arr, n_heads, block, dim = xs.shape
    seq = block * n_dev
    n_chips = n_dev // 2
    n_tiles = seq // ROWS // 2
    anyw = pl.BlockSpec(memory_space=pl.ANY)
    vmem = pl.BlockSpec(memory_space=pltpu.VMEM)
    dma = pltpu.SemaphoreType.DMA
    return pl.pallas_call(
        group_kernel,
        name='rel_attention',
        in_specs=[anyw, vmem, vmem],
        out_specs=[anyw, anyw, vmem],
        out_shape=[
            jax.ShapeDtypeStruct((2, n_heads, block, dim), BF16),
            jax.ShapeDtypeStruct((3, n_heads, dim, block), BF16),
            jax.ShapeDtypeStruct((n_heads, 8, dim), F32),
        ],
        scratch_shapes=[
            pltpu.VMEM((n_arr, seq, dim), BF16),
            pltpu.VMEM((seq + COLS, dim), BF16),
            pltpu.VMEM((n_heads, block, dim), BF16),
            pltpu.VMEM((dim, seq), F32),
            pltpu.VMEM((dim, seq), F32),
            pltpu.VMEM((dim, seq + COLS), F32),
            pltpu.VMEM((3, n_chips, dim, block), F32),
            pltpu.VMEM((3, n_chips, dim, block), BF16),
            pltpu.VMEM((2, seq // 2, dim), BF16),
            pltpu.VMEM((8, dim), F32),
            pltpu.VMEM((2 * n_heads, 8, dim), F32),
            pltpu.VMEM((ROWS, seq + ROWS + COLS), F32),
            pltpu.VMEM((ROWS, 128), F32),
            pltpu.VMEM((ROWS, 128), F32),
            pltpu.VMEM((ROWS, dim), F32),
            pltpu.VMEM((ROWS, dim), F32),
            pltpu.VMEM((ROWS, dim), F32),
            dma((n_heads, 2)), dma((n_chips, 2)), dma((n_chips, 2)), dma((n_chips, 2)),
            dma((3, n_chips)), dma((3, n_chips)), dma((n_tiles, ROWS // 256)), dma((3, n_chips)), dma((n_dev,)), dma, dma, dma,
        ],
        compiler_params=pltpu.CompilerParams(vmem_limit_bytes=63 * 2**20, collective_id=0, has_side_effects=True),
    )(xs, rels, bias)


def solution(mesh):
    n_dev = mesh.shape['cp']
    seq_spec = P('cp', 'hp', None)
    head_spec = P('hp', None)
    weight_spec = P(None, 'hp', None)

    def local_fn(q, k, v, u_bias, v_bias, rel_table, w_rel, d_out):
        block, n_heads, dim = q.shape
        rel = jnp.einsum('uo,ojf->juf', rel_table, w_rel, preferred_element_type=F32).astype(BF16)
        xs = jnp.stack([x.transpose(1, 0, 2) for x in (q, k, v, d_out)])
        bias = jnp.pad(jnp.stack([u_bias, v_bias], axis=1), ((0, 0), (0, 6), (0, 0)))
        o, g, d_bias = group_call(xs, rel, bias, n_dev)
        d_rel = g[2][:, :, ::-1]
        d_w_rel = lax.psum(jnp.einsum('uo,jfu->ojf', rel_table, d_rel, preferred_element_type=F32), 'cp')
        return (
            o[0].transpose(1, 0, 2),
            o[1].transpose(1, 0, 2),
            g[0].transpose(2, 0, 1),
            g[1].transpose(2, 0, 1),
            d_bias[:, 0],
            d_bias[:, 1],
            d_w_rel,
        )

    return jax.shard_map(
        local_fn,
        mesh=mesh,
        in_specs=(seq_spec, seq_spec, seq_spec, head_spec, head_spec, P('cp', None), weight_spec, seq_spec),
        out_specs=(seq_spec, seq_spec, seq_spec, seq_spec, head_spec, head_spec, weight_spec),
        check_vma=False,
    )
```

```python
import functools
import math

import jax
import jax.numpy as jnp
from jax import lax
from jax.experimental import pallas as pl
from jax.experimental.pallas import tpu as pltpu
from jax.sharding import PartitionSpec as P

F32, BF16 = jnp.float32, jnp.bfloat16
ROWS = 512
COLS = 512
SUBS = 4
NT = (((1,), (1,)), ((), ()))
NN = (((1,), (0,)), ((), ()))


def mm(a, b, dims=NN, precision=None):
    return lax.dot_general(a, b, dims, preferred_element_type=F32, precision=precision)


def fold_lanes(op, x):
    acc = x[:, :128]
    for g in range(1, x.shape[1] // 128):
        acc = op(acc, x[:, g * 128:(g + 1) * 128])
    return acc


def shear(buf, start, shift):
    out = []
    for g in range(ROWS // 128):
        part = buf[g * 128:(g + 1) * 128, pl.ds(pl.multiple_of(start - (g + 1) * 128, 128), COLS + 128)]
        out.append(pltpu.roll(part, shift, 1, stride=1, stride_axis=0)[:, 128:])
    return jnp.concatenate(out, axis=0)


def flip_rows(anti, x):
    return jnp.concatenate([mm(anti, x[g * 256:(g + 1) * 256]) for g in reversed(range(x.shape[0] // 256))], axis=0)


def tile_grads(q0, out_row, q_ref, k_ref, v_ref, do_ref, rel_ref, bias_ref, o_ref, dq_ref, dkt, dvt, drt, bias_acc, buf, m_ref, l_ref, acc_ref, gu_ref, gv_ref, after_step=None):
    seq, dim = k_ref.shape
    scale = dim ** -0.5
    steps = (q0 + ROWS + COLS - 1) // COLS
    rel0 = seq - ROWS - q0

    def at(base, size):
        return pl.ds(pl.multiple_of(base, 256), size)

    q_wide = q_ref[at(q0, ROWS), :].astype(F32)
    q_u = (q_wide + bias_ref[0:1, :]).astype(BF16)
    q_v = (q_wide + bias_ref[1:2, :]).astype(BF16)

    def offset_scores(c):
        buf[:, at(c * COLS + ROWS, COLS)] = mm(q_v, rel_ref[at(rel0 + c * COLS, COLS), :], NT)

    def scores(c):
        j0 = c * COLS
        return mm(q_u, k_ref[at(j0, COLS), :], NT) + shear(buf, j0 + 2 * ROWS, 1)

    def keep(c, score):
        buf[:, at(c * COLS + ROWS, COLS)] = score
        m_ref[...] = jnp.maximum(m_ref[...], fold_lanes(jnp.maximum, score))

    m_ref[...] = jnp.full_like(m_ref, -jnp.inf)
    offset_scores(0)

    @pl.loop(0, steps - 1)
    def _(c):
        offset_scores(c + 1)
        keep(c, scores(c))

    row_minus_col = lax.broadcasted_iota(jnp.int32, (ROWS, COLS), 0) - lax.broadcasted_iota(jnp.int32, (ROWS, COLS), 1)
    last = steps - 1
    keep(last, jnp.where(row_minus_col >= last * COLS - q0, scores(last), -jnp.inf))

    row_max = jnp.max(m_ref[...], axis=1, keepdims=True)
    l_ref[...] = jnp.zeros_like(l_ref)
    acc_ref[...] = jnp.zeros_like(acc_ref)

    @pl.loop(0, steps)
    def _(c):
        j0 = c * COLS
        prob = jnp.exp2((buf[:, at(j0 + ROWS, COLS)] - row_max) * (scale * math.log2(math.e)))
        buf[:, at(j0 + ROWS, COLS)] = prob
        l_ref[...] += fold_lanes(jnp.add, prob)
        acc_ref[...] += mm(prob.astype(BF16), v_ref[at(j0, COLS), :])

    inv_sum = 1.0 / jnp.sum(l_ref[...], axis=1, keepdims=True)
    out = acc_ref[...] * inv_sum
    o_ref[at(out_row, ROWS), :] = out.astype(BF16)
    d_out = do_ref[at(q0, ROWS), :]
    do_wide = d_out.astype(F32)
    delta = jnp.sum(do_wide * out, axis=1, keepdims=True)
    anti = (lax.broadcasted_iota(jnp.int32, (256, 256), 0) + lax.broadcasted_iota(jnp.int32, (256, 256), 1) == 255)
    anti_b = anti.astype(F32).astype(BF16)
    do_t = do_wide.T.astype(BF16)
    qu_t = q_u.astype(F32).T.astype(BF16)
    qv_rt = flip_rows(anti_b, q_v).T.astype(BF16)
    gu_ref[...] = jnp.zeros_like(gu_ref)
    gv_ref[...] = jnp.zeros_like(gv_ref)

    def by_key(c):
        j0 = c * COLS
        cols = at(j0, COLS)
        prob = buf[:, at(j0 + ROWS, COLS)] * inv_sum
        ds = (prob * (mm(d_out, v_ref[cols, :], NT) - delta)).astype(BF16)
        dvt[:, cols] += mm(do_t, prob.astype(BF16))
        dkt[:, cols] += mm(qu_t, ds)
        gu_ref[...] += mm(ds, k_ref[cols, :])
        buf[:, at(j0 + ROWS, COLS)] = flip_rows(anti_b, ds)

    def by_offset(c):
        c0 = c * COLS
        ds = shear(buf, c0 + ROWS, 0).astype(BF16)
        cols = at(rel0 + c0, COLS)
        gv_ref[...] += mm(ds, rel_ref[cols, :])
        drt[:, cols] += mm(qv_rt, ds)

    by_key(0)

    @pl.loop(1, steps)
    def _(c):
        by_offset(c - 1)
        by_key(c)
        if after_step is not None:
            after_step(c - 1)

    by_offset(steps - 1)
    if after_step is not None:
        @pl.loop(steps - 1, seq // COLS)
        def _(c):
            after_step(c)

    g_u = gu_ref[...]
    g_vr = gv_ref[...]
    anti_f = anti.astype(F32)
    g_v = jnp.concatenate([mm(anti_f, g_vr[g * 256:(g + 1) * 256], precision=lax.Precision.HIGHEST) for g in reversed(range(ROWS // 256))], axis=0)
    dq_ref[at(out_row, ROWS), :] = ((g_u + g_v) * scale).astype(BF16)
    bias_acc[0:1, :] += jnp.sum(g_u, axis=0, keepdims=True) * scale
    bias_acc[1:2, :] += jnp.sum(g_vr, axis=0, keepdims=True) * scale


def tile_index(i, core):
    return 4 * (i // 2) + jnp.where(i % 2 == 0, core, 3 - core)


def group_kernel(xs, rt_hbm, w_hbm, bias_ref, o_out, g_out, bias_out, w_out, xh, relh, rel_flip, rt, w2, dkt, dvt, drt, part, red, o_tiles, bias_acc, bias_in, dr_in, w_part, w_in, rs_in, *rest):
    scratch, sems = rest[:6], rest[6:]
    (in_send, in_recv, fwd_send, fwd_recv, part_send, part_recv, tile_send, red_send, bias_send, out_recv, g_recv, bias_recv, load_sem,
     dr_recv, pair_send, pair_recv, rs_send, rs_recv, ag_send, ag_recv, agp_recv) = sems
    n_arr, n_heads, block, dim = xs.shape
    n_dev = lax.axis_size('cp')
    n_chips = n_dev // 2
    seq = block * n_dev
    n_steps = seq // COLS
    scale = dim ** -0.5
    me = lax.axis_index('cp')
    chip, core = me // 2, me % 2
    head = jnp.minimum(chip, n_heads - 1)
    active = chip < n_heads
    partner = 2 * chip + 1 - core
    n_tiles = seq // ROWS // 2

    load_rt = pltpu.make_async_copy(rt_hbm, rt, load_sem.at[0])
    load_w = pltpu.make_async_copy(w_hbm, w2, load_sem.at[1])
    load_rt.start()
    load_w.start()

    barrier = pltpu.get_barrier_semaphore()
    for d in range(1, n_dev):
        pl.semaphore_signal(barrier, inc=1, device_id={'cp': (me + d) % n_dev}, device_id_type=pl.DeviceIdType.MESH)
    pl.semaphore_wait(barrier, n_dev - 1)

    def push(src, dst, send, recv, dev):
        return pltpu.make_async_remote_copy(src_ref=src, dst_ref=dst, send_sem=send, recv_sem=recv, device_id={'cp': dev}, device_id_type=pl.DeviceIdType.MESH)

    def rows_of(dev):
        return pl.ds(pl.multiple_of(dev * block, block), block)

    def flip_rows_of(dev):
        return pl.ds(pl.multiple_of(seq - block - dev * block, block), block)

    def x_copy(dest, src_dev, src, send, recv, dev):
        return push(src, xh.at[:, rows_of(src_dev), :], send.at[0], recv.at[0], dev)

    def rel_copy(dest, src_dev, src, send, recv, dev):
        return push(src, relh.at[flip_rows_of(src_dev), :], send.at[1], recv.at[1], dev)

    def to_head(make, srcs, dest):
        return make(dest, me, srcs, in_send.at[dest], in_recv.at[chip], 2 * dest + core)

    def x_to_head(dest):
        return to_head(x_copy, xs.at[:, dest], dest)

    def rel_to_head(dest):
        return to_head(rel_copy, rel_flip.at[dest], dest)

    def x_to_partner(dev, src, recv_dev):
        return x_copy(head, dev, src, fwd_send.at[dev // 2], fwd_recv.at[dev // 2], recv_dev)

    def rel_to_partner(dev, src, recv_dev):
        return rel_copy(head, dev, src, fwd_send.at[dev // 2], fwd_recv.at[dev // 2], recv_dev)

    def x_local():
        return pltpu.make_async_copy(xs.at[:, head], xh.at[:, rows_of(me), :], in_recv.at[chip, 0])

    def rel_local():
        return pltpu.make_async_copy(rel_flip.at[head], relh.at[flip_rows_of(me), :], in_recv.at[chip, 1])

    anti = (lax.broadcasted_iota(jnp.int32, (256, 256), 0) + lax.broadcasted_iota(jnp.int32, (256, 256), 1) == 255).astype(F32).astype(BF16)
    orders = ((1, 2), (2, 0), (0, 1), (2, 0, 1))
    for z, order in enumerate(orders):
        @pl.when(chip == z)
        def _():
            for dest in order:
                if dest != z:
                    x_to_head(dest).start()

    @pl.when(active)
    def _():
        x_local().start()
        x_to_partner(me, xs.at[:, head], partner).start()

    load_rt.wait()
    load_w.wait()
    n_groups = block // 256

    @pl.loop(0, n_groups)
    def _(g):
        rows = pl.ds(pl.multiple_of(g * 256, 256), 256)
        flipped = pl.ds(pl.multiple_of((n_groups - 1 - g) * 256, 256), 256)
        rel = mm(anti, mm(rt[rows, :], w2[...]).astype(BF16)).astype(BF16)
        for h in range(n_heads):
            rel_flip[h, flipped, :] = rel[:, h * dim:(h + 1) * dim]

    for z, order in enumerate(orders):
        @pl.when(chip == z)
        def _():
            for dest in order:
                if dest != z:
                    rel_to_head(dest).start()

    @pl.when(active)
    def _():
        rel_local().start()
        rel_to_partner(me, rel_flip.at[head], partner).start()

    dkt[...] = jnp.zeros_like(dkt)
    dvt[...] = jnp.zeros_like(dvt)
    drt[...] = jnp.zeros_like(drt)
    bias_acc[...] = jnp.zeros_like(bias_acc)
    scratch[0][:, :ROWS] = jnp.zeros((ROWS, ROWS), F32)
    relh[pl.ds(seq, COLS), :] = jnp.zeros((COLS, dim), BF16)

    q_ref, k_ref, v_ref, do_ref = (xh.at[a] for a in range(4))
    pieces = ROWS // 256

    def start(owner, local, remote):
        @pl.when(owner == me)
        def _():
            local().start()

        @pl.when(owner != me)
        def _():
            remote().start()

    def finish(owner, local, remote):
        @pl.when(owner != me)
        def _():
            remote().wait_send()

    per = block // 256

    def piece_of(g):
        return pl.ds(pl.multiple_of(g * 256, 256), 256)

    def tile_copy(i, g):
        piece = tile_index(i, core) * pieces + g
        owner = piece // per
        src = o_tiles.at[:, piece_of(i * pieces + g), :]
        dst = o_out.at[:, head, piece_of(piece % per), :]
        return owner, lambda: pltpu.make_async_copy(src, dst, out_recv), lambda: push(src, dst, tile_send.at[i, g], out_recv, owner)

    def ready_blocks(i):
        return (2 * ROWS * i + block - 1) // block

    accs = (dkt, dvt, drt)
    arrays = (2, 0, 1)

    def part_copy(a, c, parity):
        return push(accs[a].at[:, piece_of(2 * c + parity)], part.at[a, c], part_send.at[a, c], part_recv.at[a, c], partner)

    def red_copy(a, c):
        piece = 2 * c + core
        if a == 2:
            owner, dst, recv = n_dev - 1 - piece // per, dr_in.at[head, :, piece_of(piece % per)], dr_recv
        else:
            owner, dst, recv = piece // per, g_out.at[a, head, :, piece_of(piece % per)], g_recv
        src = red.at[a, c]
        return owner, lambda: pltpu.make_async_copy(src, dst, recv), lambda: push(src, dst, red_send.at[a, c], recv, owner)

    def reduce(c):
        for a in arrays:
            part_copy(a, c, core).wait_recv()
            total = accs[a][:, piece_of(2 * c + core)] + part[a, c]
            red[a, c] = (total if a == 1 else total * scale).astype(BF16)
            start(*red_copy(a, c))

    lag = 2

    def after_step(c):
        for a in arrays:
            part_copy(a, c, 1 - core).start()

        @pl.when(c >= lag)
        def _():
            reduce(c - lag)

    def bias_copy(d):
        owner = (me + d) % n_dev
        src, dst = bias_acc, bias_in.at[2 * head + core]
        return owner, lambda: pltpu.make_async_copy(src, dst, bias_recv), lambda: push(src, dst, bias_send.at[d], bias_recv, owner)

    @pl.when(active)
    def _():
        def tile(i, **kw):
            @pl.loop(ready_blocks(i), ready_blocks(i + 1))
            def _(dev):
                @pl.when(dev == me)
                def _():
                    x_local().wait()
                    rel_local().wait()

                @pl.when((dev % 2 == core) & (dev != me))
                def _():
                    x_copy(head, dev, xs.at[:, head], in_send.at[0], in_recv.at[dev // 2], partner).wait_recv()
                    rel_copy(head, dev, rel_flip.at[head], in_send.at[0], in_recv.at[dev // 2], partner).wait_recv()
                    x_to_partner(dev, xh.at[:, rows_of(dev), :], partner).start()
                    rel_to_partner(dev, relh.at[flip_rows_of(dev), :], partner).start()

            @pl.loop(ready_blocks(i), ready_blocks(i + 1))
            def _(dev):
                @pl.when(dev % 2 != core)
                def _():
                    x_to_partner(dev, xs.at[:, head], partner).wait_recv()
                    rel_to_partner(dev, rel_flip.at[head], partner).wait_recv()

            tile_grads(tile_index(i, core) * ROWS, i * ROWS, q_ref, k_ref, v_ref, do_ref, relh, bias_ref.at[head], o_tiles.at[0], o_tiles.at[1], dkt, dvt, drt, bias_acc, *scratch, **kw)
            for g in range(pieces):
                start(*tile_copy(i, g))

        @pl.loop(0, n_tiles - 1)
        def _(i):
            tile(i)

        tile(jnp.int32(n_tiles - 1), after_step=after_step)

        for d in range(n_dev):
            start(*bias_copy(d))

        @pl.loop(n_steps - lag, n_steps)
        def _(c):
            reduce(c)

    half, quarter = w_part.shape[0] // 2, w_part.shape[0] // 2 // n_chips
    sub = quarter // SUBS
    pltpu.make_async_copy(dr_in, dr_in, dr_recv).wait()

    def d_rel_of(h):
        return jnp.concatenate([mm(dr_in[h, :, g * 256:(g + 1) * 256], anti) for g in reversed(range(n_groups))], axis=1).astype(BF16)

    d_rel = jnp.concatenate([d_rel_of(h) for h in range(n_heads)], axis=0)

    def half_rows(c):
        return pl.ds(pl.multiple_of(c * half, half), half)

    def w_rows(c):
        @pl.loop(0, half // 256)
        def _(g):
            rows = pl.ds(pl.multiple_of(c * half + g * 256, 256), 256)
            w_part[rows, :] = lax.dot_general(rt[:, rows], d_rel, (((0,), (1,)), ((), ())), preferred_element_type=F32)

    pair = push(w_part.at[half_rows(1 - core), :], w_in, pair_send, pair_recv, partner)
    w_rows(1 - core)
    pair.start()
    w_rows(core)
    pair.wait_recv()

    def sub_rows(q, s):
        return pl.ds(pl.multiple_of(core * half + q * quarter + s * sub, 8), sub)

    def in_rows(q, s):
        return pl.ds(pl.multiple_of(q * quarter + s * sub, 8), sub)

    def rs_copy(side, q, s):
        dev = 2 * (chip + (1 if side == 0 else -1)) + core
        dev = jnp.clip(dev, 0, n_dev - 1)
        return push(w_part.at[sub_rows(q, s), :], rs_in.at[side, in_rows(q, s), :], rs_send.at[side, q, s], rs_recv.at[side, q, s], dev)

    def ag_copy(way, q, s):
        dev = (2 * (chip + 1) + core, 2 * (chip - 1) + core, partner)[way]
        dev = jnp.clip(dev, 0, n_dev - 1)
        rows = sub_rows(q, s)
        return push(w_out.at[rows, :], w_out.at[rows, :], ag_send.at[way, q, s], agp_recv if way == 2 else ag_recv.at[q, s], dev)

    def flow(side, q, s):
        enters = (chip > 0) if side == 0 else (chip < n_chips - 1)
        rows = sub_rows(q, s)

        @pl.when((chip < q) if side == 0 else (chip > q))
        def _():
            @pl.when(enters)
            def _():
                rs_copy(side, q, s).wait_recv()
                w_part[rows, :] += rs_in[side, in_rows(q, s), :]

            rs_copy(side, q, s).start()

    def spread(q, s):
        @pl.when(chip != q)
        def _():
            ag_copy(0, q, s).wait_recv()

        @pl.when((chip >= q) & (chip < n_chips - 1))
        def _():
            ag_copy(0, q, s).start()

        @pl.when((chip <= q) & (chip > 0))
        def _():
            ag_copy(1, q, s).start()

        ag_copy(2, q, s).start()

    w_part[half_rows(core), :] += w_in[...]

    @pl.loop(0, SUBS)
    def _(s):
        for k in range(n_chips - 1):
            flow(0, n_chips - 1 - k, s)
            flow(1, k, s)
        mine = chip
        rows = sub_rows(mine, s)

        @pl.when(chip > 0)
        def _():
            rs_copy(0, mine, s).wait_recv()
            w_part[rows, :] += rs_in[0, in_rows(mine, s), :]

        @pl.when(chip < n_chips - 1)
        def _():
            rs_copy(1, mine, s).wait_recv()
            w_part[rows, :] += rs_in[1, in_rows(mine, s), :]

        w_out[rows, :] = w_part[rows, :]
        spread(mine, s)

        @pl.when(s > 0)
        def _():
            for d in range(1, n_chips):
                spread((chip + d) % n_chips, s - 1)

    for d in range(1, n_chips):
        spread((chip + d) % n_chips, SUBS - 1)

    pair.wait_send()

    @pl.loop(0, SUBS)
    def _(s):
        for q in range(n_chips):
            for side in range(2):
                @pl.when((chip < q) if side == 0 else (chip > q))
                def _():
                    rs_copy(side, q, s).wait_send()

            @pl.when((chip >= q) & (chip < n_chips - 1))
            def _():
                ag_copy(0, q, s).wait_send()

            @pl.when((chip <= q) & (chip > 0))
            def _():
                ag_copy(1, q, s).wait_send()

            ag_copy(2, q, s).wait_send()

    other = w_out.at[half_rows(1 - core), :]
    pltpu.make_async_copy(other, other, agp_recv).wait()

    @pl.when(active)
    def _():
        @pl.loop(0, n_steps)
        def _(c):
            for a in arrays:
                part_copy(a, c, 1 - core).wait_send()
                finish(*red_copy(a, c))

        for d in range(n_dev):
            finish(*bias_copy(d))

        @pl.loop(0, n_tiles)
        def _(i):
            for g in range(pieces):
                finish(*tile_copy(i, g))

        @pl.loop(0, n_chips)
        def _(z):
            x_to_partner(2 * z + core, xs.at[:, head], partner).wait_send()
            rel_to_partner(2 * z + core, rel_flip.at[head], partner).wait_send()

    for dest in range(n_heads):
        @pl.when(chip != dest)
        def _():
            x_to_head(dest).wait_send()
            rel_to_head(dest).wait_send()
    pltpu.make_async_copy(bias_in, bias_in, bias_recv).wait()
    for h in range(n_heads):
        bias_out[h] = bias_in[2 * h] + bias_in[2 * h + 1]
    pltpu.make_async_copy(o_out, o_out, out_recv).wait()
    pltpu.make_async_copy(g_out, g_out, g_recv).wait()


def group_call(xs, rel_table, w_rel, bias, n_dev):
    n_arr, n_heads, block, dim = xs.shape
    model = rel_table.shape[1]
    seq = block * n_dev
    n_chips = n_dev // 2
    n_tiles = seq // ROWS // 2
    n_steps = seq // COLS
    anyw = pl.BlockSpec(memory_space=pl.ANY)
    vmem = pl.BlockSpec(memory_space=pltpu.VMEM)
    dma = pltpu.SemaphoreType.DMA
    return pl.pallas_call(
        group_kernel,
        name='rel_attention',
        in_specs=[anyw, anyw, anyw, vmem],
        out_specs=[anyw, anyw, vmem, vmem],
        out_shape=[
            jax.ShapeDtypeStruct((2, n_heads, block, dim), BF16),
            jax.ShapeDtypeStruct((2, n_heads, dim, block), BF16),
            jax.ShapeDtypeStruct((n_heads, 8, dim), F32),
            jax.ShapeDtypeStruct((model, n_heads * dim), F32),
        ],
        scratch_shapes=[
            pltpu.VMEM((n_arr, seq, dim), BF16),
            pltpu.VMEM((seq + COLS, dim), BF16),
            pltpu.VMEM((n_heads, block, dim), BF16),
            pltpu.VMEM((block, model), BF16),
            pltpu.VMEM((model, n_heads * dim), BF16),
            pltpu.VMEM((dim, seq), F32),
            pltpu.VMEM((dim, seq), F32),
            pltpu.VMEM((dim, seq + COLS), F32),
            pltpu.VMEM((3, n_steps, dim, 256), F32),
            pltpu.VMEM((3, n_steps, dim, 256), BF16),
            pltpu.VMEM((2, seq // 2, dim), BF16),
            pltpu.VMEM((8, dim), F32),
            pltpu.VMEM((2 * n_heads, 8, dim), F32),
            pltpu.VMEM((n_heads, dim, block), BF16),
            pltpu.VMEM((model, n_heads * dim), F32),
            pltpu.VMEM((model // 2, n_heads * dim), F32),
            pltpu.VMEM((2, model // 2, n_heads * dim), F32),
            pltpu.VMEM((ROWS, seq + ROWS + COLS), F32),
            pltpu.VMEM((ROWS, 128), F32),
            pltpu.VMEM((ROWS, 128), F32),
            pltpu.VMEM((ROWS, dim), F32),
            pltpu.VMEM((ROWS, dim), F32),
            pltpu.VMEM((ROWS, dim), F32),
            dma((n_heads, 2)), dma((n_chips, 2)), dma((n_chips, 2)), dma((n_chips, 2)),
            dma((3, n_steps)), dma((3, n_steps)), dma((n_tiles, ROWS // 256)), dma((3, n_steps)), dma((n_dev,)), dma, dma, dma, dma((2,)),
            dma, dma, dma, dma((2, n_chips, SUBS)), dma((2, n_chips, SUBS)), dma((3, n_chips, SUBS)), dma((n_chips, SUBS)), dma,
        ],
        compiler_params=pltpu.CompilerParams(vmem_limit_bytes=67043328, collective_id=0, has_side_effects=True),
    )(xs, rel_table, w_rel, bias)


def solution(mesh):
    n_dev = mesh.shape['cp']
    seq_spec = P('cp', 'hp', None)
    head_spec = P('hp', None)
    weight_spec = P(None, 'hp', None)

    def local_fn(q, k, v, u_bias, v_bias, rel_table, w_rel, d_out):
        block, n_heads, dim = q.shape
        xs = jnp.stack([x.transpose(1, 0, 2) for x in (q, k, v, d_out)])
        bias = jnp.pad(jnp.stack([u_bias, v_bias], axis=1), ((0, 0), (0, 6), (0, 0)))
        o, g, d_bias, d_w = group_call(xs, rel_table, w_rel.reshape(-1, n_heads * dim), bias, n_dev)
        return (
            o[0].transpose(1, 0, 2),
            o[1].transpose(1, 0, 2),
            g[0].transpose(2, 0, 1),
            g[1].transpose(2, 0, 1),
            d_bias[:, 0],
            d_bias[:, 1],
            d_w.reshape(-1, n_heads, dim),
        )

    return jax.shard_map(
        local_fn,
        mesh=mesh,
        in_specs=(seq_spec, seq_spec, seq_spec, head_spec, head_spec, P('cp', None), weight_spec, seq_spec),
        out_specs=(seq_spec, seq_spec, seq_spec, seq_spec, head_spec, head_spec, weight_spec),
        check_vma=False,
    )
```

```python
import functools
import math

import jax
import jax.numpy as jnp
from jax import lax
from jax.experimental import pallas as pl
from jax.experimental.pallas import tpu as pltpu
from jax.sharding import PartitionSpec as P

F32, BF16 = jnp.float32, jnp.bfloat16
ROWS = 512
COLS = 512
SUBS = 4
NT = (((1,), (1,)), ((), ()))
NN = (((1,), (0,)), ((), ()))


def mm(a, b, dims=NN, precision=None):
    return lax.dot_general(a, b, dims, preferred_element_type=F32, precision=precision)


def fold_lanes(op, x):
    acc = x[:, :128]
    for g in range(1, x.shape[1] // 128):
        acc = op(acc, x[:, g * 128:(g + 1) * 128])
    return acc


def shear(buf, start, shift):
    out = []
    for g in range(ROWS // 128):
        part = buf[g * 128:(g + 1) * 128, pl.ds(pl.multiple_of(start - (g + 1) * 128, 128), COLS + 128)]
        out.append(pltpu.roll(part, shift, 1, stride=1, stride_axis=0)[:, 128:])
    return jnp.concatenate(out, axis=0)


def flip_rows(anti, x):
    return jnp.concatenate([mm(anti, x[g * 256:(g + 1) * 256]) for g in reversed(range(x.shape[0] // 256))], axis=0)


def tile_grads(q0, out_row, q_ref, k_ref, v_ref, do_ref, rel_ref, u_ref, vb_ref, o_ref, dq_ref, dkt, dvt, drt, bias_acc, buf, m_ref, l_ref, acc_ref, gu_ref, gv_ref, after_step=None):
    seq, dim = k_ref.shape
    scale = dim ** -0.5
    steps = (q0 + ROWS + COLS - 1) // COLS
    rel0 = seq - ROWS - q0

    def at(base, size):
        return pl.ds(pl.multiple_of(base, 256), size)

    q_wide = q_ref[at(q0, ROWS), :].astype(F32)
    q_u = (q_wide + u_ref[...]).astype(BF16)
    q_v = (q_wide + vb_ref[...]).astype(BF16)

    def offset_scores(c):
        buf[:, at(c * COLS + ROWS, COLS)] = mm(q_v, rel_ref[at(rel0 + c * COLS, COLS), :], NT)

    def scores(c):
        j0 = c * COLS
        return mm(q_u, k_ref[at(j0, COLS), :], NT) + shear(buf, j0 + 2 * ROWS, 1)

    def keep(c, score):
        buf[:, at(c * COLS + ROWS, COLS)] = score
        m_ref[...] = jnp.maximum(m_ref[...], fold_lanes(jnp.maximum, score))

    m_ref[...] = jnp.full_like(m_ref, -jnp.inf)
    offset_scores(0)

    @pl.loop(0, steps - 1)
    def _(c):
        offset_scores(c + 1)
        keep(c, scores(c))

    row_minus_col = lax.broadcasted_iota(jnp.int32, (ROWS, COLS), 0) - lax.broadcasted_iota(jnp.int32, (ROWS, COLS), 1)
    last = steps - 1
    keep(last, jnp.where(row_minus_col >= last * COLS - q0, scores(last), -jnp.inf))

    row_max = jnp.max(m_ref[...], axis=1, keepdims=True)
    l_ref[...] = jnp.zeros_like(l_ref)
    acc_ref[...] = jnp.zeros_like(acc_ref)

    @pl.loop(0, steps)
    def _(c):
        j0 = c * COLS
        prob = jnp.exp2((buf[:, at(j0 + ROWS, COLS)] - row_max) * (scale * math.log2(math.e)))
        buf[:, at(j0 + ROWS, COLS)] = prob
        l_ref[...] += fold_lanes(jnp.add, prob)
        acc_ref[...] += mm(prob.astype(BF16), v_ref[at(j0, COLS), :])

    inv_sum = 1.0 / jnp.sum(l_ref[...], axis=1, keepdims=True)
    out = acc_ref[...] * inv_sum
    o_ref[at(out_row, ROWS), :] = out.astype(BF16)
    d_out = do_ref[at(q0, ROWS), :]
    do_wide = d_out.astype(F32)
    delta = jnp.sum(do_wide * out, axis=1, keepdims=True)
    anti = (lax.broadcasted_iota(jnp.int32, (256, 256), 0) + lax.broadcasted_iota(jnp.int32, (256, 256), 1) == 255)
    anti_b = anti.astype(F32).astype(BF16)
    do_t = do_wide.T.astype(BF16)
    qu_t = q_u.astype(F32).T.astype(BF16)
    qv_rt = flip_rows(anti_b, q_v).T.astype(BF16)
    gu_ref[...] = jnp.zeros_like(gu_ref)
    gv_ref[...] = jnp.zeros_like(gv_ref)

    def by_key(c):
        j0 = c * COLS
        cols = at(j0, COLS)
        prob = buf[:, at(j0 + ROWS, COLS)] * inv_sum
        ds = (prob * (mm(d_out, v_ref[cols, :], NT) - delta)).astype(BF16)
        dvt[:, cols] += mm(do_t, prob.astype(BF16))
        dkt[:, cols] += mm(qu_t, ds)
        gu_ref[...] += mm(ds, k_ref[cols, :])
        buf[:, at(j0 + ROWS, COLS)] = flip_rows(anti_b, ds)

    def by_offset(c):
        c0 = c * COLS
        ds = shear(buf, c0 + ROWS, 0).astype(BF16)
        cols = at(rel0 + c0, COLS)
        gv_ref[...] += mm(ds, rel_ref[cols, :])
        drt[:, cols] += mm(qv_rt, ds)

    by_key(0)

    @pl.loop(1, steps)
    def _(c):
        by_offset(c - 1)
        by_key(c)
        if after_step is not None:
            after_step(c - 1)

    by_offset(steps - 1)
    if after_step is not None:
        @pl.loop(steps - 1, seq // COLS)
        def _(c):
            after_step(c)

    g_u = gu_ref[...]
    g_vr = gv_ref[...]
    anti_f = anti.astype(F32)
    g_v = jnp.concatenate([mm(anti_f, g_vr[g * 256:(g + 1) * 256], precision=lax.Precision.HIGHEST) for g in reversed(range(ROWS // 256))], axis=0)
    dq_ref[at(out_row, ROWS), :] = ((g_u + g_v) * scale).astype(BF16)
    bias_acc[0:1, :] += jnp.sum(g_u, axis=0, keepdims=True) * scale
    bias_acc[1:2, :] += jnp.sum(g_vr, axis=0, keepdims=True) * scale


def tile_index(i, core):
    return 4 * (i // 2) + jnp.where(i % 2 == 0, core, 3 - core)


def group_kernel(q_hbm, k_hbm, v_hbm, do_hbm, rt_hbm, w_hbm, u_ref, vb_ref, o_out, dq_out, dk_out, dv_out, du_out, dvb_out, w_out, xh, relh, rel_flip, rt, w2, dkt, dvt, drt, part, red, red_r, o_tiles, bias_acc, bias_in, dr_in, w_part, w_in, rs_in, *rest):
    scratch, sems = rest[:6], rest[6:]
    (in_send, in_recv, fwd_send, fwd_recv, part_send, part_recv, tile_send, red_send, bias_send, out_recv, g_recv, bias_recv, load_sem,
     dr_recv, pair_send, pair_recv, rs_send, rs_recv, ag_send, ag_recv, agp_recv) = sems
    inputs = (q_hbm, k_hbm, v_hbm, do_hbm)
    n_heads, block, dim = q_hbm.shape
    n_dev = lax.axis_size('cp')
    n_chips = n_dev // 2
    seq = block * n_dev
    n_steps = seq // COLS
    scale = dim ** -0.5
    me = lax.axis_index('cp')
    chip, core = me // 2, me % 2
    head = jnp.minimum(chip, n_heads - 1)
    active = chip < n_heads
    partner = 2 * chip + 1 - core
    n_tiles = seq // ROWS // 2

    load_rt = pltpu.make_async_copy(rt_hbm, rt, load_sem.at[0])
    loads_w = [pltpu.make_async_copy(w_hbm.at[h], w2.at[:, h * dim:(h + 1) * dim], load_sem.at[1 + h]) for h in range(n_heads)]
    load_rt.start()
    for load_w in loads_w:
        load_w.start()

    barrier = pltpu.get_barrier_semaphore()
    for d in range(1, n_dev):
        pl.semaphore_signal(barrier, inc=1, device_id={'cp': (me + d) % n_dev}, device_id_type=pl.DeviceIdType.MESH)
    pl.semaphore_wait(barrier, n_dev - 1)

    def push(src, dst, send, recv, dev):
        return pltpu.make_async_remote_copy(src_ref=src, dst_ref=dst, send_sem=send, recv_sem=recv, device_id={'cp': dev}, device_id_type=pl.DeviceIdType.MESH)

    def rows_of(dev):
        return pl.ds(pl.multiple_of(dev * block, block), block)

    def flip_rows_of(dev):
        return pl.ds(pl.multiple_of(seq - block - dev * block, block), block)

    def x_copies(src_dev, srcs, send, recv, dev):
        return [push(srcs[a], xh.at[a, rows_of(src_dev), :], send.at[0], recv.at[0], dev) for a in range(4)]

    def x_all(src_dev, send, recv):
        rows = xh.at[:, rows_of(src_dev), :]
        return push(rows, rows, send.at[0], recv.at[0], partner)

    def rel_copy(src_dev, src, send, recv, dev):
        return push(src, relh.at[flip_rows_of(src_dev), :], send.at[1], recv.at[1], dev)

    def x_to_head(dest):
        for copy in x_copies(me, [x.at[dest] for x in inputs], in_send.at[dest], in_recv.at[chip], 2 * dest + core):
            copy.start()

    def rel_to_head(dest):
        return rel_copy(me, rel_flip.at[dest], in_send.at[dest], in_recv.at[chip], 2 * dest + core)

    def x_to_partner(dev, srcs):
        for copy in x_copies(dev, srcs, fwd_send.at[dev // 2], fwd_recv.at[dev // 2], partner):
            copy.start()

    def rel_to_partner(dev, src):
        return rel_copy(dev, src, fwd_send.at[dev // 2], fwd_recv.at[dev // 2], partner)

    def rel_local():
        return pltpu.make_async_copy(rel_flip.at[head], relh.at[flip_rows_of(me), :], in_recv.at[chip, 1])

    anti = (lax.broadcasted_iota(jnp.int32, (256, 256), 0) + lax.broadcasted_iota(jnp.int32, (256, 256), 1) == 255).astype(F32).astype(BF16)
    orders = ((1, 2), (2, 0), (0, 1), (2, 0, 1))
    for z, order in enumerate(orders):
        @pl.when(chip == z)
        def _():
            for dest in order:
                if dest != z:
                    x_to_head(dest)

    @pl.when(active)
    def _():
        for a, x in enumerate(inputs):
            pltpu.make_async_copy(x.at[head], xh.at[a, rows_of(me), :], in_recv.at[chip, 0]).start()
        x_to_partner(me, [x.at[head] for x in inputs])

    load_rt.wait()
    for load_w in loads_w:
        load_w.wait()
    n_groups = block // 256

    @pl.loop(0, n_groups)
    def _(g):
        rows = pl.ds(pl.multiple_of(g * 256, 256), 256)
        flipped = pl.ds(pl.multiple_of((n_groups - 1 - g) * 256, 256), 256)
        rel = mm(anti, mm(rt[rows, :], w2[...]).astype(BF16)).astype(BF16)
        for h in range(n_heads):
            rel_flip[h, flipped, :] = rel[:, h * dim:(h + 1) * dim]

    for z, order in enumerate(orders):
        @pl.when(chip == z)
        def _():
            for dest in order:
                if dest != z:
                    rel_to_head(dest).start()

    @pl.when(active)
    def _():
        rel_local().start()
        rel_to_partner(me, rel_flip.at[head]).start()

    dkt[...] = jnp.zeros_like(dkt)
    dvt[...] = jnp.zeros_like(dvt)
    drt[...] = jnp.zeros_like(drt)
    bias_acc[...] = jnp.zeros_like(bias_acc)
    scratch[0][:, :ROWS] = jnp.zeros((ROWS, ROWS), F32)
    relh[pl.ds(seq, COLS), :] = jnp.zeros((COLS, dim), BF16)

    q_ref, k_ref, v_ref, do_ref = (xh.at[a] for a in range(4))
    pieces = ROWS // 256

    def start(owner, local, remote):
        @pl.when(owner == me)
        def _():
            local().start()

        @pl.when(owner != me)
        def _():
            remote().start()

    def finish(owner, local, remote):
        @pl.when(owner != me)
        def _():
            remote().wait_send()

    per = block // 256

    def piece_of(g):
        return pl.ds(pl.multiple_of(g * 256, 256), 256)

    def tile_copy(i, g, a):
        piece = tile_index(i, core) * pieces + g
        owner = piece // per
        src = o_tiles.at[a, piece_of(i * pieces + g), :]
        dst = (o_out, dq_out)[a].at[head, piece_of(piece % per), :]
        return owner, lambda: pltpu.make_async_copy(src, dst, out_recv.at[a]), lambda: push(src, dst, tile_send.at[i, g, a], out_recv.at[a], owner)

    def ready_blocks(i):
        return (2 * ROWS * i + block - 1) // block

    accs = (dkt, dvt, drt)
    arrays = (2, 0, 1)

    def part_copy(a, c, parity):
        return push(accs[a].at[:, piece_of(2 * c + parity)], part.at[a, c], part_send.at[a, c], part_recv.at[a, c], partner)

    def red_copy(a, c):
        piece = 2 * c + core
        if a == 2:
            src, owner, dst, recv = red_r.at[c], n_dev - 1 - piece // per, dr_in.at[head, :, piece_of(piece % per)], dr_recv
        else:
            src, owner, dst, recv = red.at[a, c], piece // per, (dk_out, dv_out)[a].at[head, piece_of(piece % per), :], g_recv.at[a]
        return owner, lambda: pltpu.make_async_copy(src, dst, recv), lambda: push(src, dst, red_send.at[a, c], recv, owner)

    def reduce(c):
        for a in arrays:
            part_copy(a, c, core).wait_recv()
            total = accs[a][:, piece_of(2 * c + core)] + part[a, c]
            if a == 2:
                red_r[c] = (total * scale).astype(BF16)
            else:
                red[a, c] = (total if a == 1 else total * scale).T.astype(BF16)
            start(*red_copy(a, c))

    lag = 2

    def after_step(c):
        for a in arrays:
            part_copy(a, c, 1 - core).start()

        @pl.when(c >= lag)
        def _():
            reduce(c - lag)

    def bias_copy(d):
        owner = (me + d) % n_dev
        src, dst = bias_acc, bias_in.at[2 * head + core]
        return owner, lambda: pltpu.make_async_copy(src, dst, bias_recv), lambda: push(src, dst, bias_send.at[d], bias_recv, owner)

    @pl.when(active)
    def _():
        def tile(i, **kw):
            with jax.named_scope('wait_ici'):
                @pl.loop(ready_blocks(i), ready_blocks(i + 1))
                def _(dev):
                    @pl.when(dev == me)
                    def _():
                        local = xh.at[:, rows_of(me), :]
                        pltpu.make_async_copy(local, local, in_recv.at[chip, 0]).wait()
                        rel_local().wait()

                    @pl.when((dev % 2 == core) & (dev != me))
                    def _():
                        x_all(dev, in_send.at[0], in_recv.at[dev // 2]).wait_recv()
                        rel_copy(dev, rel_flip.at[head], in_send.at[0], in_recv.at[dev // 2], partner).wait_recv()
                        x_to_partner(dev, [xh.at[a, rows_of(dev), :] for a in range(4)])
                        rel_to_partner(dev, relh.at[flip_rows_of(dev), :]).start()

            with jax.named_scope('wait_core'):
                @pl.loop(ready_blocks(i), ready_blocks(i + 1))
                def _(dev):
                    @pl.when(dev % 2 != core)
                    def _():
                        x_all(dev, fwd_send.at[dev // 2], fwd_recv.at[dev // 2]).wait_recv()
                        rel_to_partner(dev, rel_flip.at[head]).wait_recv()

            tile_grads(tile_index(i, core) * ROWS, i * ROWS, q_ref, k_ref, v_ref, do_ref, relh, u_ref.at[pl.ds(head, 1), :], vb_ref.at[pl.ds(head, 1), :], o_tiles.at[0], o_tiles.at[1], dkt, dvt, drt, bias_acc, *scratch, **kw)
            for g in range(pieces):
                for a in range(2):
                    start(*tile_copy(i, g, a))

        @pl.loop(0, n_tiles - 1)
        def _(i):
            tile(i)

        tile(jnp.int32(n_tiles - 1), after_step=after_step)

        for d in range(n_dev):
            start(*bias_copy(d))

        @pl.loop(n_steps - lag, n_steps)
        def _(c):
            reduce(c)

    half, quarter = w_part.shape[1] // 2, w_part.shape[1] // 2 // n_chips
    sub = quarter // SUBS
    with jax.named_scope('wait_drel'):
        pltpu.make_async_copy(dr_in, dr_in, dr_recv).wait()

    def d_rel_of(h):
        return jnp.concatenate([mm(dr_in[h, :, g * 256:(g + 1) * 256], anti) for g in reversed(range(n_groups))], axis=1).astype(BF16)

    d_rel = jnp.concatenate([d_rel_of(h) for h in range(n_heads)], axis=0)

    def half_rows(c):
        return pl.ds(pl.multiple_of(c * half, half), half)

    def w_rows(c):
        @pl.loop(0, half // 256)
        def _(g):
            rows = pl.ds(pl.multiple_of(c * half + g * 256, 256), 256)
            term = lax.dot_general(rt[:, rows], d_rel, (((0,), (1,)), ((), ())), preferred_element_type=F32)
            for h in range(n_heads):
                w_part[h, rows, :] = term[:, h * dim:(h + 1) * dim]

    pair = push(w_part.at[:, half_rows(1 - core), :], w_in, pair_send, pair_recv, partner)
    with jax.named_scope('w_mm'):
        w_rows(1 - core)
        pair.start()
        w_rows(core)
        pair.wait_recv()
        w_part[:, half_rows(core), :] += w_in[...]

    def sub_rows(q, s):
        return pl.ds(pl.multiple_of(core * half + q * quarter + s * sub, 8), sub)

    def in_rows(q, s):
        return pl.ds(pl.multiple_of(q * quarter + s * sub, 8), sub)

    def rs_copy(side, q, s):
        dev = jnp.clip(2 * (chip + (1 if side == 0 else -1)) + core, 0, n_dev - 1)
        return push(w_part.at[:, sub_rows(q, s), :], rs_in.at[side, :, in_rows(q, s), :], rs_send.at[side, q, s], rs_recv.at[side, q, s], dev)

    def ag_copy(way, q, s):
        dev = jnp.clip((2 * (chip + 1) + core, 2 * (chip - 1) + core, partner)[way], 0, n_dev - 1)
        rows = w_out.at[:, sub_rows(q, s), :]
        return push(rows, rows, ag_send.at[way, q, s], agp_recv if way == 2 else ag_recv.at[q, s], dev)

    def add_in(side, q, s):
        rs_copy(side, q, s).wait_recv()
        rows = sub_rows(q, s)
        w_part[:, rows, :] += rs_in[side, :, in_rows(q, s), :]

    def flow(side, q, s):
        middle = (chip > 0) & (chip < n_chips - 1)

        @pl.when(middle & ((chip < q) if side == 0 else (chip > q)))
        def _():
            add_in(side, q, s)
            rs_copy(side, q, s).start()

    def settle(s):
        @pl.when(chip > 0)
        def _():
            add_in(0, chip, s)

        @pl.when(chip < n_chips - 1)
        def _():
            add_in(1, chip, s)

        rows = sub_rows(chip, s)
        w_out[:, rows, :] = w_part[:, rows, :]
        spread(chip, s)

    def spread(q, s):
        @pl.when(chip != q)
        def _():
            ag_copy(0, q, s).wait_recv()

        @pl.when((chip >= q) & (chip < n_chips - 1))
        def _():
            ag_copy(0, q, s).start()

        @pl.when((chip <= q) & (chip > 0))
        def _():
            ag_copy(1, q, s).start()

        ag_copy(2, q, s).start()

    with jax.named_scope('rs_ag'):
        @pl.when(chip == 0)
        def _():
            for s in range(SUBS):
                for q in reversed(range(1, n_chips)):
                    rs_copy(0, q, s).start()

        @pl.when(chip == n_chips - 1)
        def _():
            for s in range(SUBS):
                for q in range(n_chips - 1):
                    rs_copy(1, q, s).start()

        for s in range(SUBS + 2):
            if s < SUBS:
                for k in range(n_chips - 1):
                    flow(0, n_chips - 1 - k, s)
                    flow(1, k, s)
            if 1 <= s <= SUBS:
                settle(s - 1)
            if s >= 2:
                for d in range(1, n_chips):
                    spread((chip + d) % n_chips, s - 2)

    pair.wait_send()

    @pl.loop(0, SUBS)
    def _(s):
        for q in range(n_chips):
            for side in range(2):
                @pl.when((chip < q) if side == 0 else (chip > q))
                def _():
                    rs_copy(side, q, s).wait_send()

            @pl.when((chip >= q) & (chip < n_chips - 1))
            def _():
                ag_copy(0, q, s).wait_send()

            @pl.when((chip <= q) & (chip > 0))
            def _():
                ag_copy(1, q, s).wait_send()

            ag_copy(2, q, s).wait_send()

    other = w_out.at[:, half_rows(1 - core), :]
    pltpu.make_async_copy(other, other, agp_recv).wait()

    @pl.when(active)
    def _():
        @pl.loop(0, n_steps)
        def _(c):
            for a in arrays:
                part_copy(a, c, 1 - core).wait_send()
                finish(*red_copy(a, c))

        for d in range(n_dev):
            finish(*bias_copy(d))

        @pl.loop(0, n_tiles)
        def _(i):
            for g in range(pieces):
                for a in range(2):
                    finish(*tile_copy(i, g, a))

        @pl.loop(0, n_chips)
        def _(z):
            dev = 2 * z + core
            x_all(dev, fwd_send.at[z], fwd_recv.at[z]).wait_send()
            rel_to_partner(dev, rel_flip.at[head]).wait_send()

    for dest in range(n_heads):
        @pl.when(chip != dest)
        def _():
            x_all(me, in_send.at[dest], in_recv.at[chip]).wait_send()
            rel_to_head(dest).wait_send()
    pltpu.make_async_copy(bias_in, bias_in, bias_recv).wait()
    for h in range(n_heads):
        both = bias_in[2 * h] + bias_in[2 * h + 1]
        du_out[h:h + 1, :] = both[0:1]
        dvb_out[h:h + 1, :] = both[1:2]
    with jax.named_scope('wait_results'):
        for a in range(2):
            pltpu.make_async_copy((o_out, dq_out)[a], (o_out, dq_out)[a], out_recv.at[a]).wait()
            pltpu.make_async_copy((dk_out, dv_out)[a], (dk_out, dv_out)[a], g_recv.at[a]).wait()


def group_call(q, k, v, d_out, rel_table, w_rel, u_bias, v_bias, n_dev):
    n_heads, block, dim = q.shape
    like_q = jax.ShapeDtypeStruct((n_heads, block, dim), BF16)
    like_u = jax.ShapeDtypeStruct((n_heads, dim), F32)
    model = rel_table.shape[1]
    seq = block * n_dev
    n_chips = n_dev // 2
    n_tiles = seq // ROWS // 2
    n_steps = seq // COLS
    anyw = pl.BlockSpec(memory_space=pl.ANY)
    vmem = pl.BlockSpec(memory_space=pltpu.VMEM)
    dma = pltpu.SemaphoreType.DMA
    return pl.pallas_call(
        group_kernel,
        name='rel_attention',
        in_specs=[anyw] * 6 + [vmem] * 2,
        out_specs=[anyw] * 4 + [vmem] * 3,
        out_shape=[like_q] * 4 + [like_u] * 2 + [jax.ShapeDtypeStruct((n_heads, model, dim), F32)],
        scratch_shapes=[
            pltpu.VMEM((4, seq, dim), BF16),
            pltpu.VMEM((seq + COLS, dim), BF16),
            pltpu.VMEM((n_heads, block, dim), BF16),
            pltpu.VMEM((block, model), BF16),
            pltpu.VMEM((model, n_heads * dim), BF16),
            pltpu.VMEM((dim, seq), F32),
            pltpu.VMEM((dim, seq), F32),
            pltpu.VMEM((dim, seq + COLS), F32),
            pltpu.VMEM((3, n_steps, dim, 256), F32),
            pltpu.VMEM((2, n_steps, 256, dim), BF16),
            pltpu.VMEM((n_steps, dim, 256), BF16),
            pltpu.VMEM((2, seq // 2, dim), BF16),
            pltpu.VMEM((8, dim), F32),
            pltpu.VMEM((2 * n_heads, 8, dim), F32),
            pltpu.VMEM((n_heads, dim, block), BF16),
            pltpu.VMEM((n_heads, model, dim), F32),
            pltpu.VMEM((n_heads, model // 2, dim), F32),
            pltpu.VMEM((2, n_heads, model // 2, dim), F32),
            pltpu.VMEM((ROWS, seq + ROWS + COLS), F32),
            pltpu.VMEM((ROWS, 128), F32),
            pltpu.VMEM((ROWS, 128), F32),
            pltpu.VMEM((ROWS, dim), F32),
            pltpu.VMEM((ROWS, dim), F32),
            pltpu.VMEM((ROWS, dim), F32),
            dma((n_heads, 2)), dma((n_chips, 2)), dma((n_chips, 2)), dma((n_chips, 2)),
            dma((3, n_steps)), dma((3, n_steps)), dma((n_tiles, ROWS // 256, 2)), dma((3, n_steps)), dma((n_dev,)), dma((2,)), dma((2,)), dma, dma((1 + n_heads,)),
            dma, dma, dma, dma((2, n_chips, SUBS)), dma((2, n_chips, SUBS)), dma((3, n_chips, SUBS)), dma((n_chips, SUBS)), dma,
        ],
        compiler_params=pltpu.CompilerParams(vmem_limit_bytes=67043328, collective_id=0, has_side_effects=True),
    )(q, k, v, d_out, rel_table, w_rel, u_bias, v_bias)


def solution(mesh):
    n_dev = mesh.shape['cp']
    seq_spec = P('cp', 'hp', None)
    head_spec = P('hp', None)
    weight_spec = P(None, 'hp', None)

    def local_fn(q, k, v, u_bias, v_bias, rel_table, w_rel, d_out):
        swap = lambda x: x.transpose(1, 0, 2)
        *rows, d_u, d_v, d_w = group_call(swap(q), swap(k), swap(v), swap(d_out), rel_table, swap(w_rel), u_bias, v_bias, n_dev)
        return (*(swap(x) for x in rows), d_u, d_v, swap(d_w))

    return jax.shard_map(
        local_fn,
        mesh=mesh,
        in_specs=(seq_spec, seq_spec, seq_spec, head_spec, head_spec, P('cp', None), weight_spec, seq_spec),
        out_specs=(seq_spec, seq_spec, seq_spec, seq_spec, head_spec, head_spec, weight_spec),
        check_vma=False,
    )
```

```python
import functools
import math

import jax
import jax.numpy as jnp
from jax import lax
from jax.experimental import pallas as pl
from jax.experimental.pallas import tpu as pltpu
from jax.sharding import PartitionSpec as P

F32, BF16 = jnp.float32, jnp.bfloat16
ROWS = 512
COLS = 512
SUBS = 4
NT = (((1,), (1,)), ((), ()))
NN = (((1,), (0,)), ((), ()))


def mm(a, b, dims=NN, precision=None):
    return lax.dot_general(a, b, dims, preferred_element_type=F32, precision=precision)


def fold_lanes(op, x):
    acc = x[:, :128]
    for g in range(1, x.shape[1] // 128):
        acc = op(acc, x[:, g * 128:(g + 1) * 128])
    return acc


def shear(buf, start, shift):
    out = []
    for g in range(ROWS // 128):
        part = buf[g * 128:(g + 1) * 128, pl.ds(pl.multiple_of(start - (g + 1) * 128, 128), COLS + 128)]
        out.append(pltpu.roll(part, shift, 1, stride=1, stride_axis=0)[:, 128:])
    return jnp.concatenate(out, axis=0)


def flip_rows(anti, x):
    return jnp.concatenate([mm(anti, x[g * 256:(g + 1) * 256]) for g in reversed(range(x.shape[0] // 256))], axis=0)


def tile_grads(q0, out_row, q_ref, k_ref, v_ref, do_ref, rel_ref, u_ref, vb_ref, o_ref, dq_ref, dkt, dvt, drt, bias_acc, buf, m_ref, l_ref, acc_ref, gu_ref, gv_ref, after_step=None):
    seq, dim = k_ref.shape
    scale = dim ** -0.5
    steps = (q0 + ROWS + COLS - 1) // COLS
    rel0 = seq - ROWS - q0

    def at(base, size):
        return pl.ds(pl.multiple_of(base, 256), size)

    q_wide = q_ref[at(q0, ROWS), :].astype(F32)
    q_u = (q_wide + u_ref[...]).astype(BF16)
    q_v = (q_wide + vb_ref[...]).astype(BF16)

    def offset_scores(c):
        buf[:, at(c * COLS + ROWS, COLS)] = mm(q_v, rel_ref[at(rel0 + c * COLS, COLS), :], NT)

    def scores(c):
        j0 = c * COLS
        return mm(q_u, k_ref[at(j0, COLS), :], NT) + shear(buf, j0 + 2 * ROWS, 1)

    def keep(c, score):
        buf[:, at(c * COLS + ROWS, COLS)] = score
        m_ref[...] = jnp.maximum(m_ref[...], fold_lanes(jnp.maximum, score))

    m_ref[...] = jnp.full_like(m_ref, -jnp.inf)
    offset_scores(0)

    @pl.loop(0, steps - 1)
    def _(c):
        offset_scores(c + 1)
        keep(c, scores(c))

    row_minus_col = lax.broadcasted_iota(jnp.int32, (ROWS, COLS), 0) - lax.broadcasted_iota(jnp.int32, (ROWS, COLS), 1)
    last = steps - 1
    keep(last, jnp.where(row_minus_col >= last * COLS - q0, scores(last), -jnp.inf))

    row_max = jnp.max(m_ref[...], axis=1, keepdims=True)
    l_ref[...] = jnp.zeros_like(l_ref)
    acc_ref[...] = jnp.zeros_like(acc_ref)

    @pl.loop(0, steps)
    def _(c):
        j0 = c * COLS
        prob = jnp.exp2((buf[:, at(j0 + ROWS, COLS)] - row_max) * (scale * math.log2(math.e)))
        buf[:, at(j0 + ROWS, COLS)] = prob
        l_ref[...] += fold_lanes(jnp.add, prob)
        acc_ref[...] += mm(prob.astype(BF16), v_ref[at(j0, COLS), :])

    inv_sum = 1.0 / jnp.sum(l_ref[...], axis=1, keepdims=True)
    out = acc_ref[...] * inv_sum
    o_ref[at(out_row, ROWS), :] = out.astype(BF16)
    d_out = do_ref[at(q0, ROWS), :]
    do_wide = d_out.astype(F32)
    delta = jnp.sum(do_wide * out, axis=1, keepdims=True)
    anti = (lax.broadcasted_iota(jnp.int32, (256, 256), 0) + lax.broadcasted_iota(jnp.int32, (256, 256), 1) == 255)
    anti_b = anti.astype(F32).astype(BF16)
    do_t = do_wide.T.astype(BF16)
    qu_t = q_u.astype(F32).T.astype(BF16)
    qv_rt = flip_rows(anti_b, q_v).T.astype(BF16)
    gu_ref[...] = jnp.zeros_like(gu_ref)
    gv_ref[...] = jnp.zeros_like(gv_ref)

    def by_key(c):
        j0 = c * COLS
        cols = at(j0, COLS)
        prob = buf[:, at(j0 + ROWS, COLS)] * inv_sum
        ds = (prob * (mm(d_out, v_ref[cols, :], NT) - delta)).astype(BF16)
        dvt[:, cols] += mm(do_t, prob.astype(BF16))
        dkt[:, cols] += mm(qu_t, ds)
        gu_ref[...] += mm(ds, k_ref[cols, :])
        buf[:, at(j0 + ROWS, COLS)] = flip_rows(anti_b, ds)

    def by_offset(c):
        c0 = c * COLS
        ds = shear(buf, c0 + ROWS, 0).astype(BF16)
        cols = at(rel0 + c0, COLS)
        gv_ref[...] += mm(ds, rel_ref[cols, :])
        drt[:, cols] += mm(qv_rt, ds)

    by_key(0)

    @pl.loop(1, steps)
    def _(c):
        by_offset(c - 1)
        by_key(c)
        if after_step is not None:
            after_step(c - 1)

    by_offset(steps - 1)
    if after_step is not None:
        @pl.loop(steps - 1, seq // COLS)
        def _(c):
            after_step(c)

    g_u = gu_ref[...]
    g_vr = gv_ref[...]
    anti_f = anti.astype(F32)
    g_v = jnp.concatenate([mm(anti_f, g_vr[g * 256:(g + 1) * 256], precision=lax.Precision.HIGHEST) for g in reversed(range(ROWS // 256))], axis=0)
    dq_ref[at(out_row, ROWS), :] = ((g_u + g_v) * scale).astype(BF16)
    bias_acc[0:1, :] += jnp.sum(g_u, axis=0, keepdims=True) * scale
    bias_acc[1:2, :] += jnp.sum(g_vr, axis=0, keepdims=True) * scale


def tile_index(i, core):
    return 4 * (i // 2) + jnp.where(i % 2 == 0, core, 3 - core)


def group_kernel(q_hbm, k_hbm, v_hbm, do_hbm, rt_hbm, w_hbm, u_ref, vb_ref, o_out, dq_out, dk_out, dv_out, du_out, dvb_out, w_out, xh, relh, rel_flip, rt, w2, dkt, dvt, drt, part, red, red_r, o_tiles, bias_acc, bias_in, dr_in, w_part, w_in, rs_in, *rest):
    scratch, sems = rest[:6], rest[6:]
    (in_send, in_recv, fwd_send, fwd_recv, part_send, part_recv, tile_send, red_send, bias_send, out_recv, g_recv, bias_recv, load_sem,
     dr_recv, pair_send, pair_recv, rs_send, rs_recv, ag_send, ag_recv, agp_recv, go_sem) = sems
    inputs = (q_hbm, k_hbm, v_hbm, do_hbm)
    n_heads, block, dim = q_hbm.shape
    n_dev = lax.axis_size('cp')
    n_chips = n_dev // 2
    seq = block * n_dev
    n_steps = seq // COLS
    scale = dim ** -0.5
    me = lax.axis_index('cp')
    chip, core = me // 2, me % 2
    head = jnp.minimum(chip, n_heads - 1)
    active = chip < n_heads
    partner = 2 * chip + 1 - core
    n_tiles = seq // ROWS // 2

    load_rt = pltpu.make_async_copy(rt_hbm, rt, load_sem.at[0])
    loads_w = [pltpu.make_async_copy(w_hbm.at[h], w2.at[:, h * dim:(h + 1) * dim], load_sem.at[1 + h]) for h in range(n_heads)]
    load_rt.start()
    for load_w in loads_w:
        load_w.start()

    barrier = pltpu.get_barrier_semaphore()
    for d in range(1, n_dev):
        pl.semaphore_signal(barrier, inc=1, device_id={'cp': (me + d) % n_dev}, device_id_type=pl.DeviceIdType.MESH)
    pl.semaphore_wait(barrier, n_dev - 1)

    def push(src, dst, send, recv, dev):
        return pltpu.make_async_remote_copy(src_ref=src, dst_ref=dst, send_sem=send, recv_sem=recv, device_id={'cp': dev}, device_id_type=pl.DeviceIdType.MESH)

    def rows_of(dev):
        return pl.ds(pl.multiple_of(dev * block, block), block)

    def flip_rows_of(dev):
        return pl.ds(pl.multiple_of(seq - block - dev * block, block), block)

    def x_copies(src_dev, srcs, send, recv, dev):
        return [push(srcs[a], xh.at[a, rows_of(src_dev), :], send.at[0], recv.at[0], dev) for a in range(4)]

    def x_all(src_dev, send, recv):
        rows = xh.at[:, rows_of(src_dev), :]
        return push(rows, rows, send.at[0], recv.at[0], partner)

    def rel_copy(src_dev, src, send, recv, dev):
        return push(src, relh.at[flip_rows_of(src_dev), :], send.at[1], recv.at[1], dev)

    def x_to_head(dest):
        for copy in x_copies(me, [x.at[dest] for x in inputs], in_send.at[dest], in_recv.at[chip], 2 * dest + core):
            copy.start()

    def rel_to_head(dest):
        return rel_copy(me, rel_flip.at[dest], in_send.at[dest], in_recv.at[chip], 2 * dest + core)

    def x_to_partner(dev, srcs):
        for copy in x_copies(dev, srcs, fwd_send.at[dev // 2], fwd_recv.at[dev // 2], partner):
            copy.start()

    def rel_to_partner(dev, src):
        return rel_copy(dev, src, fwd_send.at[dev // 2], fwd_recv.at[dev // 2], partner)

    def rel_local():
        return pltpu.make_async_copy(rel_flip.at[head], relh.at[flip_rows_of(me), :], in_recv.at[chip, 1])

    anti = (lax.broadcasted_iota(jnp.int32, (256, 256), 0) + lax.broadcasted_iota(jnp.int32, (256, 256), 1) == 255).astype(F32).astype(BF16)
    orders = ((1, 2), (0, 2), (1, 0), (2, 0, 1))

    def first_to_head():
        for z, order in enumerate(orders):
            @pl.when(chip == z)
            def _():
                x_to_head(order[0])

    def rest_to_head(z, order):
        for dest in order[1:]:
            x_to_head(dest)
            rel_to_head(dest).start()

    first_to_head()

    @pl.when(active)
    def _():
        for a, x in enumerate(inputs):
            pltpu.make_async_copy(x.at[head], xh.at[a, rows_of(me), :], in_recv.at[chip, 0]).start()
        x_to_partner(me, [x.at[head] for x in inputs])

    load_rt.wait()
    for load_w in loads_w:
        load_w.wait()
    n_groups = block // 256

    @pl.loop(0, n_groups)
    def _(g):
        rows = pl.ds(pl.multiple_of(g * 256, 256), 256)
        flipped = pl.ds(pl.multiple_of((n_groups - 1 - g) * 256, 256), 256)
        rel = mm(anti, mm(rt[rows, :], w2[...]).astype(BF16)).astype(BF16)
        for h in range(n_heads):
            rel_flip[h, flipped, :] = rel[:, h * dim:(h + 1) * dim]

    for z, order in enumerate(orders):
        @pl.when(chip == z)
        def _():
            rel_to_head(order[0]).start()
            if z < n_chips - 1:
                rest_to_head(z, order)

    @pl.when(active)
    def _():
        rel_local().start()
        rel_to_partner(me, rel_flip.at[head]).start()

    dkt[...] = jnp.zeros_like(dkt)
    dvt[...] = jnp.zeros_like(dvt)
    drt[...] = jnp.zeros_like(drt)
    bias_acc[...] = jnp.zeros_like(bias_acc)
    scratch[0][:, :ROWS] = jnp.zeros((ROWS, ROWS), F32)
    relh[pl.ds(seq, COLS), :] = jnp.zeros((COLS, dim), BF16)

    def sent_to_head(dest):
        x_all(me, in_send.at[dest], in_recv.at[chip]).wait_send()
        rel_to_head(dest).wait_send()

    @pl.when(chip == n_chips - 2)
    def _():
        for dest in orders[n_chips - 2]:
            sent_to_head(dest)
        pl.semaphore_signal(go_sem, inc=1, device_id={'cp': jnp.minimum(me + 2, n_dev - 1)}, device_id_type=pl.DeviceIdType.MESH)

    @pl.when(chip == n_chips - 1)
    def _():
        pl.semaphore_wait(go_sem, 1)
        rest_to_head(n_chips - 1, orders[n_chips - 1])

    q_ref, k_ref, v_ref, do_ref = (xh.at[a] for a in range(4))
    pieces = ROWS // 256

    def start(owner, local, remote):
        @pl.when(owner == me)
        def _():
            local().start()

        @pl.when(owner != me)
        def _():
            remote().start()

    def finish(owner, local, remote):
        @pl.when(owner != me)
        def _():
            remote().wait_send()

    per = block // 256

    def piece_of(g):
        return pl.ds(pl.multiple_of(g * 256, 256), 256)

    def tile_copy(i, g, a):
        piece = tile_index(i, core) * pieces + g
        owner = piece // per
        src = o_tiles.at[a, piece_of(i * pieces + g), :]
        dst = (o_out, dq_out)[a].at[head, piece_of(piece % per), :]
        return owner, lambda: pltpu.make_async_copy(src, dst, out_recv.at[a]), lambda: push(src, dst, tile_send.at[i, g, a], out_recv.at[a], owner)

    def ready_blocks(i):
        return (2 * ROWS * i + block - 1) // block

    accs = (dkt, dvt, drt)
    arrays = (2, 0, 1)

    def part_copy(a, c, parity):
        return push(accs[a].at[:, piece_of(2 * c + parity)], part.at[a, c], part_send.at[a, c], part_recv.at[a, c], partner)

    def red_copy(a, c):
        piece = 2 * c + core
        if a == 2:
            src, owner, dst, recv = red_r.at[c], n_dev - 1 - piece // per, dr_in.at[head, :, piece_of(piece % per)], dr_recv
        else:
            src, owner, dst, recv = red.at[a, c], piece // per, (dk_out, dv_out)[a].at[head, piece_of(piece % per), :], g_recv.at[a]
        return owner, lambda: pltpu.make_async_copy(src, dst, recv), lambda: push(src, dst, red_send.at[a, c], recv, owner)

    def reduce(c):
        for a in arrays:
            part_copy(a, c, core).wait_recv()
            total = accs[a][:, piece_of(2 * c + core)] + part[a, c]
            if a == 2:
                red_r[c] = (total * scale).astype(BF16)
            else:
                red[a, c] = (total if a == 1 else total * scale).T.astype(BF16)
            start(*red_copy(a, c))

    lag = 2

    def after_step(c):
        for a in arrays:
            part_copy(a, c, 1 - core).start()

        @pl.when(c >= lag)
        def _():
            reduce(c - lag)

    def bias_copy(d):
        owner = (me + d) % n_dev
        src, dst = bias_acc, bias_in.at[2 * head + core]
        return owner, lambda: pltpu.make_async_copy(src, dst, bias_recv), lambda: push(src, dst, bias_send.at[d], bias_recv, owner)

    @pl.when(active)
    def _():
        def tile(i, **kw):
            with jax.named_scope('wait_ici'):
                @pl.loop(ready_blocks(i), ready_blocks(i + 1))
                def _(dev):
                    @pl.when(dev == me)
                    def _():
                        local = xh.at[:, rows_of(me), :]
                        pltpu.make_async_copy(local, local, in_recv.at[chip, 0]).wait()
                        rel_local().wait()

                    @pl.when((dev % 2 == core) & (dev != me))
                    def _():
                        x_all(dev, in_send.at[0], in_recv.at[dev // 2]).wait_recv()
                        rel_copy(dev, rel_flip.at[head], in_send.at[0], in_recv.at[dev // 2], partner).wait_recv()
                        x_to_partner(dev, [xh.at[a, rows_of(dev), :] for a in range(4)])
                        rel_to_partner(dev, relh.at[flip_rows_of(dev), :]).start()

            with jax.named_scope('wait_core'):
                @pl.loop(ready_blocks(i), ready_blocks(i + 1))
                def _(dev):
                    @pl.when(dev % 2 != core)
                    def _():
                        x_all(dev, fwd_send.at[dev // 2], fwd_recv.at[dev // 2]).wait_recv()
                        rel_to_partner(dev, rel_flip.at[head]).wait_recv()

            tile_grads(tile_index(i, core) * ROWS, i * ROWS, q_ref, k_ref, v_ref, do_ref, relh, u_ref.at[pl.ds(head, 1), :], vb_ref.at[pl.ds(head, 1), :], o_tiles.at[0], o_tiles.at[1], dkt, dvt, drt, bias_acc, *scratch, **kw)
            for g in range(pieces):
                for a in range(2):
                    start(*tile_copy(i, g, a))

        @pl.loop(0, n_tiles - 1)
        def _(i):
            tile(i)

        tile(jnp.int32(n_tiles - 1), after_step=after_step)

        for d in range(n_dev):
            start(*bias_copy(d))

        @pl.loop(n_steps - lag, n_steps)
        def _(c):
            reduce(c)

    half, quarter = w_part.shape[1] // 2, w_part.shape[1] // 2 // n_chips
    sub = quarter // SUBS
    with jax.named_scope('wait_drel'):
        pltpu.make_async_copy(dr_in, dr_in, dr_recv).wait()

    def d_rel_of(h):
        return jnp.concatenate([mm(dr_in[h, :, g * 256:(g + 1) * 256], anti) for g in reversed(range(n_groups))], axis=1).astype(BF16)

    d_rel = jnp.concatenate([d_rel_of(h) for h in range(n_heads)], axis=0)

    def half_rows(c):
        return pl.ds(pl.multiple_of(c * half, half), half)

    def w_rows(c):
        @pl.loop(0, half // 256)
        def _(g):
            rows = pl.ds(pl.multiple_of(c * half + g * 256, 256), 256)
            term = lax.dot_general(rt[:, rows], d_rel, (((0,), (1,)), ((), ())), preferred_element_type=F32)
            for h in range(n_heads):
                w_part[h, rows, :] = term[:, h * dim:(h + 1) * dim]

    pair = push(w_part.at[:, half_rows(1 - core), :], w_in, pair_send, pair_recv, partner)
    with jax.named_scope('w_mm'):
        w_rows(1 - core)
        pair.start()
        w_rows(core)
        pair.wait_recv()
        w_part[:, half_rows(core), :] += w_in[...]

    def sub_rows(q, s):
        return pl.ds(pl.multiple_of(core * half + q * quarter + s * sub, 8), sub)

    side = chip // 2
    mate = chip + 1 - 2 * (chip % 2)
    inner = (chip > 0) & (chip < n_chips - 1)
    far_pair = 2 * (1 - side)
    gate = 2 - side

    def in_rows(s):
        return pl.ds(pl.multiple_of(s * sub, 8), sub)

    def rs_copy(q, slot, s, to):
        return push(w_part.at[:, sub_rows(q, s), :], rs_in.at[slot, :, in_rows(s), :], rs_send.at[slot, s], rs_recv.at[slot, s], 2 * to + core)

    def ag_copy(way, q, s):
        rows = w_out.at[:, sub_rows(q, s), :]
        return push(rows, rows, ag_send.at[way, q, s], agp_recv if way == 2 else ag_recv.at[q, s], (2 * mate + core, 2 * gate + core, partner)[way])

    def add_in(q, slot, s):
        rs_copy(q, slot, s, mate).wait_recv()
        rows = sub_rows(q, s)
        w_part[:, rows, :] += rs_in[slot, :, in_rows(s), :]

    def every_part(body):
        for s in range(SUBS):
            body(s)

    @every_part
    def _(s):
        @pl.when(jnp.logical_not(inner))
        def _():
            for f in range(2):
                rs_copy(far_pair + f, 2 + f, s, mate).start()

        rs_copy(mate, 0, s, mate).start()

    @pl.when(inner)
    def _():
        @every_part
        def _(s):
            for f in range(2):
                add_in(far_pair + f, 2 + f, s)
                push(w_part.at[:, sub_rows(far_pair + f, s), :], rs_in.at[1, :, in_rows(s), :], rs_send.at[2 + f, s], rs_recv.at[1, s], 2 * (far_pair + f) + core).start()

    @every_part
    def _(s):
        add_in(chip, 0, s)
        add_in(chip, 1, s)
        rows = sub_rows(chip, s)
        w_out[:, rows, :] = w_part[:, rows, :]
        for way in range(3):
            ag_copy(way, chip, s).start()

    @every_part
    def _(s):
        ag_copy(0, mate, s).wait_recv()
        ag_copy(2, mate, s).start()
        for f in range(2):
            ag_copy(0, far_pair + f, s).wait_recv()

            @pl.when(inner)
            def _():
                ag_copy(0, far_pair + f, s).start()

            ag_copy(2, far_pair + f, s).start()

    pair.wait_send()

    @pl.loop(0, SUBS)
    def _(s):
        rs_copy(mate, 0, s, mate).wait_send()
        for f in range(2):
            rs_copy(far_pair + f, 2 + f, s, mate).wait_send()

            @pl.when(inner)
            def _():
                ag_copy(0, far_pair + f, s).wait_send()

            ag_copy(2, far_pair + f, s).wait_send()
        ag_copy(2, mate, s).wait_send()
        for way in range(3):
            ag_copy(way, chip, s).wait_send()

    other = w_out.at[:, half_rows(1 - core), :]
    pltpu.make_async_copy(other, other, agp_recv).wait()

    @pl.when(active)
    def _():
        @pl.loop(0, n_steps)
        def _(c):
            for a in arrays:
                part_copy(a, c, 1 - core).wait_send()
                finish(*red_copy(a, c))

        for d in range(n_dev):
            finish(*bias_copy(d))

        @pl.loop(0, n_tiles)
        def _(i):
            for g in range(pieces):
                for a in range(2):
                    finish(*tile_copy(i, g, a))

        @pl.loop(0, n_chips)
        def _(z):
            dev = 2 * z + core
            x_all(dev, fwd_send.at[z], fwd_recv.at[z]).wait_send()
            rel_to_partner(dev, rel_flip.at[head]).wait_send()

    for dest in range(n_heads):
        @pl.when((chip != dest) & (chip != n_chips - 2))
        def _():
            sent_to_head(dest)
    pltpu.make_async_copy(bias_in, bias_in, bias_recv).wait()
    for h in range(n_heads):
        both = bias_in[2 * h] + bias_in[2 * h + 1]
        du_out[h:h + 1, :] = both[0:1]
        dvb_out[h:h + 1, :] = both[1:2]
    with jax.named_scope('wait_results'):
        for a in range(2):
            pltpu.make_async_copy((o_out, dq_out)[a], (o_out, dq_out)[a], out_recv.at[a]).wait()
            pltpu.make_async_copy((dk_out, dv_out)[a], (dk_out, dv_out)[a], g_recv.at[a]).wait()


def group_call(q, k, v, d_out, rel_table, w_rel, u_bias, v_bias, n_dev):
    n_heads, block, dim = q.shape
    like_q = jax.ShapeDtypeStruct((n_heads, block, dim), BF16)
    like_u = jax.ShapeDtypeStruct((n_heads, dim), F32)
    model = rel_table.shape[1]
    seq = block * n_dev
    n_chips = n_dev // 2
    n_tiles = seq // ROWS // 2
    n_steps = seq // COLS
    anyw = pl.BlockSpec(memory_space=pl.ANY)
    vmem = pl.BlockSpec(memory_space=pltpu.VMEM)
    dma = pltpu.SemaphoreType.DMA
    return pl.pallas_call(
        group_kernel,
        name='rel_attention',
        in_specs=[anyw] * 6 + [vmem] * 2,
        out_specs=[anyw] * 4 + [vmem] * 3,
        out_shape=[like_q] * 4 + [like_u] * 2 + [jax.ShapeDtypeStruct((n_heads, model, dim), F32)],
        scratch_shapes=[
            pltpu.VMEM((4, seq, dim), BF16),
            pltpu.VMEM((seq + COLS, dim), BF16),
            pltpu.VMEM((n_heads, block, dim), BF16),
            pltpu.VMEM((block, model), BF16),
            pltpu.VMEM((model, n_heads * dim), BF16),
            pltpu.VMEM((dim, seq), F32),
            pltpu.VMEM((dim, seq), F32),
            pltpu.VMEM((dim, seq + COLS), F32),
            pltpu.VMEM((3, n_steps, dim, 256), F32),
            pltpu.VMEM((2, n_steps, 256, dim), BF16),
            pltpu.VMEM((n_steps, dim, 256), BF16),
            pltpu.VMEM((2, seq // 2, dim), BF16),
            pltpu.VMEM((8, dim), F32),
            pltpu.VMEM((2 * n_heads, 8, dim), F32),
            pltpu.VMEM((n_heads, dim, block), BF16),
            pltpu.VMEM((n_heads, model, dim), F32),
            pltpu.VMEM((n_heads, model // 2, dim), F32),
            pltpu.VMEM((4, n_heads, model // 2 // n_chips, dim), F32),
            pltpu.VMEM((ROWS, seq + ROWS + COLS), F32),
            pltpu.VMEM((ROWS, 128), F32),
            pltpu.VMEM((ROWS, 128), F32),
            pltpu.VMEM((ROWS, dim), F32),
            pltpu.VMEM((ROWS, dim), F32),
            pltpu.VMEM((ROWS, dim), F32),
            dma((n_heads, 2)), dma((n_chips, 2)), dma((n_chips, 2)), dma((n_chips, 2)),
            dma((3, n_steps)), dma((3, n_steps)), dma((n_tiles, ROWS // 256, 2)), dma((3, n_steps)), dma((n_dev,)), dma((2,)), dma((2,)), dma, dma((1 + n_heads,)),
            dma, dma, dma, dma((4, SUBS)), dma((4, SUBS)), dma((3, n_chips, SUBS)), dma((n_chips, SUBS)), dma, pltpu.SemaphoreType.REGULAR,
        ],
        compiler_params=pltpu.CompilerParams(vmem_limit_bytes=67043328, collective_id=0, has_side_effects=True),
    )(q, k, v, d_out, rel_table, w_rel, u_bias, v_bias)


def solution(mesh):
    n_dev = mesh.shape['cp']
    seq_spec = P('cp', 'hp', None)
    head_spec = P('hp', None)
    weight_spec = P(None, 'hp', None)

    def local_fn(q, k, v, u_bias, v_bias, rel_table, w_rel, d_out):
        swap = lambda x: x.transpose(1, 0, 2)
        *rows, d_u, d_v, d_w = group_call(swap(q), swap(k), swap(v), swap(d_out), rel_table, swap(w_rel), u_bias, v_bias, n_dev)
        return (*(swap(x) for x in rows), d_u, d_v, swap(d_w))

    return jax.shard_map(
        local_fn,
        mesh=mesh,
        in_specs=(seq_spec, seq_spec, seq_spec, head_spec, head_spec, P('cp', None), weight_spec, seq_spec),
        out_specs=(seq_spec, seq_spec, seq_spec, seq_spec, head_spec, head_spec, weight_spec),
        check_vma=False,
    )
```

```python
import functools
import math

import jax
import jax.numpy as jnp
from jax import lax
from jax.experimental import pallas as pl
from jax.experimental.pallas import tpu as pltpu
from jax.sharding import PartitionSpec as P

F32, BF16 = jnp.float32, jnp.bfloat16
ROWS = 512
COLS = 512
SUBS = 4
NT = (((1,), (1,)), ((), ()))
NN = (((1,), (0,)), ((), ()))


def mm(a, b, dims=NN, precision=None):
    return lax.dot_general(a, b, dims, preferred_element_type=F32, precision=precision)


def fold_lanes(op, x):
    acc = x[:, :128]
    for g in range(1, x.shape[1] // 128):
        acc = op(acc, x[:, g * 128:(g + 1) * 128])
    return acc


def shear(buf, start, shift):
    out = []
    for g in range(ROWS // 128):
        part = buf[g * 128:(g + 1) * 128, pl.ds(pl.multiple_of(start - (g + 1) * 128, 128), COLS + 128)]
        out.append(pltpu.roll(part, shift, 1, stride=1, stride_axis=0)[:, 128:])
    return jnp.concatenate(out, axis=0)


def flip_rows(anti, x):
    return jnp.concatenate([mm(anti, x[g * 256:(g + 1) * 256]) for g in reversed(range(x.shape[0] // 256))], axis=0)


def flip_eights(x):
    back = 7 - lax.broadcasted_iota(jnp.int32, (8, 128), 0)
    rows = []
    for r in range(0, x.shape[0], 8):
        rows.append(jnp.concatenate([jnp.take_along_axis(x[r:r + 8, c:c + 128], back, axis=0, mode='promise_in_bounds') for c in range(0, x.shape[1], 128)], axis=1))
    return jnp.concatenate(rows, axis=0)


def shear_back(buf, start):
    out = []
    for g in range(ROWS // 8):
        left = ROWS - 8 - 8 * g
        base = start - 128 * (left // 128 + 1)
        part = flip_eights(buf[8 * g:8 * g + 8, pl.ds(pl.multiple_of(base, 128), COLS + 128)])
        out.append(pltpu.roll(part, left % 128, 1, stride=1, stride_axis=0)[:, 128:])
    return jnp.concatenate(out, axis=0)


def tile_grads(q0, out_row, q_ref, k_ref, v_ref, do_ref, rel_ref, u_ref, vb_ref, o_ref, dq_ref, dkt, dvt, drt, bias_acc, buf, m_ref, l_ref, acc_ref, gu_ref, gv_ref, after_step=None):
    seq, dim = k_ref.shape
    scale = dim ** -0.5
    steps = (q0 + ROWS + COLS - 1) // COLS
    rel0 = seq - ROWS - q0

    def at(base, size):
        return pl.ds(pl.multiple_of(base, 256), size)

    q_wide = q_ref[at(q0, ROWS), :].astype(F32)
    q_u = (q_wide + u_ref[...]).astype(BF16)
    q_v = (q_wide + vb_ref[...]).astype(BF16)

    def offset_scores(c):
        buf[:, at(c * COLS + ROWS, COLS)] = mm(q_v, rel_ref[at(rel0 + c * COLS, COLS), :], NT)

    def scores(c):
        j0 = c * COLS
        return mm(q_u, k_ref[at(j0, COLS), :], NT) + shear(buf, j0 + 2 * ROWS, 1)

    def keep(c, score):
        buf[:, at(c * COLS + ROWS, COLS)] = score
        m_ref[...] = jnp.maximum(m_ref[...], fold_lanes(jnp.maximum, score))

    m_ref[...] = jnp.full_like(m_ref, -jnp.inf)
    offset_scores(0)
    offset_scores(1)

    @pl.loop(0, steps - 1)
    def _(c):
        keep(c, scores(c))
        offset_scores(c + 2)

    row_minus_col = lax.broadcasted_iota(jnp.int32, (ROWS, COLS), 0) - lax.broadcasted_iota(jnp.int32, (ROWS, COLS), 1)
    last = steps - 1
    keep(last, jnp.where(row_minus_col >= last * COLS - q0, scores(last), -jnp.inf))

    row_max = jnp.max(m_ref[...], axis=1, keepdims=True)
    l_ref[...] = jnp.zeros_like(l_ref)
    acc_ref[...] = jnp.zeros_like(acc_ref)

    @pl.loop(0, steps)
    def _(c):
        j0 = c * COLS
        prob = jnp.exp2((buf[:, at(j0 + ROWS, COLS)] - row_max) * (scale * math.log2(math.e)))
        buf[:, at(j0 + ROWS, COLS)] = prob
        l_ref[...] += fold_lanes(jnp.add, prob)
        acc_ref[...] += mm(prob.astype(BF16), v_ref[at(j0, COLS), :])

    inv_sum = 1.0 / jnp.sum(l_ref[...], axis=1, keepdims=True)
    out = acc_ref[...] * inv_sum
    o_ref[at(out_row, ROWS), :] = out.astype(BF16)
    d_out = do_ref[at(q0, ROWS), :]
    do_wide = d_out.astype(F32)
    delta = jnp.sum(do_wide * out, axis=1, keepdims=True)
    do_t = do_wide.T.astype(BF16)
    qu_t = q_u.astype(F32).T.astype(BF16)
    qv_rt = flip_eights(q_v.astype(F32)).T.astype(BF16)
    gu_ref[...] = jnp.zeros_like(gu_ref)
    gv_ref[...] = jnp.zeros_like(gv_ref)

    def by_key(c):
        j0 = c * COLS
        cols = at(j0, COLS)
        prob = buf[:, at(j0 + ROWS, COLS)] * inv_sum
        ds_wide = prob * (mm(d_out, v_ref[cols, :], NT) - delta)
        ds = ds_wide.astype(BF16)
        dvt[:, cols] += mm(do_t, prob.astype(BF16))
        dkt[:, cols] += mm(qu_t, ds)
        gu_ref[...] += mm(ds, k_ref[cols, :])
        buf[:, at(j0 + ROWS, COLS)] = ds_wide

    def by_offset(c):
        c0 = c * COLS
        ds = shear_back(buf, c0 + ROWS).astype(BF16)
        cols = at(rel0 + c0, COLS)
        gv_ref[...] += mm(ds, rel_ref[cols, :])
        drt[:, cols] += mm(qv_rt, ds)

    by_key(0)

    @pl.loop(1, steps)
    def _(c):
        by_offset(c - 1)
        by_key(c)
        if after_step is not None:
            after_step(c - 1)

    by_offset(steps - 1)
    if after_step is not None:
        @pl.loop(steps - 1, seq // COLS)
        def _(c):
            after_step(c)

    g_u = gu_ref[...]
    g_vr = gv_ref[...]
    g_v = flip_eights(g_vr)
    dq_ref[at(out_row, ROWS), :] = ((g_u + g_v) * scale).astype(BF16)
    bias_acc[0:1, :] += jnp.sum(g_u, axis=0, keepdims=True) * scale
    bias_acc[1:2, :] += jnp.sum(g_vr, axis=0, keepdims=True) * scale


def tile_index(i, core):
    return 4 * (i // 2) + jnp.where(i % 2 == 0, core, 3 - core)


def group_kernel(q_hbm, k_hbm, v_hbm, do_hbm, rt_hbm, w_hbm, u_ref, vb_ref, o_out, dq_out, dk_out, dv_out, du_out, dvb_out, w_out, xh, relh, rel_flip, rt, w2, dkt, dvt, drt, part, red, red_r, o_tiles, bias_acc, bias_in, dr_in, w_part, w_in, rs_in, *rest):
    scratch, sems = rest[:6], rest[6:]
    (in_send, in_recv, fwd_send, fwd_recv, part_send, part_recv, tile_send, red_send, bias_send, out_recv, g_recv, bias_recv, load_sem,
     dr_recv, pair_send, pair_recv, rs_send, rs_recv, ag_send, ag_recv, agp_recv, go_sem) = sems
    inputs = (q_hbm, k_hbm, v_hbm, do_hbm)
    n_heads, block, dim = q_hbm.shape
    n_dev = lax.axis_size('cp')
    n_chips = n_dev // 2
    seq = block * n_dev
    n_steps = seq // COLS
    scale = dim ** -0.5
    me = lax.axis_index('cp')
    chip, core = me // 2, me % 2
    head = jnp.minimum(chip, n_heads - 1)
    active = chip < n_heads
    partner = 2 * chip + 1 - core
    n_tiles = seq // ROWS // 2

    load_rt = pltpu.make_async_copy(rt_hbm, rt, load_sem.at[0])
    loads_w = [pltpu.make_async_copy(w_hbm.at[h], w2.at[:, h * dim:(h + 1) * dim], load_sem.at[1 + h]) for h in range(n_heads)]
    load_rt.start()
    for load_w in loads_w:
        load_w.start()

    barrier = pltpu.get_barrier_semaphore()
    for d in range(1, n_dev):
        pl.semaphore_signal(barrier, inc=1, device_id={'cp': (me + d) % n_dev}, device_id_type=pl.DeviceIdType.MESH)
    pl.semaphore_wait(barrier, n_dev - 1)

    def push(src, dst, send, recv, dev):
        return pltpu.make_async_remote_copy(src_ref=src, dst_ref=dst, send_sem=send, recv_sem=recv, device_id={'cp': dev}, device_id_type=pl.DeviceIdType.MESH)

    def rows_of(dev):
        return pl.ds(pl.multiple_of(dev * block, block), block)

    def flip_rows_of(dev):
        return pl.ds(pl.multiple_of(seq - block - dev * block, block), block)

    def x_copies(src_dev, srcs, send, recv, dev):
        return [push(srcs[a], xh.at[a, rows_of(src_dev), :], send.at[0], recv.at[0], dev) for a in range(4)]

    def x_all(src_dev, send, recv):
        rows = xh.at[:, rows_of(src_dev), :]
        return push(rows, rows, send.at[0], recv.at[0], partner)

    def rel_copy(src_dev, src, send, recv, dev):
        return push(src, relh.at[flip_rows_of(src_dev), :], send.at[1], recv.at[1], dev)

    def x_to_head(dest):
        for copy in x_copies(me, [x.at[dest] for x in inputs], in_send.at[dest], in_recv.at[chip], 2 * dest + core):
            copy.start()

    def rel_to_head(dest):
        return rel_copy(me, rel_flip.at[dest], in_send.at[dest], in_recv.at[chip], 2 * dest + core)

    def x_to_partner(dev, srcs):
        for copy in x_copies(dev, srcs, fwd_send.at[dev // 2], fwd_recv.at[dev // 2], partner):
            copy.start()

    def rel_to_partner(dev, src):
        return rel_copy(dev, src, fwd_send.at[dev // 2], fwd_recv.at[dev // 2], partner)

    def rel_local():
        return pltpu.make_async_copy(rel_flip.at[head], relh.at[flip_rows_of(me), :], in_recv.at[chip, 1])

    anti = (lax.broadcasted_iota(jnp.int32, (256, 256), 0) + lax.broadcasted_iota(jnp.int32, (256, 256), 1) == 255).astype(F32).astype(BF16)
    orders = ((2, 1), (0, 2), (1, 0), (2, 0, 1))

    def first_to_head():
        for z, order in enumerate(orders):
            @pl.when(chip == z)
            def _():
                x_to_head(order[0])

    def rest_to_head(z, order):
        for dest in order[1:]:
            x_to_head(dest)
            rel_to_head(dest).start()

    first_to_head()

    @pl.when(active)
    def _():
        for a, x in enumerate(inputs):
            pltpu.make_async_copy(x.at[head], xh.at[a, rows_of(me), :], in_recv.at[chip, 0]).start()
        x_to_partner(me, [x.at[head] for x in inputs])

    load_rt.wait()
    for load_w in loads_w:
        load_w.wait()
    n_groups = block // 256

    @pl.loop(0, n_groups)
    def _(g):
        rows = pl.ds(pl.multiple_of(g * 256, 256), 256)
        flipped = pl.ds(pl.multiple_of((n_groups - 1 - g) * 256, 256), 256)
        rel = mm(anti, mm(rt[rows, :], w2[...]).astype(BF16)).astype(BF16)
        for h in range(n_heads):
            rel_flip[h, flipped, :] = rel[:, h * dim:(h + 1) * dim]

    for z, order in enumerate(orders):
        @pl.when(chip == z)
        def _():
            rel_to_head(order[0]).start()
            if z < n_chips - 1:
                rest_to_head(z, order)

    @pl.when(active)
    def _():
        rel_local().start()
        rel_to_partner(me, rel_flip.at[head]).start()

    dkt[...] = jnp.zeros_like(dkt)
    dvt[...] = jnp.zeros_like(dvt)
    drt[...] = jnp.zeros_like(drt)
    bias_acc[...] = jnp.zeros_like(bias_acc)
    scratch[0][:, :ROWS] = jnp.zeros((ROWS, ROWS), F32)
    relh[pl.ds(seq, COLS), :] = jnp.zeros((COLS, dim), BF16)

    def sent_to_head(dest):
        x_all(me, in_send.at[dest], in_recv.at[chip]).wait_send()
        rel_to_head(dest).wait_send()

    @pl.when(chip == n_chips - 2)
    def _():
        for dest in orders[n_chips - 2]:
            sent_to_head(dest)
        pl.semaphore_signal(go_sem, inc=1, device_id={'cp': jnp.minimum(me + 2, n_dev - 1)}, device_id_type=pl.DeviceIdType.MESH)

    @pl.when(chip == n_chips - 1)
    def _():
        pl.semaphore_wait(go_sem, 1)
        rest_to_head(n_chips - 1, orders[n_chips - 1])

    q_ref, k_ref, v_ref, do_ref = (xh.at[a] for a in range(4))
    pieces = ROWS // 256

    def start(owner, local, remote):
        @pl.when(owner == me)
        def _():
            local().start()

        @pl.when(owner != me)
        def _():
            remote().start()

    def finish(owner, local, remote):
        @pl.when(owner != me)
        def _():
            remote().wait_send()

    per = block // 256

    def piece_of(g):
        return pl.ds(pl.multiple_of(g * 256, 256), 256)

    def tile_copy(i, g, a):
        piece = tile_index(i, core) * pieces + g
        owner = piece // per
        src = o_tiles.at[a, piece_of(i * pieces + g), :]
        dst = (o_out, dq_out)[a].at[head, piece_of(piece % per), :]
        return owner, lambda: pltpu.make_async_copy(src, dst, out_recv.at[a]), lambda: push(src, dst, tile_send.at[i, g, a], out_recv.at[a], owner)

    def ready_blocks(i):
        return (2 * ROWS * i + block - 1) // block

    accs = (dkt, dvt, drt)
    arrays = (2, 0, 1)

    def part_copy(a, c, parity):
        return push(accs[a].at[:, piece_of(2 * c + parity)], part.at[a, c], part_send.at[a, c], part_recv.at[a, c], partner)

    def red_copy(a, c):
        piece = 2 * c + core
        if a == 2:
            src, owner, dst, recv = red_r.at[c], n_dev - 1 - piece // per, dr_in.at[head, :, piece_of(piece % per)], dr_recv
        else:
            src, owner, dst, recv = red.at[a, c], piece // per, (dk_out, dv_out)[a].at[head, piece_of(piece % per), :], g_recv.at[a]
        return owner, lambda: pltpu.make_async_copy(src, dst, recv), lambda: push(src, dst, red_send.at[a, c], recv, owner)

    def reduce(c):
        for a in arrays:
            part_copy(a, c, core).wait_recv()
            total = accs[a][:, piece_of(2 * c + core)] + part[a, c]
            if a == 2:
                red_r[c] = (total * scale).astype(BF16)
            else:
                red[a, c] = (total if a == 1 else total * scale).T.astype(BF16)
            start(*red_copy(a, c))

    lag = 2

    def after_step(c):
        for a in arrays:
            part_copy(a, c, 1 - core).start()

        @pl.when(c >= lag)
        def _():
            reduce(c - lag)

    def bias_copy(d):
        owner = (me + d) % n_dev
        src, dst = bias_acc, bias_in.at[2 * head + core]
        return owner, lambda: pltpu.make_async_copy(src, dst, bias_recv), lambda: push(src, dst, bias_send.at[d], bias_recv, owner)

    @pl.when(active)
    def _():
        def tile(i, **kw):
            with jax.named_scope('wait_ici'):
                @pl.loop(ready_blocks(i), ready_blocks(i + 1))
                def _(dev):
                    @pl.when(dev == me)
                    def _():
                        local = xh.at[:, rows_of(me), :]
                        pltpu.make_async_copy(local, local, in_recv.at[chip, 0]).wait()
                        rel_local().wait()

                    @pl.when((dev % 2 == core) & (dev != me))
                    def _():
                        x_all(dev, in_send.at[0], in_recv.at[dev // 2]).wait_recv()
                        rel_copy(dev, rel_flip.at[head], in_send.at[0], in_recv.at[dev // 2], partner).wait_recv()
                        x_to_partner(dev, [xh.at[a, rows_of(dev), :] for a in range(4)])
                        rel_to_partner(dev, relh.at[flip_rows_of(dev), :]).start()

            with jax.named_scope('wait_core'):
                @pl.loop(ready_blocks(i), ready_blocks(i + 1))
                def _(dev):
                    @pl.when(dev % 2 != core)
                    def _():
                        x_all(dev, fwd_send.at[dev // 2], fwd_recv.at[dev // 2]).wait_recv()
                        rel_to_partner(dev, rel_flip.at[head]).wait_recv()

            tile_grads(tile_index(i, core) * ROWS, i * ROWS, q_ref, k_ref, v_ref, do_ref, relh, u_ref.at[pl.ds(head, 1), :], vb_ref.at[pl.ds(head, 1), :], o_tiles.at[0], o_tiles.at[1], dkt, dvt, drt, bias_acc, *scratch, **kw)
            for g in range(pieces):
                for a in range(2):
                    start(*tile_copy(i, g, a))

        @pl.loop(0, n_tiles - 1)
        def _(i):
            tile(i)

        tile(jnp.int32(n_tiles - 1), after_step=after_step)

        for d in range(n_dev):
            start(*bias_copy(d))

        @pl.loop(n_steps - lag, n_steps)
        def _(c):
            reduce(c)

    half, quarter = w_part.shape[1] // 2, w_part.shape[1] // 2 // n_chips
    sub = quarter // SUBS
    with jax.named_scope('wait_drel'):
        pltpu.make_async_copy(dr_in, dr_in, dr_recv).wait()

    def d_rel_of(h):
        return jnp.concatenate([mm(dr_in[h, :, g * 256:(g + 1) * 256], anti) for g in reversed(range(n_groups))], axis=1).astype(BF16)

    d_rel = jnp.concatenate([d_rel_of(h) for h in range(n_heads)], axis=0)

    def half_rows(c):
        return pl.ds(pl.multiple_of(c * half, half), half)

    def w_rows(c):
        @pl.loop(0, half // 256)
        def _(g):
            rows = pl.ds(pl.multiple_of(c * half + g * 256, 256), 256)
            term = lax.dot_general(rt[:, rows], d_rel, (((0,), (1,)), ((), ())), preferred_element_type=F32)
            for h in range(n_heads):
                w_part[h, rows, :] = term[:, h * dim:(h + 1) * dim]

    pair = push(w_part.at[:, half_rows(1 - core), :], w_in, pair_send, pair_recv, partner)
    with jax.named_scope('w_mm'):
        w_rows(1 - core)
        pair.start()
        w_rows(core)
        pair.wait_recv()
        w_part[:, half_rows(core), :] += w_in[...]

    def sub_rows(q, s):
        return pl.ds(pl.multiple_of(core * half + q * quarter + s * sub, 8), sub)

    side = chip // 2
    mate = chip + 1 - 2 * (chip % 2)
    inner = (chip > 0) & (chip < n_chips - 1)
    far_pair = 2 * (1 - side)
    gate = 2 - side

    def in_rows(s):
        return pl.ds(pl.multiple_of(s * sub, 8), sub)

    def rs_copy(q, slot, s, to):
        return push(w_part.at[:, sub_rows(q, s), :], rs_in.at[slot, :, in_rows(s), :], rs_send.at[slot, s], rs_recv.at[slot, s], 2 * to + core)

    def ag_copy(way, q, s):
        rows = w_out.at[:, sub_rows(q, s), :]
        return push(rows, rows, ag_send.at[way, q, s], agp_recv if way == 2 else ag_recv.at[q, s], (2 * mate + core, 2 * gate + core, partner)[way])

    def add_in(q, slot, s):
        rs_copy(q, slot, s, mate).wait_recv()
        rows = sub_rows(q, s)
        w_part[:, rows, :] += rs_in[slot, :, in_rows(s), :]

    def every_part(body):
        for s in range(SUBS):
            body(s)

    @every_part
    def _(s):
        @pl.when(jnp.logical_not(inner))
        def _():
            for f in range(2):
                rs_copy(far_pair + f, 2 + f, s, mate).start()

        rs_copy(mate, 0, s, mate).start()

    @pl.when(inner)
    def _():
        @every_part
        def _(s):
            for f in range(2):
                add_in(far_pair + f, 2 + f, s)
                push(w_part.at[:, sub_rows(far_pair + f, s), :], rs_in.at[1, :, in_rows(s), :], rs_send.at[2 + f, s], rs_recv.at[1, s], 2 * (far_pair + f) + core).start()

    @every_part
    def _(s):
        add_in(chip, 0, s)
        add_in(chip, 1, s)
        rows = sub_rows(chip, s)
        w_out[:, rows, :] = w_part[:, rows, :]
        for way in range(3):
            ag_copy(way, chip, s).start()

    @every_part
    def _(s):
        ag_copy(0, mate, s).wait_recv()
        ag_copy(2, mate, s).start()
        for f in range(2):
            ag_copy(0, far_pair + f, s).wait_recv()

            @pl.when(inner)
            def _():
                ag_copy(0, far_pair + f, s).start()

            ag_copy(2, far_pair + f, s).start()

    pair.wait_send()

    @pl.loop(0, SUBS)
    def _(s):
        rs_copy(mate, 0, s, mate).wait_send()
        for f in range(2):
            rs_copy(far_pair + f, 2 + f, s, mate).wait_send()

            @pl.when(inner)
            def _():
                ag_copy(0, far_pair + f, s).wait_send()

            ag_copy(2, far_pair + f, s).wait_send()
        ag_copy(2, mate, s).wait_send()
        for way in range(3):
            ag_copy(way, chip, s).wait_send()

    other = w_out.at[:, half_rows(1 - core), :]
    pltpu.make_async_copy(other, other, agp_recv).wait()

    @pl.when(active)
    def _():
        @pl.loop(0, n_steps)
        def _(c):
            for a in arrays:
                part_copy(a, c, 1 - core).wait_send()
                finish(*red_copy(a, c))

        for d in range(n_dev):
            finish(*bias_copy(d))

        @pl.loop(0, n_tiles)
        def _(i):
            for g in range(pieces):
                for a in range(2):
                    finish(*tile_copy(i, g, a))

        @pl.loop(0, n_chips)
        def _(z):
            dev = 2 * z + core
            x_all(dev, fwd_send.at[z], fwd_recv.at[z]).wait_send()
            rel_to_partner(dev, rel_flip.at[head]).wait_send()

    for dest in range(n_heads):
        @pl.when((chip != dest) & (chip != n_chips - 2))
        def _():
            sent_to_head(dest)
    pltpu.make_async_copy(bias_in, bias_in, bias_recv).wait()
    for h in range(n_heads):
        both = bias_in[2 * h] + bias_in[2 * h + 1]
        du_out[h:h + 1, :] = both[0:1]
        dvb_out[h:h + 1, :] = both[1:2]
    with jax.named_scope('wait_results'):
        for a in range(2):
            pltpu.make_async_copy((o_out, dq_out)[a], (o_out, dq_out)[a], out_recv.at[a]).wait()
            pltpu.make_async_copy((dk_out, dv_out)[a], (dk_out, dv_out)[a], g_recv.at[a]).wait()


def group_call(q, k, v, d_out, rel_table, w_rel, u_bias, v_bias, n_dev):
    n_heads, block, dim = q.shape
    like_q = jax.ShapeDtypeStruct((n_heads, block, dim), BF16)
    like_u = jax.ShapeDtypeStruct((n_heads, dim), F32)
    model = rel_table.shape[1]
    seq = block * n_dev
    n_chips = n_dev // 2
    n_tiles = seq // ROWS // 2
    n_steps = seq // COLS
    anyw = pl.BlockSpec(memory_space=pl.ANY)
    vmem = pl.BlockSpec(memory_space=pltpu.VMEM)
    dma = pltpu.SemaphoreType.DMA
    return pl.pallas_call(
        group_kernel,
        name='rel_attention',
        in_specs=[anyw] * 6 + [vmem] * 2,
        out_specs=[anyw] * 4 + [vmem] * 3,
        out_shape=[like_q] * 4 + [like_u] * 2 + [jax.ShapeDtypeStruct((n_heads, model, dim), F32)],
        scratch_shapes=[
            pltpu.VMEM((4, seq, dim), BF16),
            pltpu.VMEM((seq + COLS, dim), BF16),
            pltpu.VMEM((n_heads, block, dim), BF16),
            pltpu.VMEM((block, model), BF16),
            pltpu.VMEM((model, n_heads * dim), BF16),
            pltpu.VMEM((dim, seq), F32),
            pltpu.VMEM((dim, seq), F32),
            pltpu.VMEM((dim, seq + COLS), F32),
            pltpu.VMEM((3, n_steps, dim, 256), F32),
            pltpu.VMEM((2, n_steps, 256, dim), BF16),
            pltpu.VMEM((n_steps, dim, 256), BF16),
            pltpu.VMEM((2, seq // 2, dim), BF16),
            pltpu.VMEM((8, dim), F32),
            pltpu.VMEM((2 * n_heads, 8, dim), F32),
            pltpu.VMEM((n_heads, dim, block), BF16),
            pltpu.VMEM((n_heads, model, dim), F32),
            pltpu.VMEM((n_heads, model // 2, dim), F32),
            pltpu.VMEM((4, n_heads, model // 2 // n_chips, dim), F32),
            pltpu.VMEM((ROWS, seq + ROWS + COLS), F32),
            pltpu.VMEM((ROWS, 128), F32),
            pltpu.VMEM((ROWS, 128), F32),
            pltpu.VMEM((ROWS, dim), F32),
            pltpu.VMEM((ROWS, dim), F32),
            pltpu.VMEM((ROWS, dim), F32),
            dma((n_heads, 2)), dma((n_chips, 2)), dma((n_chips, 2)), dma((n_chips, 2)),
            dma((3, n_steps)), dma((3, n_steps)), dma((n_tiles, ROWS // 256, 2)), dma((3, n_steps)), dma((n_dev,)), dma((2,)), dma((2,)), dma, dma((1 + n_heads,)),
            dma, dma, dma, dma((4, SUBS)), dma((4, SUBS)), dma((3, n_chips, SUBS)), dma((n_chips, SUBS)), dma, pltpu.SemaphoreType.REGULAR,
        ],
        compiler_params=pltpu.CompilerParams(vmem_limit_bytes=67043328, collective_id=0, has_side_effects=True),
    )(q, k, v, d_out, rel_table, w_rel, u_bias, v_bias)


def solution(mesh):
    n_dev = mesh.shape['cp']
    seq_spec = P('cp', 'hp', None)
    head_spec = P('hp', None)
    weight_spec = P(None, 'hp', None)

    def local_fn(q, k, v, u_bias, v_bias, rel_table, w_rel, d_out):
        swap = lambda x: x.transpose(1, 0, 2)
        *rows, d_u, d_v, d_w = group_call(swap(q), swap(k), swap(v), swap(d_out), rel_table, swap(w_rel), u_bias, v_bias, n_dev)
        return (*(swap(x) for x in rows), d_u, d_v, swap(d_w))

    return jax.shard_map(
        local_fn,
        mesh=mesh,
        in_specs=(seq_spec, seq_spec, seq_spec, head_spec, head_spec, P('cp', None), weight_spec, seq_spec),
        out_specs=(seq_spec, seq_spec, seq_spec, seq_spec, head_spec, head_spec, weight_spec),
        check_vma=False,
    )
```

```python
import functools
import math

import jax
import jax.numpy as jnp
from jax import lax
from jax.experimental import pallas as pl
from jax.experimental.pallas import tpu as pltpu
from jax.sharding import PartitionSpec as P

F32, BF16 = jnp.float32, jnp.bfloat16
ROWS = 512
COLS = 512
SUBS = 4
NT = (((1,), (1,)), ((), ()))
NN = (((1,), (0,)), ((), ()))


def mm(a, b, dims=NN, precision=None):
    return lax.dot_general(a, b, dims, preferred_element_type=F32, precision=precision)


def fold_lanes(op, x):
    acc = x[:, :128]
    for g in range(1, x.shape[1] // 128):
        acc = op(acc, x[:, g * 128:(g + 1) * 128])
    return acc


def shear(buf, start, shift):
    out = []
    for g in range(ROWS // 128):
        part = buf[g * 128:(g + 1) * 128, pl.ds(pl.multiple_of(start - (g + 1) * 128, 128), COLS + 128)]
        out.append(pltpu.roll(part, shift, 1, stride=1, stride_axis=0)[:, 128:])
    return jnp.concatenate(out, axis=0)


def flip_rows(anti, x):
    return jnp.concatenate([mm(anti, x[g * 256:(g + 1) * 256]) for g in reversed(range(x.shape[0] // 256))], axis=0)


def flip_eights(x):
    back = 7 - lax.broadcasted_iota(jnp.int32, (8, 128), 0)
    rows = []
    for r in range(0, x.shape[0], 8):
        rows.append(jnp.concatenate([jnp.take_along_axis(x[r:r + 8, c:c + 128], back, axis=0, mode='promise_in_bounds') for c in range(0, x.shape[1], 128)], axis=1))
    return jnp.concatenate(rows, axis=0)


def shear_back(buf, start):
    out = []
    for g in range(ROWS // 8):
        left = ROWS - 8 - 8 * g
        base = start - 128 * (left // 128 + 1)
        part = flip_eights(buf[8 * g:8 * g + 8, pl.ds(pl.multiple_of(base, 128), COLS + 128)])
        out.append(pltpu.roll(part, left % 128, 1, stride=1, stride_axis=0)[:, 128:])
    return jnp.concatenate(out, axis=0)


def tile_grads(q0, out_row, q_ref, k_ref, v_ref, do_ref, rel_ref, u_ref, vb_ref, o_ref, dq_ref, dkt, dvt, drt, bias_acc, buf, m_ref, l_ref, acc_ref, gu_ref, gv_ref, after_step=None):
    seq, dim = k_ref.shape
    scale = dim ** -0.5
    steps = (q0 + ROWS + COLS - 1) // COLS
    rel0 = seq - ROWS - q0

    def at(base, size):
        return pl.ds(pl.multiple_of(base, 256), size)

    q_wide = q_ref[at(q0, ROWS), :].astype(F32)
    q_u = (q_wide + u_ref[...]).astype(BF16)
    q_v = (q_wide + vb_ref[...]).astype(BF16)

    def offset_scores(c):
        buf[:, at(c * COLS + ROWS, COLS)] = mm(q_v, rel_ref[at(rel0 + c * COLS, COLS), :], NT)

    def scores(c):
        j0 = c * COLS
        return mm(q_u, k_ref[at(j0, COLS), :], NT) + shear(buf, j0 + 2 * ROWS, 1)

    def keep(c, score):
        buf[:, at(c * COLS + ROWS, COLS)] = score
        m_ref[...] = jnp.maximum(m_ref[...], fold_lanes(jnp.maximum, score))

    m_ref[...] = jnp.full_like(m_ref, -jnp.inf)
    offset_scores(0)
    offset_scores(1)

    @pl.loop(0, steps - 1)
    def _(c):
        keep(c, scores(c))
        offset_scores(c + 2)

    row_minus_col = lax.broadcasted_iota(jnp.int32, (ROWS, COLS), 0) - lax.broadcasted_iota(jnp.int32, (ROWS, COLS), 1)
    last = steps - 1
    keep(last, jnp.where(row_minus_col >= last * COLS - q0, scores(last), -jnp.inf))

    row_max = jnp.max(m_ref[...], axis=1, keepdims=True)
    l_ref[...] = jnp.zeros_like(l_ref)
    acc_ref[...] = jnp.zeros_like(acc_ref)

    @pl.loop(0, steps)
    def _(c):
        j0 = c * COLS
        prob = jnp.exp2((buf[:, at(j0 + ROWS, COLS)] - row_max) * (scale * math.log2(math.e)))
        buf[:, at(j0 + ROWS, COLS)] = prob
        l_ref[...] += fold_lanes(jnp.add, prob)
        acc_ref[...] += mm(prob.astype(BF16), v_ref[at(j0, COLS), :])

    inv_sum = 1.0 / jnp.sum(l_ref[...], axis=1, keepdims=True)
    out = acc_ref[...] * inv_sum
    o_ref[at(out_row, ROWS), :] = out.astype(BF16)
    d_out = do_ref[at(q0, ROWS), :]
    do_wide = d_out.astype(F32)
    delta = jnp.sum(do_wide * out, axis=1, keepdims=True)
    do_t = do_wide.T.astype(BF16)
    qu_t = q_u.astype(F32).T.astype(BF16)
    qv_rt = flip_eights(q_v.astype(F32)).T.astype(BF16)
    gu_ref[...] = jnp.zeros_like(gu_ref)
    gv_ref[...] = jnp.zeros_like(gv_ref)

    def by_key(c):
        j0 = c * COLS
        cols = at(j0, COLS)
        prob = buf[:, at(j0 + ROWS, COLS)] * inv_sum
        ds_wide = prob * (mm(d_out, v_ref[cols, :], NT) - delta)
        ds = ds_wide.astype(BF16)
        dvt[:, cols] += mm(do_t, prob.astype(BF16))
        dkt[:, cols] += mm(qu_t, ds)
        gu_ref[...] += mm(ds, k_ref[cols, :])
        buf[:, at(j0 + ROWS, COLS)] = ds_wide

    def by_offset(c):
        c0 = c * COLS
        ds = shear_back(buf, c0 + ROWS).astype(BF16)
        cols = at(rel0 + c0, COLS)
        gv_ref[...] += mm(ds, rel_ref[cols, :])
        drt[:, cols] += mm(qv_rt, ds)

    by_key(0)

    @pl.loop(1, steps)
    def _(c):
        by_offset(c - 1)
        by_key(c)
        if after_step is not None:
            after_step(c - 1)

    by_offset(steps - 1)
    if after_step is not None:
        @pl.loop(steps - 1, seq // COLS)
        def _(c):
            after_step(c)

    g_u = gu_ref[...]
    g_vr = gv_ref[...]
    g_v = flip_eights(g_vr)
    dq_ref[at(out_row, ROWS), :] = ((g_u + g_v) * scale).astype(BF16)
    bias_acc[0:1, :] += jnp.sum(g_u, axis=0, keepdims=True) * scale
    bias_acc[1:2, :] += jnp.sum(g_vr, axis=0, keepdims=True) * scale


def tile_index(i, core):
    return 4 * (i // 2) + jnp.where(i % 2 == 0, core, 3 - core)


def group_kernel(q_hbm, k_hbm, v_hbm, do_hbm, rt_hbm, w_hbm, u_ref, vb_ref, o_out, dq_out, dk_out, dv_out, du_out, dvb_out, w_out, xh, relh, rel_flip, rt, w2, dkt, dvt, drt, part, red, red_r, o_tiles, bias_acc, bias_in, dr_in, w_part, w_in, rs_in, *rest):
    scratch, sems = rest[:6], rest[6:]
    (in_send, in_recv, fwd_send, fwd_recv, part_send, part_recv, tile_send, red_send, bias_send, out_recv, g_recv, bias_recv, load_sem,
     dr_recv, pair_send, pair_recv, rs_send, rs_recv, ag_send, ag_recv, agp_recv, go_sem) = sems
    inputs = (q_hbm, k_hbm, v_hbm, do_hbm)
    n_heads, block, dim = q_hbm.shape
    n_dev = lax.axis_size('cp')
    n_chips = n_dev // 2
    seq = block * n_dev
    n_steps = seq // COLS
    scale = dim ** -0.5
    me = lax.axis_index('cp')
    chip, core = me // 2, me % 2
    head = jnp.minimum(chip, n_heads - 1)
    active = chip < n_heads
    partner = 2 * chip + 1 - core
    n_tiles = seq // ROWS // 2

    load_rt = pltpu.make_async_copy(rt_hbm, rt, load_sem.at[0])
    loads_w = [pltpu.make_async_copy(w_hbm.at[h], w2.at[:, h * dim:(h + 1) * dim], load_sem.at[1 + h]) for h in range(n_heads)]
    load_rt.start()
    for load_w in loads_w:
        load_w.start()

    barrier = pltpu.get_barrier_semaphore()
    for d in range(1, n_dev):
        pl.semaphore_signal(barrier, inc=1, device_id={'cp': (me + d) % n_dev}, device_id_type=pl.DeviceIdType.MESH)
    pl.semaphore_wait(barrier, n_dev - 1)

    def push(src, dst, send, recv, dev):
        return pltpu.make_async_remote_copy(src_ref=src, dst_ref=dst, send_sem=send, recv_sem=recv, device_id={'cp': dev}, device_id_type=pl.DeviceIdType.MESH)

    def rows_of(dev):
        return pl.ds(pl.multiple_of(dev * block, block), block)

    def flip_rows_of(dev):
        return pl.ds(pl.multiple_of(seq - block - dev * block, block), block)

    def x_copies(src_dev, srcs, send, recv, dev):
        return [push(srcs[a], xh.at[a, rows_of(src_dev), :], send.at[0], recv.at[0], dev) for a in range(4)]

    def x_all(src_dev, send, recv):
        rows = xh.at[:, rows_of(src_dev), :]
        return push(rows, rows, send.at[0], recv.at[0], partner)

    def rel_copy(src_dev, src, send, recv, dev):
        return push(src, relh.at[flip_rows_of(src_dev), :], send.at[1], recv.at[1], dev)

    def x_to_head(dest):
        for copy in x_copies(me, [x.at[dest] for x in inputs], in_send.at[dest], in_recv.at[chip], 2 * dest + core):
            copy.start()

    def rel_to_head(dest):
        return rel_copy(me, rel_flip.at[dest], in_send.at[dest], in_recv.at[chip], 2 * dest + core)

    def x_to_partner(dev, srcs):
        for copy in x_copies(dev, srcs, fwd_send.at[dev // 2], fwd_recv.at[dev // 2], partner):
            copy.start()

    def rel_to_partner(dev, src):
        return rel_copy(dev, src, fwd_send.at[dev // 2], fwd_recv.at[dev // 2], partner)

    def rel_local():
        return pltpu.make_async_copy(rel_flip.at[head], relh.at[flip_rows_of(me), :], in_recv.at[chip, 1])

    anti = (lax.broadcasted_iota(jnp.int32, (256, 256), 0) + lax.broadcasted_iota(jnp.int32, (256, 256), 1) == 255).astype(F32).astype(BF16)
    orders = ((1, 2), (0, 2), (1, 0), (2, 0, 1))

    def first_to_head():
        for z, order in enumerate(orders):
            @pl.when(chip == z)
            def _():
                x_to_head(order[0])

    def rest_to_head(z, order):
        for dest in order[1:]:
            x_to_head(dest)
            rel_to_head(dest).start()

    first_to_head()

    @pl.when(active)
    def _():
        for a, x in enumerate(inputs):
            pltpu.make_async_copy(x.at[head], xh.at[a, rows_of(me), :], in_recv.at[chip, 0]).start()
        x_to_partner(me, [x.at[head] for x in inputs])

    load_rt.wait()
    for load_w in loads_w:
        load_w.wait()
    n_groups = block // 256

    @pl.loop(0, n_groups)
    def _(g):
        rows = pl.ds(pl.multiple_of(g * 256, 256), 256)
        flipped = pl.ds(pl.multiple_of((n_groups - 1 - g) * 256, 256), 256)
        rel = mm(anti, mm(rt[rows, :], w2[...]).astype(BF16)).astype(BF16)
        for h in range(n_heads):
            rel_flip[h, flipped, :] = rel[:, h * dim:(h + 1) * dim]

    for z, order in enumerate(orders):
        @pl.when(chip == z)
        def _():
            rel_to_head(order[0]).start()
            if z < n_chips - 1:
                rest_to_head(z, order)

    @pl.when(active)
    def _():
        rel_local().start()
        rel_to_partner(me, rel_flip.at[head]).start()

    dkt[...] = jnp.zeros_like(dkt)
    dvt[...] = jnp.zeros_like(dvt)
    drt[...] = jnp.zeros_like(drt)
    bias_acc[...] = jnp.zeros_like(bias_acc)
    scratch[0][:, :ROWS] = jnp.zeros((ROWS, ROWS), F32)
    relh[pl.ds(seq, COLS), :] = jnp.zeros((COLS, dim), BF16)

    def sent_to_head(dest):
        x_all(me, in_send.at[dest], in_recv.at[chip]).wait_send()
        rel_to_head(dest).wait_send()

    @pl.when(chip == n_chips - 2)
    def _():
        for dest in orders[n_chips - 2]:
            sent_to_head(dest)
        pl.semaphore_signal(go_sem, inc=1, device_id={'cp': jnp.minimum(me + 2, n_dev - 1)}, device_id_type=pl.DeviceIdType.MESH)

    @pl.when(chip == n_chips - 1)
    def _():
        @pl.when(core == 0)
        def _():
            pl.semaphore_wait(go_sem, 1)
            rest_to_head(n_chips - 1, orders[n_chips - 1])
            for dest in orders[n_chips - 1]:
                sent_to_head(dest)
            pl.semaphore_signal(go_sem, inc=1, device_id={'cp': partner}, device_id_type=pl.DeviceIdType.MESH)

        @pl.when(core == 1)
        def _():
            pl.semaphore_wait(go_sem, 2)
            rest_to_head(n_chips - 1, orders[n_chips - 1])

    q_ref, k_ref, v_ref, do_ref = (xh.at[a] for a in range(4))
    pieces = ROWS // 256

    def start(owner, local, remote):
        @pl.when(owner == me)
        def _():
            local().start()

        @pl.when(owner != me)
        def _():
            remote().start()

    def finish(owner, local, remote):
        @pl.when(owner != me)
        def _():
            remote().wait_send()

    per = block // 256

    def piece_of(g):
        return pl.ds(pl.multiple_of(g * 256, 256), 256)

    def tile_copy(i, g, a):
        piece = tile_index(i, core) * pieces + g
        owner = piece // per
        src = o_tiles.at[a, piece_of(i * pieces + g), :]
        dst = (o_out, dq_out)[a].at[head, piece_of(piece % per), :]
        return owner, lambda: pltpu.make_async_copy(src, dst, out_recv.at[a]), lambda: push(src, dst, tile_send.at[i, g, a], out_recv.at[a], owner)

    def ready_blocks(i):
        return (2 * ROWS * i + block - 1) // block

    accs = (dkt, dvt, drt)
    arrays = (2, 0, 1)

    def part_copy(a, c, parity):
        return push(accs[a].at[:, piece_of(2 * c + parity)], part.at[a, c], part_send.at[a, c], part_recv.at[a, c], partner)

    def red_copy(a, c):
        piece = 2 * c + core
        if a == 2:
            src, owner, dst, recv = red_r.at[c], n_dev - 1 - piece // per, dr_in.at[head, :, piece_of(piece % per)], dr_recv
        else:
            src, owner, dst, recv = red.at[a, c], piece // per, (dk_out, dv_out)[a].at[head, piece_of(piece % per), :], g_recv.at[a]
        return owner, lambda: pltpu.make_async_copy(src, dst, recv), lambda: push(src, dst, red_send.at[a, c], recv, owner)

    def reduce(c):
        for a in arrays:
            part_copy(a, c, core).wait_recv()
            total = accs[a][:, piece_of(2 * c + core)] + part[a, c]
            if a == 2:
                red_r[c] = (total * scale).astype(BF16)
            else:
                red[a, c] = (total if a == 1 else total * scale).T.astype(BF16)
            start(*red_copy(a, c))

    lag = 2

    def after_step(c):
        for a in arrays:
            part_copy(a, c, 1 - core).start()

        @pl.when(c >= lag)
        def _():
            reduce(c - lag)

    def bias_copy(d):
        owner = (me + d) % n_dev
        src, dst = bias_acc, bias_in.at[2 * head + core]
        return owner, lambda: pltpu.make_async_copy(src, dst, bias_recv), lambda: push(src, dst, bias_send.at[d], bias_recv, owner)

    @pl.when(active)
    def _():
        def tile(i, **kw):
            with jax.named_scope('wait_ici'):
                @pl.loop(ready_blocks(i), ready_blocks(i + 1))
                def _(dev):
                    @pl.when(dev == me)
                    def _():
                        local = xh.at[:, rows_of(me), :]
                        pltpu.make_async_copy(local, local, in_recv.at[chip, 0]).wait()
                        rel_local().wait()

                    @pl.when((dev % 2 == core) & (dev != me))
                    def _():
                        x_all(dev, in_send.at[0], in_recv.at[dev // 2]).wait_recv()
                        rel_copy(dev, rel_flip.at[head], in_send.at[0], in_recv.at[dev // 2], partner).wait_recv()
                        x_to_partner(dev, [xh.at[a, rows_of(dev), :] for a in range(4)])
                        rel_to_partner(dev, relh.at[flip_rows_of(dev), :]).start()

            with jax.named_scope('wait_core'):
                @pl.loop(ready_blocks(i), ready_blocks(i + 1))
                def _(dev):
                    @pl.when(dev % 2 != core)
                    def _():
                        x_all(dev, fwd_send.at[dev // 2], fwd_recv.at[dev // 2]).wait_recv()
                        rel_to_partner(dev, rel_flip.at[head]).wait_recv()

            tile_grads(tile_index(i, core) * ROWS, i * ROWS, q_ref, k_ref, v_ref, do_ref, relh, u_ref.at[pl.ds(head, 1), :], vb_ref.at[pl.ds(head, 1), :], o_tiles.at[0], o_tiles.at[1], dkt, dvt, drt, bias_acc, *scratch, **kw)
            for g in range(pieces):
                for a in range(2):
                    start(*tile_copy(i, g, a))

        @pl.loop(0, n_tiles - 1)
        def _(i):
            tile(i)

        tile(jnp.int32(n_tiles - 1), after_step=after_step)

        for d in range(n_dev):
            start(*bias_copy(d))

        @pl.loop(n_steps - lag, n_steps)
        def _(c):
            reduce(c)

    half, quarter = w_part.shape[1] // 2, w_part.shape[1] // 2 // n_chips
    sub = quarter // SUBS
    with jax.named_scope('wait_drel'):
        pltpu.make_async_copy(dr_in, dr_in, dr_recv).wait()

    def d_rel_of(h):
        return jnp.concatenate([mm(dr_in[h, :, g * 256:(g + 1) * 256], anti) for g in reversed(range(n_groups))], axis=1).astype(BF16)

    d_rel = jnp.concatenate([d_rel_of(h) for h in range(n_heads)], axis=0)

    def half_rows(c):
        return pl.ds(pl.multiple_of(c * half, half), half)

    def w_rows(c):
        @pl.loop(0, half // 256)
        def _(g):
            rows = pl.ds(pl.multiple_of(c * half + g * 256, 256), 256)
            term = lax.dot_general(rt[:, rows], d_rel, (((0,), (1,)), ((), ())), preferred_element_type=F32)
            for h in range(n_heads):
                w_part[h, rows, :] = term[:, h * dim:(h + 1) * dim]

    pair = push(w_part.at[:, half_rows(1 - core), :], w_in, pair_send, pair_recv, partner)
    with jax.named_scope('w_mm'):
        w_rows(1 - core)
        pair.start()
        w_rows(core)
        pair.wait_recv()
        w_part[:, half_rows(core), :] += w_in[...]

    def sub_rows(q, s):
        return pl.ds(pl.multiple_of(core * half + q * quarter + s * sub, 8), sub)

    side = chip // 2
    mate = chip + 1 - 2 * (chip % 2)
    inner = (chip > 0) & (chip < n_chips - 1)
    far_pair = 2 * (1 - side)
    gate = 2 - side

    def in_rows(s):
        return pl.ds(pl.multiple_of(s * sub, 8), sub)

    def rs_copy(q, slot, s, to):
        return push(w_part.at[:, sub_rows(q, s), :], rs_in.at[slot, :, in_rows(s), :], rs_send.at[slot, s], rs_recv.at[slot, s], 2 * to + core)

    def ag_copy(way, q, s):
        rows = w_out.at[:, sub_rows(q, s), :]
        return push(rows, rows, ag_send.at[way, q, s], agp_recv if way == 2 else ag_recv.at[q, s], (2 * mate + core, 2 * gate + core, partner)[way])

    def add_in(q, slot, s):
        rs_copy(q, slot, s, mate).wait_recv()
        rows = sub_rows(q, s)
        w_part[:, rows, :] += rs_in[slot, :, in_rows(s), :]

    def every_part(body):
        for s in range(SUBS):
            body(s)

    @every_part
    def _(s):
        @pl.when(jnp.logical_not(inner))
        def _():
            for f in range(2):
                rs_copy(far_pair + f, 2 + f, s, mate).start()

        rs_copy(mate, 0, s, mate).start()

    @pl.when(inner)
    def _():
        @every_part
        def _(s):
            for f in range(2):
                add_in(far_pair + f, 2 + f, s)
                push(w_part.at[:, sub_rows(far_pair + f, s), :], rs_in.at[1, :, in_rows(s), :], rs_send.at[2 + f, s], rs_recv.at[1, s], 2 * (far_pair + f) + core).start()

    @every_part
    def _(s):
        add_in(chip, 0, s)
        add_in(chip, 1, s)
        rows = sub_rows(chip, s)
        w_out[:, rows, :] = w_part[:, rows, :]
        ag_copy(0, chip, s).start()

        @pl.when(inner)
        def _():
            ag_copy(1, chip, s).start()

        ag_copy(2, chip, s).start()

    @every_part
    def _(s):
        ag_copy(0, mate, s).wait_recv()

        @pl.when(inner)
        def _():
            ag_copy(1, mate, s).start()

        ag_copy(2, mate, s).start()
        for f in range(2):
            ag_copy(0, far_pair + f, s).wait_recv()

            @pl.when(inner)
            def _():
                ag_copy(0, far_pair + f, s).start()

            ag_copy(2, far_pair + f, s).start()

    pair.wait_send()

    @pl.loop(0, SUBS)
    def _(s):
        rs_copy(mate, 0, s, mate).wait_send()
        for f in range(2):
            rs_copy(far_pair + f, 2 + f, s, mate).wait_send()

            @pl.when(inner)
            def _():
                ag_copy(0, far_pair + f, s).wait_send()

            ag_copy(2, far_pair + f, s).wait_send()
        ag_copy(2, mate, s).wait_send()
        ag_copy(0, chip, s).wait_send()
        ag_copy(2, chip, s).wait_send()

        @pl.when(inner)
        def _():
            ag_copy(1, chip, s).wait_send()
            ag_copy(1, mate, s).wait_send()

    other = w_out.at[:, half_rows(1 - core), :]
    pltpu.make_async_copy(other, other, agp_recv).wait()

    @pl.when(active)
    def _():
        @pl.loop(0, n_steps)
        def _(c):
            for a in arrays:
                part_copy(a, c, 1 - core).wait_send()
                finish(*red_copy(a, c))

        for d in range(n_dev):
            finish(*bias_copy(d))

        @pl.loop(0, n_tiles)
        def _(i):
            for g in range(pieces):
                for a in range(2):
                    finish(*tile_copy(i, g, a))

        @pl.loop(0, n_chips)
        def _(z):
            dev = 2 * z + core
            x_all(dev, fwd_send.at[z], fwd_recv.at[z]).wait_send()
            rel_to_partner(dev, rel_flip.at[head]).wait_send()

    for dest in range(n_heads):
        @pl.when((chip != dest) & (chip != n_chips - 2) & jnp.logical_not((chip == n_chips - 1) & (core == 0)))
        def _():
            sent_to_head(dest)
    pltpu.make_async_copy(bias_in, bias_in, bias_recv).wait()
    for h in range(n_heads):
        both = bias_in[2 * h] + bias_in[2 * h + 1]
        du_out[h:h + 1, :] = both[0:1]
        dvb_out[h:h + 1, :] = both[1:2]
    with jax.named_scope('wait_results'):
        for a in range(2):
            pltpu.make_async_copy((o_out, dq_out)[a], (o_out, dq_out)[a], out_recv.at[a]).wait()
            pltpu.make_async_copy((dk_out, dv_out)[a], (dk_out, dv_out)[a], g_recv.at[a]).wait()


def group_call(q, k, v, d_out, rel_table, w_rel, u_bias, v_bias, n_dev):
    n_heads, block, dim = q.shape
    like_q = jax.ShapeDtypeStruct((n_heads, block, dim), BF16)
    like_u = jax.ShapeDtypeStruct((n_heads, dim), F32)
    model = rel_table.shape[1]
    seq = block * n_dev
    n_chips = n_dev // 2
    n_tiles = seq // ROWS // 2
    n_steps = seq // COLS
    anyw = pl.BlockSpec(memory_space=pl.ANY)
    vmem = pl.BlockSpec(memory_space=pltpu.VMEM)
    dma = pltpu.SemaphoreType.DMA
    return pl.pallas_call(
        group_kernel,
        name='rel_attention',
        in_specs=[anyw] * 6 + [vmem] * 2,
        out_specs=[anyw] * 4 + [vmem] * 3,
        out_shape=[like_q] * 4 + [like_u] * 2 + [jax.ShapeDtypeStruct((n_heads, model, dim), F32)],
        scratch_shapes=[
            pltpu.VMEM((4, seq, dim), BF16),
            pltpu.VMEM((seq + COLS, dim), BF16),
            pltpu.VMEM((n_heads, block, dim), BF16),
            pltpu.VMEM((block, model), BF16),
            pltpu.VMEM((model, n_heads * dim), BF16),
            pltpu.VMEM((dim, seq), F32),
            pltpu.VMEM((dim, seq), F32),
            pltpu.VMEM((dim, seq + COLS), F32),
            pltpu.VMEM((3, n_steps, dim, 256), F32),
            pltpu.VMEM((2, n_steps, 256, dim), BF16),
            pltpu.VMEM((n_steps, dim, 256), BF16),
            pltpu.VMEM((2, seq // 2, dim), BF16),
            pltpu.VMEM((8, dim), F32),
            pltpu.VMEM((2 * n_heads, 8, dim), F32),
            pltpu.VMEM((n_heads, dim, block), BF16),
            pltpu.VMEM((n_heads, model, dim), F32),
            pltpu.VMEM((n_heads, model // 2, dim), F32),
            pltpu.VMEM((4, n_heads, model // 2 // n_chips, dim), F32),
            pltpu.VMEM((ROWS, seq + ROWS + COLS), F32),
            pltpu.VMEM((ROWS, 128), F32),
            pltpu.VMEM((ROWS, 128), F32),
            pltpu.VMEM((ROWS, dim), F32),
            pltpu.VMEM((ROWS, dim), F32),
            pltpu.VMEM((ROWS, dim), F32),
            dma((n_heads, 2)), dma((n_chips, 2)), dma((n_chips, 2)), dma((n_chips, 2)),
            dma((3, n_steps)), dma((3, n_steps)), dma((n_tiles, ROWS // 256, 2)), dma((3, n_steps)), dma((n_dev,)), dma((2,)), dma((2,)), dma, dma((1 + n_heads,)),
            dma, dma, dma, dma((4, SUBS)), dma((4, SUBS)), dma((3, n_chips, SUBS)), dma((n_chips, SUBS)), dma, pltpu.SemaphoreType.REGULAR,
        ],
        compiler_params=pltpu.CompilerParams(vmem_limit_bytes=67043328, collective_id=0, has_side_effects=True),
    )(q, k, v, d_out, rel_table, w_rel, u_bias, v_bias)


def hand_over(*refs):
    n = (len(refs) - 2) // 3
    srcs, dsts, bufs = refs[:n], refs[n:2 * n], refs[2 * n:3 * n]
    in_sem, out_sem = refs[3 * n:]
    loads = [pltpu.make_async_copy(srcs[i], bufs[i], in_sem.at[i]) for i in range(n)]
    stores = [pltpu.make_async_copy(bufs[i], dsts[i], out_sem.at[i]) for i in range(n)]
    for load in loads:
        load.start()
    for load, store in zip(loads, stores):
        load.wait()
        store.start()
    for store in stores:
        store.wait()


def hand_over_call(arrays):
    n = len(arrays)
    anyw = pl.BlockSpec(memory_space=pl.ANY)
    return pl.pallas_call(
        hand_over,
        name='hand_over',
        in_specs=[anyw] * n,
        out_specs=[anyw] * n,
        out_shape=[jax.ShapeDtypeStruct(x.shape, x.dtype) for x in arrays],
        scratch_shapes=[pltpu.VMEM(x.shape, x.dtype) for x in arrays] + [pltpu.SemaphoreType.DMA((n,))] * 2,
        compiler_params=pltpu.CompilerParams(vmem_limit_bytes=67043328),
    )(*arrays)


def solution(mesh):
    n_dev = mesh.shape['cp']
    seq_spec = P('cp', 'hp', None)
    head_spec = P('hp', None)
    weight_spec = P(None, 'hp', None)

    def local_fn(q, k, v, u_bias, v_bias, rel_table, w_rel, d_out):
        swap = lambda x: x.transpose(1, 0, 2)
        *rows, d_u, d_v, d_w = hand_over_call(group_call(swap(q), swap(k), swap(v), swap(d_out), rel_table, swap(w_rel), u_bias, v_bias, n_dev))
        return (*(swap(x) for x in rows), d_u, d_v, swap(d_w))

    return jax.shard_map(
        local_fn,
        mesh=mesh,
        in_specs=(seq_spec, seq_spec, seq_spec, head_spec, head_spec, P('cp', None), weight_spec, seq_spec),
        out_specs=(seq_spec, seq_spec, seq_spec, seq_spec, head_spec, head_spec, weight_spec),
        check_vma=False,
    )
```

```python
import functools
import math

import jax
import jax.numpy as jnp
from jax import lax
from jax.experimental import pallas as pl
from jax.experimental.pallas import tpu as pltpu
from jax.sharding import PartitionSpec as P

F32, BF16 = jnp.float32, jnp.bfloat16
ROWS = 512
COLS = 512
SUBS = 8
NT = (((1,), (1,)), ((), ()))
NN = (((1,), (0,)), ((), ()))


def mm(a, b, dims=NN, precision=None):
    return lax.dot_general(a, b, dims, preferred_element_type=F32, precision=precision)


def fold_lanes(op, x):
    acc = x[:, :128]
    for g in range(1, x.shape[1] // 128):
        acc = op(acc, x[:, g * 128:(g + 1) * 128])
    return acc


def shear(buf, start, shift):
    out = []
    for g in range(ROWS // 128):
        part = buf[g * 128:(g + 1) * 128, pl.ds(pl.multiple_of(start - (g + 1) * 128, 128), COLS + 128)]
        out.append(pltpu.roll(part, shift, 1, stride=1, stride_axis=0)[:, 128:])
    return jnp.concatenate(out, axis=0)


def flip_rows(anti, x):
    return jnp.concatenate([mm(anti, x[g * 256:(g + 1) * 256]) for g in reversed(range(x.shape[0] // 256))], axis=0)


def flip_eights(x):
    back = 7 - lax.broadcasted_iota(jnp.int32, (8, 128), 0)
    rows = []
    for r in range(0, x.shape[0], 8):
        rows.append(jnp.concatenate([jnp.take_along_axis(x[r:r + 8, c:c + 128], back, axis=0, mode='promise_in_bounds') for c in range(0, x.shape[1], 128)], axis=1))
    return jnp.concatenate(rows, axis=0)


def shear_back(buf, start):
    out = []
    for g in range(ROWS // 8):
        left = ROWS - 8 - 8 * g
        base = start - 128 * (left // 128 + 1)
        part = flip_eights(buf[8 * g:8 * g + 8, pl.ds(pl.multiple_of(base, 128), COLS + 128)])
        out.append(pltpu.roll(part, left % 128, 1, stride=1, stride_axis=0)[:, 128:])
    return jnp.concatenate(out, axis=0)


def tile_grads(q0, out_row, q_ref, k_ref, v_ref, do_ref, rel_ref, u_ref, vb_ref, o_ref, dq_ref, dkt, dvt, drt, bias_acc, buf, m_ref, l_ref, acc_ref, gu_ref, gv_ref, after_step=None):
    seq, dim = k_ref.shape
    scale = dim ** -0.5
    steps = (q0 + ROWS + COLS - 1) // COLS
    rel0 = seq - ROWS - q0

    def at(base, size):
        return pl.ds(pl.multiple_of(base, 256), size)

    q_wide = q_ref[at(q0, ROWS), :].astype(F32)
    q_u = (q_wide + u_ref[...]).astype(BF16)
    q_v = (q_wide + vb_ref[...]).astype(BF16)

    def offset_scores(c):
        buf[:, at(c * COLS + ROWS, COLS)] = mm(q_v, rel_ref[at(rel0 + c * COLS, COLS), :], NT)

    def scores(c):
        j0 = c * COLS
        return mm(q_u, k_ref[at(j0, COLS), :], NT) + shear(buf, j0 + 2 * ROWS, 1)

    def keep(c, score):
        buf[:, at(c * COLS + ROWS, COLS)] = score
        m_ref[...] = jnp.maximum(m_ref[...], fold_lanes(jnp.maximum, score))

    m_ref[...] = jnp.full_like(m_ref, -jnp.inf)
    offset_scores(0)
    offset_scores(1)

    @pl.loop(0, steps - 1)
    def _(c):
        keep(c, scores(c))
        offset_scores(c + 2)

    row_minus_col = lax.broadcasted_iota(jnp.int32, (ROWS, COLS), 0) - lax.broadcasted_iota(jnp.int32, (ROWS, COLS), 1)
    last = steps - 1
    keep(last, jnp.where(row_minus_col >= last * COLS - q0, scores(last), -jnp.inf))

    row_max = jnp.max(m_ref[...], axis=1, keepdims=True)
    l_ref[...] = jnp.zeros_like(l_ref)
    acc_ref[...] = jnp.zeros_like(acc_ref)

    @pl.loop(0, steps)
    def _(c):
        j0 = c * COLS
        prob = jnp.exp2((buf[:, at(j0 + ROWS, COLS)] - row_max) * (scale * math.log2(math.e)))
        buf[:, at(j0 + ROWS, COLS)] = prob
        l_ref[...] += fold_lanes(jnp.add, prob)
        acc_ref[...] += mm(prob.astype(BF16), v_ref[at(j0, COLS), :])

    inv_sum = 1.0 / jnp.sum(l_ref[...], axis=1, keepdims=True)
    out = acc_ref[...] * inv_sum
    o_ref[at(out_row, ROWS), :] = out.astype(BF16)
    d_out = do_ref[at(q0, ROWS), :]
    do_wide = d_out.astype(F32)
    delta = jnp.sum(do_wide * out, axis=1, keepdims=True)
    do_t = do_wide.T.astype(BF16)
    qu_t = q_u.astype(F32).T.astype(BF16)
    qv_rt = flip_eights(q_v.astype(F32)).T.astype(BF16)
    gu_ref[...] = jnp.zeros_like(gu_ref)
    gv_ref[...] = jnp.zeros_like(gv_ref)

    def by_key(c):
        j0 = c * COLS
        cols = at(j0, COLS)
        prob = buf[:, at(j0 + ROWS, COLS)] * inv_sum
        ds_wide = prob * (mm(d_out, v_ref[cols, :], NT) - delta)
        ds = ds_wide.astype(BF16)
        dvt[:, cols] += mm(do_t, prob.astype(BF16))
        dkt[:, cols] += mm(qu_t, ds)
        gu_ref[...] += mm(ds, k_ref[cols, :])
        buf[:, at(j0 + ROWS, COLS)] = ds_wide

    def by_offset(c):
        c0 = c * COLS
        ds = shear_back(buf, c0 + ROWS).astype(BF16)
        cols = at(rel0 + c0, COLS)
        gv_ref[...] += mm(ds, rel_ref[cols, :])
        drt[:, cols] += mm(qv_rt, ds)

    by_key(0)

    @pl.loop(1, steps)
    def _(c):
        by_offset(c - 1)
        by_key(c)
        if after_step is not None:
            after_step(c - 1)

    by_offset(steps - 1)
    if after_step is not None:
        @pl.loop(steps - 1, seq // COLS)
        def _(c):
            after_step(c)

    g_u = gu_ref[...]
    g_vr = gv_ref[...]
    g_v = flip_eights(g_vr)
    dq_ref[at(out_row, ROWS), :] = ((g_u + g_v) * scale).astype(BF16)
    bias_acc[0:1, :] += jnp.sum(g_u, axis=0, keepdims=True) * scale
    bias_acc[1:2, :] += jnp.sum(g_vr, axis=0, keepdims=True) * scale


def tile_index(i, core):
    return 4 * (i // 2) + jnp.where(i % 2 == 0, core, 3 - core)


def group_kernel(q_hbm, k_hbm, v_hbm, do_hbm, rt_hbm, w_hbm, u_ref, vb_ref, o_out, dq_out, dk_out, dv_out, du_out, dvb_out, w_out, xh, relh, rel_flip, rt, w2, dkt, dvt, drt, part, red, red_r, o_tiles, bias_acc, bias_in, dr_in, w_part, w_in, rs_in, *rest):
    scratch, sems = rest[:6], rest[6:]
    (in_send, in_recv, fwd_send, fwd_recv, part_send, part_recv, tile_send, red_send, bias_send, out_recv, g_recv, bias_recv, load_sem,
     dr_recv, pair_send, pair_recv, rs_send, rs_recv, ag_send, ag_recv, agp_recv, go_sem) = sems
    inputs = (q_hbm, k_hbm, v_hbm, do_hbm)
    n_heads, block, dim = q_hbm.shape
    n_dev = lax.axis_size('cp')
    n_chips = n_dev // 2
    seq = block * n_dev
    n_steps = seq // COLS
    scale = dim ** -0.5
    me = lax.axis_index('cp')
    chip, core = me // 2, me % 2
    head = jnp.minimum(chip, n_heads - 1)
    active = chip < n_heads
    partner = 2 * chip + 1 - core
    n_tiles = seq // ROWS // 2

    load_rt = pltpu.make_async_copy(rt_hbm, rt, load_sem.at[0])
    loads_w = [pltpu.make_async_copy(w_hbm.at[h], w2.at[:, h * dim:(h + 1) * dim], load_sem.at[1 + h]) for h in range(n_heads)]
    load_rt.start()
    for load_w in loads_w:
        load_w.start()

    barrier = pltpu.get_barrier_semaphore()
    for d in range(1, n_dev):
        pl.semaphore_signal(barrier, inc=1, device_id={'cp': (me + d) % n_dev}, device_id_type=pl.DeviceIdType.MESH)
    pl.semaphore_wait(barrier, n_dev - 1)

    def push(src, dst, send, recv, dev):
        return pltpu.make_async_remote_copy(src_ref=src, dst_ref=dst, send_sem=send, recv_sem=recv, device_id={'cp': dev}, device_id_type=pl.DeviceIdType.MESH)

    def rows_of(dev):
        return pl.ds(pl.multiple_of(dev * block, block), block)

    def flip_rows_of(dev):
        return pl.ds(pl.multiple_of(seq - block - dev * block, block), block)

    def x_copies(src_dev, srcs, send, recv, dev):
        return [push(srcs[a], xh.at[a, rows_of(src_dev), :], send.at[0], recv.at[0], dev) for a in range(4)]

    def x_all(src_dev, send, recv):
        rows = xh.at[:, rows_of(src_dev), :]
        return push(rows, rows, send.at[0], recv.at[0], partner)

    def rel_copy(src_dev, src, send, recv, dev):
        return push(src, relh.at[flip_rows_of(src_dev), :], send.at[1], recv.at[1], dev)

    def x_to_head(dest):
        for copy in x_copies(me, [x.at[dest] for x in inputs], in_send.at[dest], in_recv.at[chip], 2 * dest + core):
            copy.start()

    def rel_to_head(dest):
        return rel_copy(me, rel_flip.at[dest], in_send.at[dest], in_recv.at[chip], 2 * dest + core)

    def x_to_partner(dev, srcs):
        for copy in x_copies(dev, srcs, fwd_send.at[dev // 2], fwd_recv.at[dev // 2], partner):
            copy.start()

    def rel_to_partner(dev, src):
        return rel_copy(dev, src, fwd_send.at[dev // 2], fwd_recv.at[dev // 2], partner)

    def rel_local():
        return pltpu.make_async_copy(rel_flip.at[head], relh.at[flip_rows_of(me), :], in_recv.at[chip, 1])

    anti = (lax.broadcasted_iota(jnp.int32, (256, 256), 0) + lax.broadcasted_iota(jnp.int32, (256, 256), 1) == 255).astype(F32).astype(BF16)
    orders = ((1, 2), (0, 2), (1, 0), (2, 0, 1))

    def first_to_head():
        for z, order in enumerate(orders):
            @pl.when(chip == z)
            def _():
                x_to_head(order[0])

    def rest_to_head(z, order):
        for dest in order[1:]:
            x_to_head(dest)
            rel_to_head(dest).start()

    first_to_head()

    @pl.when(active)
    def _():
        for a, x in enumerate(inputs):
            pltpu.make_async_copy(x.at[head], xh.at[a, rows_of(me), :], in_recv.at[chip, 0]).start()
        x_to_partner(me, [x.at[head] for x in inputs])

    load_rt.wait()
    for load_w in loads_w:
        load_w.wait()
    n_groups = block // 256

    @pl.loop(0, n_groups)
    def _(g):
        rows = pl.ds(pl.multiple_of(g * 256, 256), 256)
        flipped = pl.ds(pl.multiple_of((n_groups - 1 - g) * 256, 256), 256)
        rel = mm(anti, mm(rt[rows, :], w2[...]).astype(BF16)).astype(BF16)
        for h in range(n_heads):
            rel_flip[h, flipped, :] = rel[:, h * dim:(h + 1) * dim]

    for z, order in enumerate(orders):
        @pl.when(chip == z)
        def _():
            rel_to_head(order[0]).start()
            if z < n_chips - 1:
                rest_to_head(z, order)

    @pl.when(active)
    def _():
        rel_local().start()
        rel_to_partner(me, rel_flip.at[head]).start()

    dkt[...] = jnp.zeros_like(dkt)
    dvt[...] = jnp.zeros_like(dvt)
    drt[...] = jnp.zeros_like(drt)
    bias_acc[...] = jnp.zeros_like(bias_acc)
    scratch[0][:, :ROWS] = jnp.zeros((ROWS, ROWS), F32)
    relh[pl.ds(seq, COLS), :] = jnp.zeros((COLS, dim), BF16)

    def sent_to_head(dest):
        x_all(me, in_send.at[dest], in_recv.at[chip]).wait_send()
        rel_to_head(dest).wait_send()

    @pl.when(chip == n_chips - 2)
    def _():
        for dest in orders[n_chips - 2]:
            sent_to_head(dest)
        pl.semaphore_signal(go_sem, inc=1, device_id={'cp': jnp.minimum(me + 2, n_dev - 1)}, device_id_type=pl.DeviceIdType.MESH)

    @pl.when(chip == n_chips - 1)
    def _():
        @pl.when(core == 0)
        def _():
            pl.semaphore_wait(go_sem, 1)
            rest_to_head(n_chips - 1, orders[n_chips - 1])
            for dest in orders[n_chips - 1]:
                sent_to_head(dest)
            pl.semaphore_signal(go_sem, inc=1, device_id={'cp': partner}, device_id_type=pl.DeviceIdType.MESH)

        @pl.when(core == 1)
        def _():
            pl.semaphore_wait(go_sem, 2)
            rest_to_head(n_chips - 1, orders[n_chips - 1])

    q_ref, k_ref, v_ref, do_ref = (xh.at[a] for a in range(4))
    pieces = ROWS // 256

    def start(owner, local, remote):
        @pl.when(owner == me)
        def _():
            local().start()

        @pl.when(owner != me)
        def _():
            remote().start()

    def finish(owner, local, remote):
        @pl.when(owner != me)
        def _():
            remote().wait_send()

    per = block // 256

    def piece_of(g):
        return pl.ds(pl.multiple_of(g * 256, 256), 256)

    def tile_copy(i, g, a):
        piece = tile_index(i, core) * pieces + g
        owner = piece // per
        src = o_tiles.at[a, piece_of(i * pieces + g), :]
        dst = (o_out, dq_out)[a].at[head, piece_of(piece % per), :]
        return owner, lambda: pltpu.make_async_copy(src, dst, out_recv.at[a]), lambda: push(src, dst, tile_send.at[i, g, a], out_recv.at[a], owner)

    def ready_blocks(i):
        return (2 * ROWS * i + block - 1) // block

    accs = (dkt, dvt, drt)
    arrays = (2, 0, 1)

    def part_copy(a, c, parity):
        return push(accs[a].at[:, piece_of(2 * c + parity)], part.at[a, c], part_send.at[a, c], part_recv.at[a, c], partner)

    def red_copy(a, c):
        piece = 2 * c + core
        if a == 2:
            src, owner, dst, recv = red_r.at[c], n_dev - 1 - piece // per, dr_in.at[head, :, piece_of(piece % per)], dr_recv
        else:
            src, owner, dst, recv = red.at[a, c], piece // per, (dk_out, dv_out)[a].at[head, piece_of(piece % per), :], g_recv.at[a]
        return owner, lambda: pltpu.make_async_copy(src, dst, recv), lambda: push(src, dst, red_send.at[a, c], recv, owner)

    def reduce(c):
        for a in arrays:
            part_copy(a, c, core).wait_recv()
            total = accs[a][:, piece_of(2 * c + core)] + part[a, c]
            if a == 2:
                red_r[c] = (total * scale).astype(BF16)
            else:
                red[a, c] = (total if a == 1 else total * scale).T.astype(BF16)
            start(*red_copy(a, c))

    lag = 2

    def after_step(c):
        for a in arrays:
            part_copy(a, c, 1 - core).start()

        @pl.when(c >= lag)
        def _():
            reduce(c - lag)

    def bias_copy(d):
        owner = (me + d) % n_dev
        src, dst = bias_acc, bias_in.at[2 * head + core]
        return owner, lambda: pltpu.make_async_copy(src, dst, bias_recv), lambda: push(src, dst, bias_send.at[d], bias_recv, owner)

    @pl.when(active)
    def _():
        def tile(i, **kw):
            with jax.named_scope('wait_ici'):
                @pl.loop(ready_blocks(i), ready_blocks(i + 1))
                def _(dev):
                    @pl.when(dev == me)
                    def _():
                        local = xh.at[:, rows_of(me), :]
                        pltpu.make_async_copy(local, local, in_recv.at[chip, 0]).wait()
                        rel_local().wait()

                    @pl.when((dev % 2 == core) & (dev != me))
                    def _():
                        x_all(dev, in_send.at[0], in_recv.at[dev // 2]).wait_recv()
                        rel_copy(dev, rel_flip.at[head], in_send.at[0], in_recv.at[dev // 2], partner).wait_recv()
                        x_to_partner(dev, [xh.at[a, rows_of(dev), :] for a in range(4)])
                        rel_to_partner(dev, relh.at[flip_rows_of(dev), :]).start()

            with jax.named_scope('wait_core'):
                @pl.loop(ready_blocks(i), ready_blocks(i + 1))
                def _(dev):
                    @pl.when(dev % 2 != core)
                    def _():
                        x_all(dev, fwd_send.at[dev // 2], fwd_recv.at[dev // 2]).wait_recv()
                        rel_to_partner(dev, rel_flip.at[head]).wait_recv()

            tile_grads(tile_index(i, core) * ROWS, i * ROWS, q_ref, k_ref, v_ref, do_ref, relh, u_ref.at[pl.ds(head, 1), :], vb_ref.at[pl.ds(head, 1), :], o_tiles.at[0], o_tiles.at[1], dkt, dvt, drt, bias_acc, *scratch, **kw)
            for g in range(pieces):
                for a in range(2):
                    start(*tile_copy(i, g, a))

        @pl.loop(0, n_tiles - 1)
        def _(i):
            tile(i)

        tile(jnp.int32(n_tiles - 1), after_step=after_step)

        for d in range(n_dev):
            start(*bias_copy(d))

        @pl.loop(n_steps - lag, n_steps)
        def _(c):
            reduce(c)

    half, quarter = w_part.shape[1] // 2, w_part.shape[1] // 2 // n_chips
    sub = quarter // SUBS
    with jax.named_scope('wait_drel'):
        pltpu.make_async_copy(dr_in, dr_in, dr_recv).wait()

    def d_rel_of(h):
        return jnp.concatenate([mm(dr_in[h, :, g * 256:(g + 1) * 256], anti) for g in reversed(range(n_groups))], axis=1).astype(BF16)

    d_rel = jnp.concatenate([d_rel_of(h) for h in range(n_heads)], axis=0)

    def half_rows(c):
        return pl.ds(pl.multiple_of(c * half, half), half)

    def w_rows(c):
        @pl.loop(0, half // 256)
        def _(g):
            rows = pl.ds(pl.multiple_of(c * half + g * 256, 256), 256)
            term = lax.dot_general(rt[:, rows], d_rel, (((0,), (1,)), ((), ())), preferred_element_type=F32)
            for h in range(n_heads):
                w_part[h, rows, :] = term[:, h * dim:(h + 1) * dim]

    pair = push(w_part.at[:, half_rows(1 - core), :], w_in, pair_send, pair_recv, partner)
    with jax.named_scope('w_mm'):
        w_rows(1 - core)
        pair.start()
        w_rows(core)
        pair.wait_recv()
        w_part[:, half_rows(core), :] += w_in[...]

    def sub_rows(q, s):
        return pl.ds(pl.multiple_of(core * half + q * quarter + s * sub, 8), sub)

    side = chip // 2
    mate = chip + 1 - 2 * (chip % 2)
    inner = (chip > 0) & (chip < n_chips - 1)
    far_pair = 2 * (1 - side)
    gate = 2 - side

    def in_rows(s):
        return pl.ds(pl.multiple_of(s * sub, 8), sub)

    def rs_copy(q, slot, s, to):
        return push(w_part.at[:, sub_rows(q, s), :], rs_in.at[slot, :, in_rows(s), :], rs_send.at[slot, s], rs_recv.at[slot, s], 2 * to + core)

    def ag_copy(way, q, s):
        rows = w_out.at[:, sub_rows(q, s), :]
        return push(rows, rows, ag_send.at[way, q, s], agp_recv if way == 2 else ag_recv.at[q, s], (2 * mate + core, 2 * gate + core, partner)[way])

    def add_in(q, slot, s):
        rs_copy(q, slot, s, mate).wait_recv()
        rows = sub_rows(q, s)
        w_part[:, rows, :] += rs_in[slot, :, in_rows(s), :]

    def every_part(body):
        for s in range(SUBS):
            body(s)

    @every_part
    def _(s):
        @pl.when(jnp.logical_not(inner))
        def _():
            for f in range(2):
                rs_copy(far_pair + f, 2 + f, s, mate).start()

        rs_copy(mate, 0, s, mate).start()

    @pl.when(inner)
    def _():
        @every_part
        def _(s):
            for f in range(2):
                add_in(far_pair + f, 2 + f, s)
                push(w_part.at[:, sub_rows(far_pair + f, s), :], rs_in.at[1, :, in_rows(s), :], rs_send.at[2 + f, s], rs_recv.at[1, s], 2 * (far_pair + f) + core).start()

    @every_part
    def _(s):
        add_in(chip, 0, s)
        add_in(chip, 1, s)
        rows = sub_rows(chip, s)
        w_out[:, rows, :] = w_part[:, rows, :]
        ag_copy(0, chip, s).start()

        @pl.when(inner)
        def _():
            ag_copy(1, chip, s).start()

        ag_copy(2, chip, s).start()

    @every_part
    def _(s):
        ag_copy(0, mate, s).wait_recv()

        @pl.when(inner)
        def _():
            ag_copy(1, mate, s).start()

        ag_copy(2, mate, s).start()
        for f in range(2):
            ag_copy(0, far_pair + f, s).wait_recv()

            @pl.when(inner)
            def _():
                ag_copy(0, far_pair + f, s).start()

            ag_copy(2, far_pair + f, s).start()

    pair.wait_send()

    @pl.loop(0, SUBS)
    def _(s):
        rs_copy(mate, 0, s, mate).wait_send()
        for f in range(2):
            rs_copy(far_pair + f, 2 + f, s, mate).wait_send()

            @pl.when(inner)
            def _():
                ag_copy(0, far_pair + f, s).wait_send()

            ag_copy(2, far_pair + f, s).wait_send()
        ag_copy(2, mate, s).wait_send()
        ag_copy(0, chip, s).wait_send()
        ag_copy(2, chip, s).wait_send()

        @pl.when(inner)
        def _():
            ag_copy(1, chip, s).wait_send()
            ag_copy(1, mate, s).wait_send()

    other = w_out.at[:, half_rows(1 - core), :]
    pltpu.make_async_copy(other, other, agp_recv).wait()

    @pl.when(active)
    def _():
        @pl.loop(0, n_steps)
        def _(c):
            for a in arrays:
                part_copy(a, c, 1 - core).wait_send()
                finish(*red_copy(a, c))

        for d in range(n_dev):
            finish(*bias_copy(d))

        @pl.loop(0, n_tiles)
        def _(i):
            for g in range(pieces):
                for a in range(2):
                    finish(*tile_copy(i, g, a))

        @pl.loop(0, n_chips)
        def _(z):
            dev = 2 * z + core
            x_all(dev, fwd_send.at[z], fwd_recv.at[z]).wait_send()
            rel_to_partner(dev, rel_flip.at[head]).wait_send()

    for dest in range(n_heads):
        @pl.when((chip != dest) & (chip != n_chips - 2) & jnp.logical_not((chip == n_chips - 1) & (core == 0)))
        def _():
            sent_to_head(dest)
    pltpu.make_async_copy(bias_in, bias_in, bias_recv).wait()
    for h in range(n_heads):
        both = bias_in[2 * h] + bias_in[2 * h + 1]
        du_out[h:h + 1, :] = both[0:1]
        dvb_out[h:h + 1, :] = both[1:2]
    with jax.named_scope('wait_results'):
        for a in range(2):
            pltpu.make_async_copy((o_out, dq_out)[a], (o_out, dq_out)[a], out_recv.at[a]).wait()
            pltpu.make_async_copy((dk_out, dv_out)[a], (dk_out, dv_out)[a], g_recv.at[a]).wait()


def group_call(q, k, v, d_out, rel_table, w_rel, u_bias, v_bias, n_dev):
    n_heads, block, dim = q.shape
    like_q = jax.ShapeDtypeStruct((n_heads, block, dim), BF16)
    like_u = jax.ShapeDtypeStruct((n_heads, dim), F32)
    model = rel_table.shape[1]
    seq = block * n_dev
    n_chips = n_dev // 2
    n_tiles = seq // ROWS // 2
    n_steps = seq // COLS
    anyw = pl.BlockSpec(memory_space=pl.ANY)
    vmem = pl.BlockSpec(memory_space=pltpu.VMEM)
    dma = pltpu.SemaphoreType.DMA
    return pl.pallas_call(
        group_kernel,
        name='rel_attention',
        in_specs=[anyw] * 6 + [vmem] * 2,
        out_specs=[anyw] * 4 + [vmem] * 3,
        out_shape=[like_q] * 4 + [like_u] * 2 + [jax.ShapeDtypeStruct((n_heads, model, dim), F32)],
        scratch_shapes=[
            pltpu.VMEM((4, seq, dim), BF16),
            pltpu.VMEM((seq + COLS, dim), BF16),
            pltpu.VMEM((n_heads, block, dim), BF16),
            pltpu.VMEM((block, model), BF16),
            pltpu.VMEM((model, n_heads * dim), BF16),
            pltpu.VMEM((dim, seq), F32),
            pltpu.VMEM((dim, seq), F32),
            pltpu.VMEM((dim, seq + COLS), F32),
            pltpu.VMEM((3, n_steps, dim, 256), F32),
            pltpu.VMEM((2, n_steps, 256, dim), BF16),
            pltpu.VMEM((n_steps, dim, 256), BF16),
            pltpu.VMEM((2, seq // 2, dim), BF16),
            pltpu.VMEM((8, dim), F32),
            pltpu.VMEM((2 * n_heads, 8, dim), F32),
            pltpu.VMEM((n_heads, dim, block), BF16),
            pltpu.VMEM((n_heads, model, dim), F32),
            pltpu.VMEM((n_heads, model // 2, dim), F32),
            pltpu.VMEM((4, n_heads, model // 2 // n_chips, dim), F32),
            pltpu.VMEM((ROWS, seq + ROWS + COLS), F32),
            pltpu.VMEM((ROWS, 128), F32),
            pltpu.VMEM((ROWS, 128), F32),
            pltpu.VMEM((ROWS, dim), F32),
            pltpu.VMEM((ROWS, dim), F32),
            pltpu.VMEM((ROWS, dim), F32),
            dma((n_heads, 2)), dma((n_chips, 2)), dma((n_chips, 2)), dma((n_chips, 2)),
            dma((3, n_steps)), dma((3, n_steps)), dma((n_tiles, ROWS // 256, 2)), dma((3, n_steps)), dma((n_dev,)), dma((2,)), dma((2,)), dma, dma((1 + n_heads,)),
            dma, dma, dma, dma((4, SUBS)), dma((4, SUBS)), dma((3, n_chips, SUBS)), dma((n_chips, SUBS)), dma, pltpu.SemaphoreType.REGULAR,
        ],
        compiler_params=pltpu.CompilerParams(vmem_limit_bytes=67043328, collective_id=0, has_side_effects=True),
    )(q, k, v, d_out, rel_table, w_rel, u_bias, v_bias)


def hand_over(*refs):
    n = (len(refs) - 2) // 3
    srcs, dsts, bufs = refs[:n], refs[n:2 * n], refs[2 * n:3 * n]
    in_sem, out_sem = refs[3 * n:]
    loads = [pltpu.make_async_copy(srcs[i], bufs[i], in_sem.at[i]) for i in range(n)]
    stores = [pltpu.make_async_copy(bufs[i], dsts[i], out_sem.at[i]) for i in range(n)]
    for load in loads:
        load.start()
    for load, store in zip(loads, stores):
        load.wait()
        store.start()
    for store in stores:
        store.wait()


def hand_over_call(arrays):
    n = len(arrays)
    anyw = pl.BlockSpec(memory_space=pl.ANY)
    return pl.pallas_call(
        hand_over,
        name='hand_over',
        in_specs=[anyw] * n,
        out_specs=[anyw] * n,
        out_shape=[jax.ShapeDtypeStruct(x.shape, x.dtype) for x in arrays],
        scratch_shapes=[pltpu.VMEM(x.shape, x.dtype) for x in arrays] + [pltpu.SemaphoreType.DMA((n,))] * 2,
        compiler_params=pltpu.CompilerParams(vmem_limit_bytes=67043328),
    )(*arrays)


def solution(mesh):
    n_dev = mesh.shape['cp']
    seq_spec = P('cp', 'hp', None)
    head_spec = P('hp', None)
    weight_spec = P(None, 'hp', None)

    def local_fn(q, k, v, u_bias, v_bias, rel_table, w_rel, d_out):
        swap = lambda x: x.transpose(1, 0, 2)
        *rows, d_u, d_v, d_w = hand_over_call(group_call(swap(q), swap(k), swap(v), swap(d_out), rel_table, swap(w_rel), u_bias, v_bias, n_dev))
        return (*(swap(x) for x in rows), d_u, d_v, swap(d_w))

    return jax.shard_map(
        local_fn,
        mesh=mesh,
        in_specs=(seq_spec, seq_spec, seq_spec, head_spec, head_spec, P('cp', None), weight_spec, seq_spec),
        out_specs=(seq_spec, seq_spec, seq_spec, seq_spec, head_spec, head_spec, weight_spec),
        check_vma=False,
    )
```
